16 devices in a mesh: dp: 2 (over y, z), sp: 8 (over x, core).
Axes of the slice: x: 4, y: 2, z: 1, core: 2. Of those that a mesh axis runs over, the one named last changes fastest.
The devices are a block of a 4x4x8 slice.
Arguments:
- u_in: bfloat16 [2, 16384, 1024], P('dp', 'sp'), parts along dimension 0
- w_in: bfloat16 [1024, 3072], replicated
- b_in: float32 [3072], replicated
- conv_taps: float32 [3, 3072], replicated
- w_out: bfloat16 [1024, 1024], replicated
- skip_one: float32 [1024], replicated
- skip_two: float32 [1024], replicated
- filt_one: float32 [16384, 1024], P('sp')
- filt_two: float32 [16384, 1024], P('sp')
Outputs:
- output: bfloat16 [2, 16384, 1024], P('dp', 'sp'), parts along dimension 0
There are 2 independent parts. The reference program is written for one: setup_inputs(seed, part) draws one part's arguments, and reference() takes and returns one part's arrays. A program takes and returns all parts, laid end to end along the dimension named above; an argument that names none is the same for every part.
All inputs are finite; a program needn't handle non-finite values.
Results may differ from the reference program's by a relative error of at most 0.0149239.
Values sent between devices are 32-bit elements.
A program may use at most 768 MiB of HBM per device.

```python
import jax
import jax.numpy as jnp
from jax import lax

BATCH_SIZE = 1
SEQ_LEN = 16384
MODEL_DIM = 1024
CHAN_BLOCK = 128


def draw_filter(filt_key):
    noise_key, rate_key = jax.random.split(filt_key)
    decay_rates = jax.random.uniform(rate_key, (MODEL_DIM,), jnp.float32, 0.0, 2.0)
    rel_pos = jnp.arange(SEQ_LEN, dtype=jnp.float32)[:, None] / SEQ_LEN
    noise_vals = jax.random.normal(noise_key, (SEQ_LEN, MODEL_DIM), jnp.float32)
    return noise_vals * jnp.exp(-decay_rates[None, :] * rel_pos) * (1.5 * SEQ_LEN ** -0.5)


def setup_inputs(seed: int = 0, part: int = 0) -> dict:
    key_list = jax.random.split(jax.random.key(seed), 9)
    model_width = MODEL_DIM
    fan_scale = model_width ** -0.5
    u_in = jax.random.normal(jax.random.fold_in(key_list[0], part), (BATCH_SIZE, SEQ_LEN, model_width), jnp.float32)
    w_in = jax.random.normal(key_list[1], (model_width, 3 * model_width), jnp.float32) * fan_scale
    b_in = 0.5 * jax.random.normal(key_list[2], (3 * model_width,), jnp.float32)
    conv_taps = 0.6 * jax.random.normal(key_list[3], (3, 3 * model_width), jnp.float32)
    w_out = jax.random.normal(key_list[4], (model_width, model_width), jnp.float32) * fan_scale
    skip_one = jax.random.normal(key_list[5], (model_width,), jnp.float32)
    skip_two = jax.random.normal(key_list[6], (model_width,), jnp.float32)
    return {'u_in': u_in.astype(jnp.bfloat16), 'w_in': w_in.astype(jnp.bfloat16), 'b_in': b_in, 'conv_taps': conv_taps, 'w_out': w_out.astype(jnp.bfloat16), 'skip_one': skip_one, 'skip_two': skip_two, 'filt_one': draw_filter(key_list[7]), 'filt_two': draw_filter(key_list[8])}


def causal_conv(signal, filt):
    seq_len = signal.shape[0]
    spectrum = jnp.fft.rfft(signal, n=2 * seq_len, axis=0) * jnp.fft.rfft(filt, n=2 * seq_len, axis=0)
    return jnp.fft.irfft(spectrum, n=2 * seq_len, axis=0)[:seq_len]


def reference(u_in, w_in, b_in, conv_taps, w_out, skip_one, skip_two, filt_one, filt_two):
    n_blocks = MODEL_DIM // CHAN_BLOCK

    def by_blocks(array_2d):
        return jnp.moveaxis(array_2d.reshape(array_2d.shape[0], n_blocks, CHAN_BLOCK), 1, 0)

    filt_blocks = (by_blocks(filt_one), by_blocks(filt_two), skip_one.reshape(n_blocks, CHAN_BLOCK), skip_two.reshape(n_blocks, CHAN_BLOCK))

    def one_block(block_args):
        gate_one, gate_two, values, h_one, h_two, d_one, d_two = block_args
        z_one = gate_one * (causal_conv(values, h_one) + d_one * values)
        return gate_two * (causal_conv(z_one, h_two) + d_two * z_one)

    def one_row(seq_row):
        projected = (jnp.dot(seq_row, w_in, preferred_element_type=jnp.float32) + b_in).astype(jnp.bfloat16).astype(jnp.float32)
        prev_one = jnp.pad(projected[:-1], ((1, 0), (0, 0)))
        prev_two = jnp.pad(projected[:-2], ((2, 0), (0, 0)))
        mixed = (conv_taps[0] * projected + conv_taps[1] * prev_one + conv_taps[2] * prev_two).astype(jnp.bfloat16).astype(jnp.float32)
        gate_one = by_blocks(mixed[:, :MODEL_DIM])
        gate_two = by_blocks(mixed[:, MODEL_DIM:2 * MODEL_DIM])
        values = by_blocks(mixed[:, 2 * MODEL_DIM:])
        gated = lax.map(one_block, (gate_one, gate_two, values) + filt_blocks)
        gated = jnp.moveaxis(gated, 0, 1).reshape(SEQ_LEN, MODEL_DIM)
        out_sum = seq_row.astype(jnp.float32) + jnp.dot(gated.astype(jnp.bfloat16), w_out, preferred_element_type=jnp.float32)
        return out_sum.astype(jnp.bfloat16)

    return lax.map(one_row, u_in)
```

```python
import functools
import jax
import jax.numpy as jnp
import numpy as np
from jax import lax
from jax.experimental import pallas as pl
from jax.experimental.pallas import tpu as pltpu
from jax.sharding import PartitionSpec as P

LANES = 128
F32 = jnp.float32
BF16 = jnp.bfloat16


def split_table(table, n_parts=3):
    parts, rest = [], np.asarray(table, np.float64)
    for _ in range(n_parts):
        part = rest.astype(jnp.bfloat16)
        parts.append(part)
        rest = rest - part.astype(np.float64)
    return parts


def transform_tables(seq_len):
    n_high = seq_len // LANES
    quarter = np.arange(n_high)[:, None] + 0.25
    high = 2.0 * np.pi * quarter * np.arange(n_high)[None, :] / n_high
    twist = 2.0 * np.pi * quarter * np.arange(LANES)[None, :] / seq_len
    low = 2.0 * np.pi * np.outer(np.arange(LANES), np.arange(LANES)) / LANES
    first = np.concatenate([np.cos(high), -np.sin(high)], axis=0)
    last = np.concatenate([np.cos(high.T), -np.sin(high.T)], axis=1)
    er, ei = np.cos(low), -np.sin(low)
    fwd = np.block([[er, ei], [-ei, er]])
    inv = np.block([[er, -ei], [ei, er]])
    a, b, c = split_table(first)
    first_wide = np.concatenate([a, a, a, b, b, c], axis=1)
    first_thin = np.concatenate([a, b, c], axis=1)
    fwd_parts = np.concatenate(split_table(fwd), axis=0)
    inv_parts = np.concatenate(split_table(inv), axis=0)
    last_parts = np.concatenate(split_table(last), axis=0)
    twist_tab = np.stack([np.cos(twist), -np.sin(twist)]).astype(np.float32)
    return first_wide, first_thin, fwd_parts, inv_parts, last_parts, twist_tab


def split3(x):
    hi = x.astype(BF16)
    rest = x - hi.astype(F32)
    mid = rest.astype(BF16)
    low = (rest - mid.astype(F32)).astype(BF16)
    return hi, mid, low


def dot32(a, b):
    return jnp.dot(a, b, preferred_element_type=F32)


def turn_filters_body(one_ref, two_ref, out_ref):
    n_rows = one_ref.shape[0] // LANES
    for which, ref in enumerate((one_ref, two_ref)):

        @pl.loop(0, n_rows)
        def _(r):
            block = ref[pl.ds(pl.multiple_of(r * LANES, LANES), LANES), :]
            out_ref[0, which, pl.ds(r, LANES, stride=n_rows), :] = block.T


def turn_filters(filt_one, filt_two, n_dev):
    rows = filt_one.shape[0]
    n_rows = rows // LANES
    spec = pl.BlockSpec((rows, LANES), lambda d: (0, d))
    return pl.pallas_call(
        turn_filters_body,
        grid=(n_dev,),
        in_specs=[spec, spec],
        out_specs=pl.BlockSpec((1, 2, LANES * n_rows, LANES), lambda d: (d, 0, 0, 0)),
        out_shape=jax.ShapeDtypeStruct((n_dev, 2, LANES * n_rows, LANES), F32),
        cost_estimate=pl.CostEstimate(flops=10**9, bytes_accessed=4 * 4 * rows * LANES * n_dev, transcendentals=0),
        compiler_params=pltpu.CompilerParams(dimension_semantics=("arbitrary",)),
        name="turn_filters",
    )(filt_one, filt_two)


def project_body(n_chunks, flag_ref, u_ref, halo_ref, *refs):
    w_refs, b_refs, tap_refs = refs[:3], refs[3:6], refs[6:9]
    sent_ref, gate_ref, p_ref = refs[9:]
    rows = u_ref.shape[0]
    n_rows = rows // LANES
    width = w_refs[0].shape[1]
    per_chunk = LANES // n_chunks
    for which in range(3):
        w = w_refs[which][...]
        bias = b_refs[which][...]
        halo = (dot32(halo_ref[...].astype(BF16), w) + bias).astype(BF16).astype(F32)
        p_ref[0:8, :] = jnp.where(flag_ref[0] > 0, halo, 0.0)
        step = 2 * LANES

        @pl.loop(0, rows // step)
        def _(i):
            start = pl.multiple_of(i * step, step)
            proj = dot32(u_ref[pl.ds(start, step), :], w) + bias
            p_ref[pl.ds(start + 8, step), :] = proj.astype(BF16).astype(F32)

        c0, c1, c2 = (tap_refs[which][t : t + 1, :] for t in range(3))

        @pl.loop(0, n_rows)
        def _(r):
            start = pl.multiple_of(r * LANES, LANES)
            window = p_ref[pl.ds(start, LANES + 8), :]
            mixed = c0 * window[8:] + c1 * window[7:-1] + c2 * window[6:-2]
            mixed = mixed.astype(BF16)
            if which == 1:
                gate_ref[pl.ds(start, LANES), :] = mixed
            else:
                slot = 1 if which == 0 else 0
                for d in range(width // LANES):
                    turned = mixed[:, d * LANES : (d + 1) * LANES].astype(F32).T
                    for k in range(n_chunks):
                        sent_ref[k, d, slot, pl.ds(r, per_chunk, stride=n_rows), :] = turned[k * per_chunk : (k + 1) * per_chunk]


def project(has_prev, u, halo, w_in, b_in, taps, n_dev, n_chunks):
    rows, depth = u.shape
    model = w_in.shape[1] // 3
    width = 2 * LANES
    steps = model // width
    n_rows = rows // LANES
    per_chunk = LANES // n_chunks
    chunk_rows = per_chunk * n_rows
    w_specs = [pl.BlockSpec((depth, width), functools.partial(lambda off, j: (0, off + j), t * steps)) for t in range(3)]
    b_specs = [pl.BlockSpec((1, width), functools.partial(lambda off, j: (0, off + j), t * steps)) for t in range(3)]
    t_specs = [pl.BlockSpec((3, width), functools.partial(lambda off, j: (0, off + j), t * steps)) for t in range(3)]
    return pl.pallas_call(
        functools.partial(project_body, n_chunks),
        grid=(steps,),
        in_specs=[
            pl.BlockSpec(memory_space=pltpu.SMEM),
            pl.BlockSpec((rows, depth), lambda j: (0, 0)),
            pl.BlockSpec((8, depth), lambda j: (0, 0)),
            *w_specs,
            *b_specs,
            *t_specs,
        ],
        out_specs=[
            pl.BlockSpec((n_chunks, 2, 2, chunk_rows, LANES), lambda j: (0, j, 0, 0, 0)),
            pl.BlockSpec((rows, width), lambda j: (0, j)),
        ],
        out_shape=[
            jax.ShapeDtypeStruct((n_chunks, n_dev, 2, chunk_rows, LANES), F32),
            jax.ShapeDtypeStruct((rows, model), BF16),
        ],
        scratch_shapes=[pltpu.VMEM((rows + 8, width), F32)],
        cost_estimate=pl.CostEstimate(flops=2 * rows * depth * 3 * model, bytes_accessed=30 * 2**20, transcendentals=0),
        compiler_params=pltpu.CompilerParams(dimension_semantics=("arbitrary",), vmem_limit_bytes=60 * 2**20),
        name="project",
    )(has_prev, u, halo, w_in, w_in, w_in, b_in, b_in, b_in, taps, taps, taps)


def spectrum_tools(group, n_high, tables, parts_ref):
    wide_ref, thin_ref, fwd_ref, inv_ref, last_ref, twist_ref = tables
    wide = 2 * LANES
    scale = 1.0 / (n_high * LANES)

    def complex_dot(tab_ref):
        return (
            dot32(parts_ref[:, 2 * wide :], tab_ref[:wide])
            + dot32(parts_ref[:, wide : 2 * wide], tab_ref[:wide])
            + dot32(parts_ref[:, :wide], tab_ref[wide : 2 * wide])
            + dot32(parts_ref[:, wide : 2 * wide], tab_ref[wide : 2 * wide])
            + dot32(parts_ref[:, :wide], tab_ref[2 * wide :])
            + dot32(parts_ref[:, :wide], tab_ref[:wide])
        )

    def store_parts(g, real, imag):
        for t, (re, im) in enumerate(zip(split3(real), split3(imag))):
            parts_ref[g * n_high : (g + 1) * n_high, 2 * t * LANES : (2 * t + 1) * LANES] = re
            parts_ref[g * n_high : (g + 1) * n_high, (2 * t + 1) * LANES : (2 * t + 2) * LANES] = im

    def spectrum(signals, exact):
        tr, ti = twist_ref[0], twist_ref[1]
        for g in range(0, group, 2):
            pair = jnp.concatenate([signals[g], signals[g + 1]], axis=1)
            if exact:
                short = pair.astype(BF16)
                coarse = dot32(thin_ref[...], jnp.concatenate([short, short, short], axis=0))
            else:
                hi, mid, low = split3(pair)
                coarse = dot32(wide_ref[...], jnp.concatenate([hi, mid, low, hi, mid, hi], axis=0))
            for j in range(2):
                re = coarse[:n_high, j * LANES : (j + 1) * LANES]
                im = coarse[n_high:, j * LANES : (j + 1) * LANES]
                store_parts(g + j, re * tr - im * ti, re * ti + im * tr)
        return complex_dot(fwd_ref)

    def signal(spec_a, spec_b):
        tr, ti = twist_ref[0], twist_ref[1]
        for g in range(group):
            rows = slice(g * n_high, (g + 1) * n_high)
            ar, ai = spec_a[rows, :LANES], spec_a[rows, LANES:]
            br, bi = spec_b[rows, :LANES], spec_b[rows, LANES:]
            store_parts(g, ar * br - ai * bi, ar * bi + ai * br)
        fine = complex_dot(inv_ref)
        results = []
        for g in range(0, group, 2):
            halves = []
            for j in range(2):
                rows = slice((g + j) * n_high, (g + j + 1) * n_high)
                re, im = fine[rows, :LANES] * scale, fine[rows, LANES:] * scale
                halves.append(jnp.concatenate([re * tr + im * ti, im * tr - re * ti], axis=0))
            hi, mid, low = split3(jnp.concatenate(halves, axis=1))
            d_hi = dot32(last_ref[...], hi)
            d_mid = dot32(last_ref[: 2 * n_high], mid)
            d_low = dot32(last_ref[:n_high], low)
            small = d_hi[2 * n_high :] + d_mid[n_high:] + d_low
            total = d_hi[:n_high] + ((d_hi[n_high : 2 * n_high] + d_mid[:n_high]) + small)
            results += [total[:, :LANES], total[:, LANES:]]
        return results

    return spectrum, signal


def exchange_body(n_dev, group, ahead, skip_ref, filt_ref, sent_ref, wide_ref, thin_ref, fwd_ref, inv_ref, last_ref, twist_ref, back_ref, got_ref, h_ref, done_ref, parts_ref, spec_one_ref, spec_two_ref, sent_sem, got_sem, h_sem, back_sem, done_sem):
    n_chunks, _, _, chunk_rows, _ = sent_ref.shape
    n_high = twist_ref.shape[1]
    per_src = n_high // n_dev
    n_chan = chunk_rows // per_src
    me = lax.axis_index("sp")
    spectrum, signal = spectrum_tools(group, n_high, (wide_ref, thin_ref, fwd_ref, inv_ref, last_ref, twist_ref), parts_ref)

    barrier = pltpu.get_barrier_semaphore()
    for off in range(1, n_dev):
        pl.semaphore_signal(barrier, inc=1, device_id={"sp": lax.rem(me + off, n_dev)}, device_id_type=pl.DeviceIdType.MESH)
    pl.semaphore_wait(barrier, n_dev - 1)

    def sending(k, off):
        dest = lax.rem(me + off, n_dev)
        return pltpu.make_async_remote_copy(
            src_ref=sent_ref.at[k, dest],
            dst_ref=got_ref.at[k, me],
            send_sem=sent_sem.at[k, off],
            recv_sem=got_sem.at[k, off],
            device_id={"sp": dest},
            device_id_type=pl.DeviceIdType.MESH,
        )

    def keeping(k):
        return pltpu.make_async_copy(sent_ref.at[k, me], got_ref.at[k, me], got_sem.at[k, 0])

    def fetching(k, slot):
        return pltpu.make_async_copy(
            filt_ref.at[:, :, pl.ds(pl.multiple_of(k * chunk_rows, chunk_rows), chunk_rows), :], h_ref.at[slot], h_sem.at[slot]
        )

    block = per_src * n_chan

    def part_of(slot, dest):
        return done_ref.at[slot, pl.ds(pl.multiple_of(dest * block, block), block), :]

    def returning(k, slot, off):
        dest = lax.rem(me + off, n_dev)
        return pltpu.make_async_remote_copy(
            src_ref=part_of(slot, dest),
            dst_ref=back_ref.at[k, me],
            send_sem=done_sem.at[slot, off],
            recv_sem=back_sem.at[k, off],
            device_id={"sp": dest},
            device_id_type=pl.DeviceIdType.MESH,
        )

    def storing(k, slot):
        return pltpu.make_async_copy(part_of(slot, me), back_ref.at[k, me], done_sem.at[slot, 0])

    def launch(k):
        keeping(k).start()
        for off in range(1, n_dev):
            sending(k, off).start()

    for k in range(ahead):
        launch(k)
    fetching(0, 0).start()

    @pl.loop(0, n_chunks)
    def _(k):
        slot = lax.rem(k, 2)

        @pl.when(k + ahead < n_chunks)
        def _():
            launch(k + ahead)

        @pl.when(k + 1 < n_chunks)
        def _():
            fetching(k + 1, 1 - slot).start()

        fetching(k, slot).wait()
        keeping(k).wait()
        for off in range(1, n_dev):
            sending(k, off).wait_recv()

        @pl.when(k >= 2)
        def _():
            storing(k - 2, slot).wait()
            for off in range(1, n_dev):
                returning(k - 2, slot, off).wait_send()

        @pl.loop(0, n_chan // group)
        def _(i):
            first = i * group

            def load_h(which, g):
                start = pl.multiple_of((first + g) * per_src, per_src)
                return h_ref[slot, :, which, pl.ds(start, per_src), :].reshape(n_high, LANES)

            def load_x(which, g):
                start = pl.multiple_of((first + g) * per_src, per_src)
                return got_ref[k, :, which, pl.ds(start, per_src), :].reshape(n_high, LANES)

            chan = k * n_chan + first
            spec_one_ref[...] = spectrum([load_h(0, g) for g in range(group)], False)
            spec_two_ref[...] = spectrum([load_h(1, g) for g in range(group)], False)
            values = [load_x(0, g) for g in range(group)]
            conv = signal(spectrum(values, True), spec_one_ref)
            gated = [load_x(1, g) * (conv[g] + skip_ref[0, chan + g] * values[g]) for g in range(group)]
            conv = signal(spectrum(gated, False), spec_two_ref)
            for g in range(group):
                done_ref[slot, pl.ds(first + g, n_high, stride=n_chan), :] = conv[g] + skip_ref[1, chan + g] * gated[g]

        storing(k, slot).start()
        for off in range(1, n_dev):
            returning(k, slot, off).start()

    for k in range(max(0, n_chunks - 2), n_chunks):
        storing(k, k % 2).wait()
        for off in range(1, n_dev):
            returning(k, k % 2, off).wait_send()

    @pl.loop(0, n_chunks)
    def _(k):
        for off in range(1, n_dev):
            sending(k, off).wait_send()
            returning(k, 0, off).wait_recv()


def exchange(skips, filters, sent, tables, n_dev, group=4, ahead=3):
    n_chunks, _, _, chunk_rows, _ = sent.shape
    n_high = tables[-1].shape[1]
    n_chan = chunk_rows // (n_high // n_dev)
    any_spec = pl.BlockSpec(memory_space=pl.ANY)
    vmem_spec = pl.BlockSpec(memory_space=pltpu.VMEM)
    return pl.pallas_call(
        functools.partial(exchange_body, n_dev, group, ahead),
        in_specs=[pl.BlockSpec(memory_space=pltpu.SMEM), any_spec, any_spec] + [vmem_spec] * len(tables),
        out_specs=any_spec,
        out_shape=jax.ShapeDtypeStruct((n_chunks, n_dev, chunk_rows, LANES), F32),
        scratch_shapes=[
            pltpu.VMEM((n_chunks, n_dev, 2, chunk_rows, LANES), F32),
            pltpu.VMEM((2, n_dev, 2, chunk_rows, LANES), F32),
            pltpu.VMEM((2, n_high * n_chan, LANES), F32),
            pltpu.VMEM((group * n_high, 6 * LANES), BF16),
            pltpu.VMEM((group * n_high, 2 * LANES), F32),
            pltpu.VMEM((group * n_high, 2 * LANES), F32),
            pltpu.SemaphoreType.DMA((n_chunks, n_dev)),
            pltpu.SemaphoreType.DMA((n_chunks, n_dev)),
            pltpu.SemaphoreType.DMA((2,)),
            pltpu.SemaphoreType.DMA((n_chunks, n_dev)),
            pltpu.SemaphoreType.DMA((2, n_dev)),
        ],
        cost_estimate=pl.CostEstimate(flops=10**11, bytes_accessed=40 * 2**20, transcendentals=0),
        compiler_params=pltpu.CompilerParams(collective_id=0, has_side_effects=True, vmem_limit_bytes=60 * 2**20),
        name="exchange",
    )(skips, filters, sent, *tables)


def finish_body(gate_ref, u_ref, w_ref, back_ref, out_ref, y_ref):
    n_chunks, n_src, n_rows, _, _ = back_ref.shape
    for r in range(n_rows):
        for s in range(n_src):
            full = jnp.concatenate([back_ref[k, s, r] for k in range(n_chunks)], axis=0)
            rows, cols = slice(r * LANES, (r + 1) * LANES), slice(s * LANES, (s + 1) * LANES)
            y_ref[rows, cols] = (gate_ref[rows, cols].astype(F32) * full.T).astype(BF16)
    out_ref[...] = (u_ref[...].astype(F32) + dot32(y_ref[...], w_ref[...])).astype(BF16)


def finish(gate, u, w_out, back, n_rows=2):
    rows, model = u.shape
    n_chunks, n_src, _, per_chunk, _ = back.shape
    tile = n_rows * LANES
    return pl.pallas_call(
        finish_body,
        grid=(rows // tile,),
        in_specs=[
            pl.BlockSpec((tile, model), lambda i: (i, 0)),
            pl.BlockSpec((tile, model), lambda i: (i, 0)),
            pl.BlockSpec(w_out.shape, lambda i: (0, 0)),
            pl.BlockSpec((n_chunks, n_src, n_rows, per_chunk, LANES), lambda i: (0, 0, i, 0, 0)),
        ],
        out_specs=pl.BlockSpec((tile, model), lambda i: (i, 0)),
        out_shape=jax.ShapeDtypeStruct((rows, model), BF16),
        scratch_shapes=[pltpu.VMEM((tile, model), BF16)],
        cost_estimate=pl.CostEstimate(flops=2 * rows * model * model, bytes_accessed=20 * 2**20, transcendentals=0),
        compiler_params=pltpu.CompilerParams(dimension_semantics=("arbitrary",), vmem_limit_bytes=48 * 2**20),
        name="finish",
    )(gate, u, w_out, back)


def solution(mesh):
    n_dev = mesh.shape["sp"]
    n_chunks = 8
    halo_perm = list(zip(range(n_dev - 1), range(1, n_dev)))

    def local_step(u_in, w_in, b_in, conv_taps, w_out, skip_one, skip_two, filt_one, filt_two):
        rank = lax.axis_index("sp")
        u = u_in[0]
        rows = u.shape[0]
        tables = [jnp.asarray(t) for t in transform_tables(rows * n_dev)]

        def swap(x):
            return lax.all_to_all(x, "sp", 0, 0, tiled=True)

        halo = lax.ppermute(u[-8:].astype(F32), "sp", halo_perm)
        has_prev = (rank > 0).astype(jnp.int32)[None]
        filters = swap(turn_filters(filt_one, filt_two, n_dev))
        sent, gate = project(has_prev, u, halo, w_in, b_in[None], conv_taps, n_dev, n_chunks)
        skips = lax.dynamic_slice_in_dim(jnp.stack([skip_one, skip_two]), rank * LANES, LANES, axis=1)
        back = exchange(skips, filters, sent, tables, n_dev)
        back = back.reshape(n_chunks, n_dev, rows // LANES, LANES // n_chunks, LANES)
        return finish(gate, u, w_out, back)[None]

    seq_spec = P("dp", "sp", None)
    filt_spec = P("sp", None)
    return jax.shard_map(
        local_step,
        mesh=mesh,
        in_specs=(seq_spec, P(), P(), P(), P(), P(), P(), filt_spec, filt_spec),
        out_specs=seq_spec,
        check_vma=False,
    )
```

```python
import functools
import jax
import jax.numpy as jnp
import numpy as np
from jax import lax
from jax.experimental import pallas as pl
from jax.experimental.pallas import tpu as pltpu
from jax.sharding import PartitionSpec as P

LANES = 128
F32 = jnp.float32
BF16 = jnp.bfloat16


def split_table(table, n_parts=3):
    parts, rest = [], np.asarray(table, np.float64)
    for _ in range(n_parts):
        part = rest.astype(jnp.bfloat16)
        parts.append(part)
        rest = rest - part.astype(np.float64)
    return parts


def transform_tables(seq_len):
    n_high = seq_len // LANES
    quarter = np.arange(n_high)[:, None] + 0.25
    high = 2.0 * np.pi * quarter * np.arange(n_high)[None, :] / n_high
    twist = 2.0 * np.pi * quarter * np.arange(LANES)[None, :] / seq_len
    low = 2.0 * np.pi * np.outer(np.arange(LANES), np.arange(LANES)) / LANES
    first = np.concatenate([np.cos(high), -np.sin(high)], axis=0)
    last = np.concatenate([np.cos(high.T), -np.sin(high.T)], axis=1)
    er, ei = np.cos(low), -np.sin(low)
    fwd = np.block([[er, ei], [-ei, er]])
    inv = np.block([[er, -ei], [ei, er]])
    a, b, c = split_table(first)
    first_wide = np.concatenate([a, a, a, b, b, c], axis=1)
    first_thin = np.concatenate([a, b, c], axis=1)
    fwd_parts = np.concatenate(split_table(fwd), axis=0)
    inv_parts = np.concatenate(split_table(inv), axis=0)
    last_parts = np.concatenate(split_table(last), axis=0)
    twist_tab = np.stack([np.cos(twist), -np.sin(twist)]).astype(np.float32)
    return first_wide, first_thin, fwd_parts, inv_parts, last_parts, twist_tab


def split3(x):
    hi = x.astype(BF16)
    rest = x - hi.astype(F32)
    mid = rest.astype(BF16)
    low = (rest - mid.astype(F32)).astype(BF16)
    return hi, mid, low


def dot32(a, b):
    return jnp.dot(a, b, preferred_element_type=F32)


def turn_share_body(n_chunks, units, place_ref, one_ref, two_ref, out_ref, *scratch):
    n_rows = one_ref.shape[0] // LANES
    n_chan = LANES // n_chunks

    def turn(ref, into_ref, base):
        @pl.loop(0, n_rows)
        def _(r):
            block = ref[pl.ds(pl.multiple_of(r * LANES, LANES), LANES), :].T
            for k in range(n_chunks):
                into_ref[k, pl.ds(base + r, n_chan, stride=n_rows), :] = block[k * n_chan : (k + 1) * n_chan]

    if units == 2 * n_chan:
        turn(one_ref, out_ref.at[0], 0)
        turn(two_ref, out_ref.at[0], n_chan * n_rows)
    else:
        into_ref = out_ref.at[0] if units == n_chan else scratch[0]
        for which, ref in enumerate((one_ref, two_ref)):

            @pl.when(place_ref[0] == which)
            def _():
                turn(ref, into_ref, 0)

        if units < n_chan:
            start = pl.multiple_of(place_ref[1] * n_rows, n_rows)
            out_ref[0] = scratch[0][:, pl.ds(start, units * n_rows), :]


def turn_share(place, filt_one, filt_two, n_dev, n_chunks, units):
    rows = filt_one.shape[0]
    n_rows = rows // LANES
    n_chan = LANES // n_chunks
    both = units == 2 * n_chan

    def pick(which):
        def index(d, place_ref):
            return 0, (d if both else jnp.where(place_ref[0] == which, d, 0))

        return pl.BlockSpec((rows, LANES), index)

    return pl.pallas_call(
        functools.partial(turn_share_body, n_chunks, units),
        grid_spec=pltpu.PrefetchScalarGridSpec(
            num_scalar_prefetch=1,
            grid=(n_dev,),
            in_specs=[pick(0), pick(1)],
            out_specs=pl.BlockSpec((1, n_chunks, units * n_rows, LANES), lambda d, place_ref: (d, 0, 0, 0)),
            scratch_shapes=[] if units >= n_chan else [pltpu.VMEM((n_chunks, n_chan * n_rows, LANES), F32)],
        ),
        out_shape=jax.ShapeDtypeStruct((n_dev, n_chunks, units * n_rows, LANES), F32),
        cost_estimate=pl.CostEstimate(flops=10**9, bytes_accessed=16 * rows * units * n_chunks * n_dev, transcendentals=0),
        compiler_params=pltpu.CompilerParams(dimension_semantics=("arbitrary",)),
        name="turn_share",
    )(place, filt_one, filt_two)


def project_body(n_chunks, flag_ref, u_ref, halo_ref, *refs):
    w_refs, b_refs, tap_refs = refs[:3], refs[3:6], refs[6:9]
    sent_ref, gate_ref, p_ref = refs[9:]
    rows = u_ref.shape[0]
    n_rows = rows // LANES
    width = w_refs[0].shape[1]
    per_chunk = LANES // n_chunks
    for which in range(3):
        w = w_refs[which][...]
        bias = b_refs[which][...]
        halo = (dot32(halo_ref[...].astype(BF16), w) + bias).astype(BF16).astype(F32)
        p_ref[0:8, :] = jnp.where(flag_ref[0] > 0, halo, 0.0)
        step = 2 * LANES

        @pl.loop(0, rows // step)
        def _(i):
            start = pl.multiple_of(i * step, step)
            proj = dot32(u_ref[pl.ds(start, step), :], w) + bias
            p_ref[pl.ds(start + 8, step), :] = proj.astype(BF16).astype(F32)

        c0, c1, c2 = (tap_refs[which][t : t + 1, :] for t in range(3))

        @pl.loop(0, n_rows)
        def _(r):
            start = pl.multiple_of(r * LANES, LANES)
            window = p_ref[pl.ds(start, LANES + 8), :]
            mixed = c0 * window[8:] + c1 * window[7:-1] + c2 * window[6:-2]
            mixed = mixed.astype(BF16)
            if which == 1:
                gate_ref[pl.ds(start, LANES), :] = mixed
            else:
                slot = 1 if which == 0 else 0
                for d in range(width // LANES):
                    turned = mixed[:, d * LANES : (d + 1) * LANES].astype(F32).T
                    for k in range(n_chunks):
                        sent_ref[k, d, slot, pl.ds(r, per_chunk, stride=n_rows), :] = turned[k * per_chunk : (k + 1) * per_chunk]


def project(has_prev, u, halo, w_in, b_in, taps, n_dev, n_chunks):
    rows, depth = u.shape
    model = w_in.shape[1] // 3
    width = 2 * LANES
    steps = model // width
    n_rows = rows // LANES
    per_chunk = LANES // n_chunks
    chunk_rows = per_chunk * n_rows
    w_specs = [pl.BlockSpec((depth, width), functools.partial(lambda off, j: (0, off + j), t * steps)) for t in range(3)]
    b_specs = [pl.BlockSpec((1, width), functools.partial(lambda off, j: (0, off + j), t * steps)) for t in range(3)]
    t_specs = [pl.BlockSpec((3, width), functools.partial(lambda off, j: (0, off + j), t * steps)) for t in range(3)]
    return pl.pallas_call(
        functools.partial(project_body, n_chunks),
        grid=(steps,),
        in_specs=[
            pl.BlockSpec(memory_space=pltpu.SMEM),
            pl.BlockSpec((rows, depth), lambda j: (0, 0)),
            pl.BlockSpec((8, depth), lambda j: (0, 0)),
            *w_specs,
            *b_specs,
            *t_specs,
        ],
        out_specs=[
            pl.BlockSpec((n_chunks, 2, 2, chunk_rows, LANES), lambda j: (0, j, 0, 0, 0)),
            pl.BlockSpec((rows, width), lambda j: (0, j)),
        ],
        out_shape=[
            jax.ShapeDtypeStruct((n_chunks, n_dev, 2, chunk_rows, LANES), F32),
            jax.ShapeDtypeStruct((rows, model), BF16),
        ],
        scratch_shapes=[pltpu.VMEM((rows + 8, width), F32)],
        cost_estimate=pl.CostEstimate(flops=2 * rows * depth * 3 * model, bytes_accessed=30 * 2**20, transcendentals=0),
        compiler_params=pltpu.CompilerParams(dimension_semantics=("arbitrary",), vmem_limit_bytes=60 * 2**20),
        name="project",
    )(has_prev, u, halo, w_in, w_in, w_in, b_in, b_in, b_in, taps, taps, taps)


def spectrum_tools(group, n_high, tables, parts_ref):
    wide_ref, thin_ref, fwd_ref, inv_ref, last_ref, twist_ref = tables
    wide = 2 * LANES
    scale = 1.0 / (n_high * LANES)

    def complex_dot(tab_ref):
        return (
            dot32(parts_ref[:, 2 * wide :], tab_ref[:wide])
            + dot32(parts_ref[:, wide : 2 * wide], tab_ref[:wide])
            + dot32(parts_ref[:, :wide], tab_ref[wide : 2 * wide])
            + dot32(parts_ref[:, wide : 2 * wide], tab_ref[wide : 2 * wide])
            + dot32(parts_ref[:, :wide], tab_ref[2 * wide :])
            + dot32(parts_ref[:, :wide], tab_ref[:wide])
        )

    def store_parts(g, real, imag):
        for t, (re, im) in enumerate(zip(split3(real), split3(imag))):
            parts_ref[g * n_high : (g + 1) * n_high, 2 * t * LANES : (2 * t + 1) * LANES] = re
            parts_ref[g * n_high : (g + 1) * n_high, (2 * t + 1) * LANES : (2 * t + 2) * LANES] = im

    def spectrum(signals, exact):
        tr, ti = twist_ref[0], twist_ref[1]
        for g in range(0, group, 2):
            pair = jnp.concatenate([signals[g], signals[g + 1]], axis=1)
            if exact:
                short = pair.astype(BF16)
                coarse = dot32(thin_ref[...], jnp.concatenate([short, short, short], axis=0))
            else:
                hi, mid, low = split3(pair)
                coarse = dot32(wide_ref[...], jnp.concatenate([hi, mid, low, hi, mid, hi], axis=0))
            for j in range(2):
                re = coarse[:n_high, j * LANES : (j + 1) * LANES]
                im = coarse[n_high:, j * LANES : (j + 1) * LANES]
                store_parts(g + j, re * tr - im * ti, re * ti + im * tr)
        return complex_dot(fwd_ref)

    def signal(spec_a, spec_b):
        tr, ti = twist_ref[0], twist_ref[1]
        for g in range(group):
            rows = slice(g * n_high, (g + 1) * n_high)
            ar, ai = spec_a[rows, :LANES], spec_a[rows, LANES:]
            br, bi = spec_b[rows, :LANES], spec_b[rows, LANES:]
            store_parts(g, ar * br - ai * bi, ar * bi + ai * br)
        fine = complex_dot(inv_ref)
        results = []
        for g in range(0, group, 2):
            halves = []
            for j in range(2):
                rows = slice((g + j) * n_high, (g + j + 1) * n_high)
                re, im = fine[rows, :LANES] * scale, fine[rows, LANES:] * scale
                halves.append(jnp.concatenate([re * tr + im * ti, im * tr - re * ti], axis=0))
            hi, mid, low = split3(jnp.concatenate(halves, axis=1))
            d_hi = dot32(last_ref[...], hi)
            d_mid = dot32(last_ref[: 2 * n_high], mid)
            d_low = dot32(last_ref[:n_high], low)
            small = d_hi[2 * n_high :] + d_mid[n_high:] + d_low
            total = d_hi[:n_high] + ((d_hi[n_high : 2 * n_high] + d_mid[:n_high]) + small)
            results += [total[:, :LANES], total[:, LANES:]]
        return results

    return spectrum, signal


def exchange_body(n_dev, n_groups, group, skip_ref, share_ref, sent_ref, wide_ref, thin_ref, fwd_ref, inv_ref, last_ref, twist_ref, back_ref, got_ref, filt_ref, done_ref, parts_ref, spec_one_ref, spec_two_ref, sent_sem, got_sem, share_sem, filt_sem, back_sem, done_sem):
    n_chunks, _, _, chunk_rows, _ = sent_ref.shape
    n_high = twist_ref.shape[1]
    per_src = n_high // n_dev
    n_chan = chunk_rows // per_src
    me, my_group = lax.axis_index("sp"), lax.axis_index("dp")
    share_rows = share_ref.shape[2]
    spectrum, signal = spectrum_tools(group, n_high, (wide_ref, thin_ref, fwd_ref, inv_ref, last_ref, twist_ref), parts_ref)

    barrier = pltpu.get_barrier_semaphore()
    for off in range(1, n_dev):
        pl.semaphore_signal(barrier, inc=1, device_id={"sp": lax.rem(me + off, n_dev)}, device_id_type=pl.DeviceIdType.MESH)
    for off in range(1, n_groups):
        pl.semaphore_signal(barrier, inc=1, device_id={"dp": lax.rem(my_group + off, n_groups)}, device_id_type=pl.DeviceIdType.MESH)
    pl.semaphore_wait(barrier, n_dev + n_groups - 2)

    def sharing(k, off):
        return pltpu.make_async_remote_copy(
            src_ref=share_ref.at[:, k],
            dst_ref=share_of(k),
            send_sem=share_sem.at[k],
            recv_sem=filt_sem.at[k],
            device_id={"dp": lax.rem(my_group + off, n_groups)},
            device_id_type=pl.DeviceIdType.MESH,
        )

    def share_of(k):
        return filt_ref.at[k, :, pl.ds(pl.multiple_of(my_group * share_rows, share_rows), share_rows), :]

    def own_share(k):
        return pltpu.make_async_copy(share_ref.at[:, k], share_of(k), filt_sem.at[k])

    def all_shares(k):
        return pltpu.make_async_copy(filt_ref.at[k], filt_ref.at[k], filt_sem.at[k])

    def sending(k, off):
        dest = lax.rem(me + off, n_dev)
        return pltpu.make_async_remote_copy(
            src_ref=sent_ref.at[k, dest],
            dst_ref=got_ref.at[k, me],
            send_sem=sent_sem.at[k, off],
            recv_sem=got_sem.at[k, off],
            device_id={"sp": dest},
            device_id_type=pl.DeviceIdType.MESH,
        )

    def keeping(k):
        return pltpu.make_async_copy(sent_ref.at[k, me], got_ref.at[k, me], got_sem.at[k, 0])

    block = per_src * n_chan

    def part_of(slot, dest):
        return done_ref.at[slot, pl.ds(pl.multiple_of(dest * block, block), block), :]

    def returning(k, slot, off):
        dest = lax.rem(me + off, n_dev)
        return pltpu.make_async_remote_copy(
            src_ref=part_of(slot, dest),
            dst_ref=back_ref.at[k, me],
            send_sem=done_sem.at[slot, off],
            recv_sem=back_sem.at[k, off],
            device_id={"sp": dest},
            device_id_type=pl.DeviceIdType.MESH,
        )

    def storing(k, slot):
        return pltpu.make_async_copy(part_of(slot, me), back_ref.at[k, me], done_sem.at[slot, 0])

    @pl.loop(0, n_chunks)
    def _(k):
        own_share(k).start()
        keeping(k).start()
        for off in range(1, n_groups):
            sharing(k, off).start()
        for off in range(1, n_dev):
            sending(k, off).start()

    @pl.loop(0, n_chunks)
    def _(k):
        slot = lax.rem(k, 2)
        all_shares(k).wait()
        keeping(k).wait()
        for off in range(1, n_dev):
            sending(k, off).wait_recv()

        @pl.when(k >= 2)
        def _():
            storing(k - 2, slot).wait()
            for off in range(1, n_dev):
                returning(k - 2, slot, off).wait_send()

        @pl.loop(0, n_chan // group)
        def _(i):
            first = i * group

            def load_h(which, g):
                start = pl.multiple_of((which * n_chan + first + g) * per_src, per_src)
                return filt_ref[k, :, pl.ds(start, per_src), :].reshape(n_high, LANES)

            def load_x(which, g):
                start = pl.multiple_of((first + g) * per_src, per_src)
                return got_ref[k, :, which, pl.ds(start, per_src), :].reshape(n_high, LANES)

            chan = k * n_chan + first
            spec_one_ref[...] = spectrum([load_h(0, g) for g in range(group)], False)
            spec_two_ref[...] = spectrum([load_h(1, g) for g in range(group)], False)
            values = [load_x(0, g) for g in range(group)]
            conv = signal(spectrum(values, True), spec_one_ref)
            gated = [load_x(1, g) * (conv[g] + skip_ref[0, chan + g] * values[g]) for g in range(group)]
            conv = signal(spectrum(gated, False), spec_two_ref)
            for g in range(group):
                done_ref[slot, pl.ds(first + g, n_high, stride=n_chan), :] = conv[g] + skip_ref[1, chan + g] * gated[g]

        storing(k, slot).start()
        for off in range(1, n_dev):
            returning(k, slot, off).start()

    for k in range(max(0, n_chunks - 2), n_chunks):
        storing(k, k % 2).wait()
        for off in range(1, n_dev):
            returning(k, k % 2, off).wait_send()

    @pl.loop(0, n_chunks)
    def _(k):
        for off in range(1, n_dev):
            sending(k, off).wait_send()
            returning(k, 0, off).wait_recv()
        for off in range(1, n_groups):
            sharing(k, off).wait_send()


def exchange(skips, share, sent, tables, n_dev, n_groups, group=4):
    n_chunks, _, _, chunk_rows, _ = sent.shape
    n_high = tables[-1].shape[1]
    n_chan = chunk_rows // (n_high // n_dev)
    any_spec = pl.BlockSpec(memory_space=pl.ANY)
    vmem_spec = pl.BlockSpec(memory_space=pltpu.VMEM)
    return pl.pallas_call(
        functools.partial(exchange_body, n_dev, n_groups, group),
        in_specs=[pl.BlockSpec(memory_space=pltpu.SMEM), any_spec, any_spec] + [vmem_spec] * len(tables),
        out_specs=any_spec,
        out_shape=jax.ShapeDtypeStruct((n_chunks, n_dev, chunk_rows, LANES), F32),
        scratch_shapes=[
            pltpu.VMEM((n_chunks, n_dev, 2, chunk_rows, LANES), F32),
            pltpu.VMEM((n_chunks, n_dev, 2 * chunk_rows, LANES), F32),
            pltpu.VMEM((2, n_high * n_chan, LANES), F32),
            pltpu.VMEM((group * n_high, 6 * LANES), BF16),
            pltpu.VMEM((group * n_high, 2 * LANES), F32),
            pltpu.VMEM((group * n_high, 2 * LANES), F32),
            pltpu.SemaphoreType.DMA((n_chunks, n_dev)),
            pltpu.SemaphoreType.DMA((n_chunks, n_dev)),
            pltpu.SemaphoreType.DMA((n_chunks,)),
            pltpu.SemaphoreType.DMA((n_chunks,)),
            pltpu.SemaphoreType.DMA((n_chunks, n_dev)),
            pltpu.SemaphoreType.DMA((2, n_dev)),
        ],
        cost_estimate=pl.CostEstimate(flops=10**11, bytes_accessed=40 * 2**20, transcendentals=0),
        compiler_params=pltpu.CompilerParams(collective_id=0, has_side_effects=True, vmem_limit_bytes=60 * 2**20),
        name="exchange",
    )(skips, share, sent, *tables)


def finish_body(gate_ref, u_ref, w_ref, back_ref, out_ref, y_ref):
    n_chunks, n_src, n_rows, _, _ = back_ref.shape
    for r in range(n_rows):
        for s in range(n_src):
            full = jnp.concatenate([back_ref[k, s, r] for k in range(n_chunks)], axis=0)
            rows, cols = slice(r * LANES, (r + 1) * LANES), slice(s * LANES, (s + 1) * LANES)
            y_ref[rows, cols] = (gate_ref[rows, cols].astype(F32) * full.T).astype(BF16)
    out_ref[...] = (u_ref[...].astype(F32) + dot32(y_ref[...], w_ref[...])).astype(BF16)


def finish(gate, u, w_out, back, n_rows=2):
    rows, model = u.shape
    n_chunks, n_src, _, per_chunk, _ = back.shape
    tile = n_rows * LANES
    return pl.pallas_call(
        finish_body,
        grid=(rows // tile,),
        in_specs=[
            pl.BlockSpec((tile, model), lambda i: (i, 0)),
            pl.BlockSpec((tile, model), lambda i: (i, 0)),
            pl.BlockSpec(w_out.shape, lambda i: (0, 0)),
            pl.BlockSpec((n_chunks, n_src, n_rows, per_chunk, LANES), lambda i: (0, 0, i, 0, 0)),
        ],
        out_specs=pl.BlockSpec((tile, model), lambda i: (i, 0)),
        out_shape=jax.ShapeDtypeStruct((rows, model), BF16),
        scratch_shapes=[pltpu.VMEM((tile, model), BF16)],
        cost_estimate=pl.CostEstimate(flops=2 * rows * model * model, bytes_accessed=20 * 2**20, transcendentals=0),
        compiler_params=pltpu.CompilerParams(dimension_semantics=("arbitrary",), vmem_limit_bytes=48 * 2**20),
        name="finish",
    )(gate, u, w_out, back)


def solution(mesh):
    n_dev, n_groups = mesh.shape["sp"], mesh.shape["dp"]
    n_chunks = 8
    n_chan = LANES // n_chunks
    if (2 * n_chan) % n_groups:
        raise ValueError("uneven groups")
    units = 2 * n_chan // n_groups
    halo_perm = list(zip(range(n_dev - 1), range(1, n_dev)))

    def local_step(u_in, w_in, b_in, conv_taps, w_out, skip_one, skip_two, filt_one, filt_two):
        rank = lax.axis_index("sp")
        u = u_in[0]
        rows = u.shape[0]
        tables = [jnp.asarray(t) for t in transform_tables(rows * n_dev)]

        halo = lax.ppermute(u[-8:].astype(F32), "sp", halo_perm)
        has_prev = (rank > 0).astype(jnp.int32)[None]
        first_unit = lax.axis_index("dp") * units
        place = jnp.stack([first_unit // n_chan, first_unit % n_chan])
        share = turn_share(place, filt_one, filt_two, n_dev, n_chunks, units)
        share, halo = lax.optimization_barrier((share, halo))
        share = lax.all_to_all(share, "sp", 0, 0, tiled=True)
        sent, gate = project(has_prev, u, halo, w_in, b_in[None], conv_taps, n_dev, n_chunks)
        skips = lax.dynamic_slice_in_dim(jnp.stack([skip_one, skip_two]), rank * LANES, LANES, axis=1)
        back = exchange(skips, share, sent, tables, n_dev, n_groups)
        back = back.reshape(n_chunks, n_dev, rows // LANES, LANES // n_chunks, LANES)
        return finish(gate, u, w_out, back)[None]

    seq_spec = P("dp", "sp", None)
    filt_spec = P("sp", None)
    return jax.shard_map(
        local_step,
        mesh=mesh,
        in_specs=(seq_spec, P(), P(), P(), P(), P(), P(), filt_spec, filt_spec),
        out_specs=seq_spec,
        check_vma=False,
    )
```

```python
import functools
import jax
import jax.numpy as jnp
import numpy as np
from jax import lax
from jax.experimental import pallas as pl
from jax.experimental.pallas import tpu as pltpu
from jax.sharding import PartitionSpec as P

LANES = 128
F32 = jnp.float32
BF16 = jnp.bfloat16


def split_table(table, n_parts=3):
    parts, rest = [], np.asarray(table, np.float64)
    for _ in range(n_parts):
        part = rest.astype(jnp.bfloat16)
        parts.append(part)
        rest = rest - part.astype(np.float64)
    return parts


def transform_tables(seq_len):
    n_high = seq_len // LANES
    quarter = np.arange(n_high)[:, None] + 0.25
    high = 2.0 * np.pi * quarter * np.arange(n_high)[None, :] / n_high
    twist = 2.0 * np.pi * quarter * np.arange(LANES)[None, :] / seq_len
    low = 2.0 * np.pi * np.outer(np.arange(LANES), np.arange(LANES)) / LANES
    first = np.concatenate([np.cos(high), -np.sin(high)], axis=0)
    last = np.concatenate([np.cos(high.T), -np.sin(high.T)], axis=1)
    er, ei = np.cos(low), -np.sin(low)
    fwd = np.block([[er, ei], [-ei, er]])
    inv = np.block([[er, -ei], [ei, er]])
    a, b, c = split_table(first)
    first_wide = np.concatenate([a, a, a, b, b, c], axis=1)
    first_thin = np.concatenate([a, b, c], axis=1)
    fwd_parts = np.concatenate(split_table(fwd), axis=0)
    inv_parts = np.concatenate(split_table(inv), axis=0)
    last_parts = np.concatenate(split_table(last), axis=0)
    twist_tab = np.stack([np.cos(twist), -np.sin(twist)]).astype(np.float32)
    return first_wide, first_thin, fwd_parts, inv_parts, last_parts, twist_tab


def split3(x):
    hi = x.astype(BF16)
    rest = x - hi.astype(F32)
    mid = rest.astype(BF16)
    low = (rest - mid.astype(F32)).astype(BF16)
    return hi, mid, low


def dot32(a, b):
    return jnp.dot(a, b, preferred_element_type=F32)


def turn_share_body(n_chunks, units, place_ref, one_ref, two_ref, out_ref, *scratch):
    n_rows = one_ref.shape[0] // LANES
    n_chan = LANES // n_chunks

    def turn(ref, into_ref, base):
        @pl.loop(0, n_rows)
        def _(r):
            block = ref[pl.ds(pl.multiple_of(r * LANES, LANES), LANES), :].T
            for k in range(n_chunks):
                into_ref[k, pl.ds(base + r, n_chan, stride=n_rows), :] = block[k * n_chan : (k + 1) * n_chan]

    if units == 2 * n_chan:
        turn(one_ref, out_ref.at[0], 0)
        turn(two_ref, out_ref.at[0], n_chan * n_rows)
    else:
        into_ref = out_ref.at[0] if units == n_chan else scratch[0]
        for which, ref in enumerate((one_ref, two_ref)):

            @pl.when(place_ref[0] == which)
            def _():
                turn(ref, into_ref, 0)

        if units < n_chan:
            start = pl.multiple_of(place_ref[1] * n_rows, n_rows)
            out_ref[0] = scratch[0][:, pl.ds(start, units * n_rows), :]


def turn_share(place, filt_one, filt_two, n_dev, n_chunks, units):
    rows = filt_one.shape[0]
    n_rows = rows // LANES
    n_chan = LANES // n_chunks
    both = units == 2 * n_chan

    def pick(which):
        def index(d, place_ref):
            return 0, (d if both else jnp.where(place_ref[0] == which, d, 0))

        return pl.BlockSpec((rows, LANES), index)

    return pl.pallas_call(
        functools.partial(turn_share_body, n_chunks, units),
        grid_spec=pltpu.PrefetchScalarGridSpec(
            num_scalar_prefetch=1,
            grid=(n_dev,),
            in_specs=[pick(0), pick(1)],
            out_specs=pl.BlockSpec((1, n_chunks, units * n_rows, LANES), lambda d, place_ref: (d, 0, 0, 0)),
            scratch_shapes=[] if units >= n_chan else [pltpu.VMEM((n_chunks, n_chan * n_rows, LANES), F32)],
        ),
        out_shape=jax.ShapeDtypeStruct((n_dev, n_chunks, units * n_rows, LANES), F32),
        cost_estimate=pl.CostEstimate(flops=10**9, bytes_accessed=16 * rows * units * n_chunks * n_dev, transcendentals=0),
        compiler_params=pltpu.CompilerParams(dimension_semantics=("arbitrary",)),
        name="turn_share",
    )(place, filt_one, filt_two)


def project_body(n_chunks, flag_ref, u_ref, halo_ref, *refs):
    w_refs, b_refs, tap_refs = refs[:3], refs[3:6], refs[6:9]
    sent_ref, gate_ref, p_ref = refs[9:]
    rows = u_ref.shape[0]
    n_rows = rows // LANES
    width = w_refs[0].shape[1]
    per_chunk = LANES // n_chunks
    for which in range(3):
        w = w_refs[which][...]
        bias = b_refs[which][...]
        halo = (dot32(halo_ref[...].astype(BF16), w) + bias).astype(BF16).astype(F32)
        p_ref[0:8, :] = jnp.where(flag_ref[0] > 0, halo, 0.0)
        step = 2 * LANES

        @pl.loop(0, rows // step)
        def _(i):
            start = pl.multiple_of(i * step, step)
            proj = dot32(u_ref[pl.ds(start, step), :], w) + bias
            p_ref[pl.ds(start + 8, step), :] = proj.astype(BF16).astype(F32)

        c0, c1, c2 = (tap_refs[which][t : t + 1, :] for t in range(3))

        @pl.loop(0, n_rows)
        def _(r):
            start = pl.multiple_of(r * LANES, LANES)
            window = p_ref[pl.ds(start, LANES + 8), :]
            mixed = c0 * window[8:] + c1 * window[7:-1] + c2 * window[6:-2]
            mixed = mixed.astype(BF16)
            if which == 1:
                gate_ref[pl.ds(start, LANES), :] = mixed
            else:
                slot = 1 if which == 0 else 0
                for d in range(width // LANES):
                    turned = mixed[:, d * LANES : (d + 1) * LANES].astype(F32).T
                    for k in range(n_chunks):
                        sent_ref[k, d, slot, pl.ds(r, per_chunk, stride=n_rows), :] = turned[k * per_chunk : (k + 1) * per_chunk]


def project(has_prev, u, halo, w_in, b_in, taps, n_dev, n_chunks):
    rows, depth = u.shape
    model = w_in.shape[1] // 3
    width = 2 * LANES
    steps = model // width
    n_rows = rows // LANES
    per_chunk = LANES // n_chunks
    chunk_rows = per_chunk * n_rows
    w_specs = [pl.BlockSpec((depth, width), functools.partial(lambda off, j: (0, off + j), t * steps)) for t in range(3)]
    b_specs = [pl.BlockSpec((1, width), functools.partial(lambda off, j: (0, off + j), t * steps)) for t in range(3)]
    t_specs = [pl.BlockSpec((3, width), functools.partial(lambda off, j: (0, off + j), t * steps)) for t in range(3)]
    return pl.pallas_call(
        functools.partial(project_body, n_chunks),
        grid=(steps,),
        in_specs=[
            pl.BlockSpec(memory_space=pltpu.SMEM),
            pl.BlockSpec((rows, depth), lambda j: (0, 0)),
            pl.BlockSpec((8, depth), lambda j: (0, 0)),
            *w_specs,
            *b_specs,
            *t_specs,
        ],
        out_specs=[
            pl.BlockSpec((n_chunks, 2, 2, chunk_rows, LANES), lambda j: (0, j, 0, 0, 0)),
            pl.BlockSpec((rows, width), lambda j: (0, j)),
        ],
        out_shape=[
            jax.ShapeDtypeStruct((n_chunks, n_dev, 2, chunk_rows, LANES), F32),
            jax.ShapeDtypeStruct((rows, model), BF16),
        ],
        scratch_shapes=[pltpu.VMEM((rows + 8, width), F32)],
        cost_estimate=pl.CostEstimate(flops=2 * rows * depth * 3 * model, bytes_accessed=30 * 2**20, transcendentals=0),
        compiler_params=pltpu.CompilerParams(dimension_semantics=("arbitrary",), vmem_limit_bytes=60 * 2**20),
        name="project",
    )(has_prev, u, halo, w_in, w_in, w_in, b_in, b_in, b_in, taps, taps, taps)


def spectrum_tools(group, n_high, tables, parts_ref):
    wide_ref, thin_ref, fwd_ref, inv_ref, last_ref, twist_ref = tables
    wide = 2 * LANES
    scale = 1.0 / (n_high * LANES)

    def complex_dot(tab_ref):
        return (
            dot32(parts_ref[:, 2 * wide :], tab_ref[:wide])
            + dot32(parts_ref[:, wide : 2 * wide], tab_ref[:wide])
            + dot32(parts_ref[:, :wide], tab_ref[wide : 2 * wide])
            + dot32(parts_ref[:, wide : 2 * wide], tab_ref[wide : 2 * wide])
            + dot32(parts_ref[:, :wide], tab_ref[2 * wide :])
            + dot32(parts_ref[:, :wide], tab_ref[:wide])
        )

    def store_parts(g, real, imag):
        for t, (re, im) in enumerate(zip(split3(real), split3(imag))):
            parts_ref[g * n_high : (g + 1) * n_high, 2 * t * LANES : (2 * t + 1) * LANES] = re
            parts_ref[g * n_high : (g + 1) * n_high, (2 * t + 1) * LANES : (2 * t + 2) * LANES] = im

    def spectrum(signals, exact):
        tr, ti = twist_ref[0], twist_ref[1]
        for g in range(0, group, 2):
            pair = jnp.concatenate([signals[g], signals[g + 1]], axis=1)
            if exact:
                short = pair.astype(BF16)
                coarse = dot32(thin_ref[...], jnp.concatenate([short, short, short], axis=0))
            else:
                hi, mid, low = split3(pair)
                coarse = dot32(wide_ref[...], jnp.concatenate([hi, mid, low, hi, mid, hi], axis=0))
            for j in range(2):
                re = coarse[:n_high, j * LANES : (j + 1) * LANES]
                im = coarse[n_high:, j * LANES : (j + 1) * LANES]
                store_parts(g + j, re * tr - im * ti, re * ti + im * tr)
        return complex_dot(fwd_ref)

    def signal(spec_a, spec_b):
        tr, ti = twist_ref[0], twist_ref[1]
        for g in range(group):
            rows = slice(g * n_high, (g + 1) * n_high)
            ar, ai = spec_a[rows, :LANES], spec_a[rows, LANES:]
            br, bi = spec_b[rows, :LANES], spec_b[rows, LANES:]
            store_parts(g, ar * br - ai * bi, ar * bi + ai * br)
        fine = complex_dot(inv_ref)
        results = []
        for g in range(0, group, 2):
            halves = []
            for j in range(2):
                rows = slice((g + j) * n_high, (g + j + 1) * n_high)
                re, im = fine[rows, :LANES] * scale, fine[rows, LANES:] * scale
                halves.append(jnp.concatenate([re * tr + im * ti, im * tr - re * ti], axis=0))
            hi, mid, low = split3(jnp.concatenate(halves, axis=1))
            d_hi = dot32(last_ref[...], hi)
            d_mid = dot32(last_ref[: 2 * n_high], mid)
            d_low = dot32(last_ref[:n_high], low)
            small = d_hi[2 * n_high :] + d_mid[n_high:] + d_low
            total = d_hi[:n_high] + ((d_hi[n_high : 2 * n_high] + d_mid[:n_high]) + small)
            results += [total[:, :LANES], total[:, LANES:]]
        return results

    return spectrum, signal


def exchange_body(n_dev, n_groups, group, skip_ref, share_ref, sent_ref, wide_ref, thin_ref, fwd_ref, inv_ref, last_ref, twist_ref, back_ref, got_ref, filt_ref, done_ref, parts_ref, spec_one_ref, spec_two_ref, sent_sem, got_sem, share_sem, filt_sem, back_sem, done_sem):
    n_chunks, _, _, chunk_rows, _ = sent_ref.shape
    n_high = twist_ref.shape[1]
    per_src = n_high // n_dev
    n_chan = chunk_rows // per_src
    me, my_group = lax.axis_index("sp"), lax.axis_index("dp")
    share_rows = share_ref.shape[2]
    spectrum, signal = spectrum_tools(group, n_high, (wide_ref, thin_ref, fwd_ref, inv_ref, last_ref, twist_ref), parts_ref)

    barrier = pltpu.get_barrier_semaphore()
    for off in range(1, n_dev):
        pl.semaphore_signal(barrier, inc=1, device_id={"sp": lax.rem(me + off, n_dev)}, device_id_type=pl.DeviceIdType.MESH)
    for off in range(1, n_groups):
        pl.semaphore_signal(barrier, inc=1, device_id={"dp": lax.rem(my_group + off, n_groups)}, device_id_type=pl.DeviceIdType.MESH)
    pl.semaphore_wait(barrier, n_dev + n_groups - 2)

    def sharing(k, off):
        return pltpu.make_async_remote_copy(
            src_ref=share_ref.at[:, k],
            dst_ref=share_of(k),
            send_sem=share_sem.at[k],
            recv_sem=filt_sem.at[k],
            device_id={"dp": lax.rem(my_group + off, n_groups)},
            device_id_type=pl.DeviceIdType.MESH,
        )

    def share_of(k):
        return filt_ref.at[k, :, pl.ds(pl.multiple_of(my_group * share_rows, share_rows), share_rows), :]

    def own_share(k):
        return pltpu.make_async_copy(share_ref.at[:, k], share_of(k), filt_sem.at[k])

    def all_shares(k):
        return pltpu.make_async_copy(filt_ref.at[k], filt_ref.at[k], filt_sem.at[k])

    def sending(k, off):
        dest = lax.rem(me + off, n_dev)
        return pltpu.make_async_remote_copy(
            src_ref=sent_ref.at[k, dest],
            dst_ref=got_ref.at[k, me],
            send_sem=sent_sem.at[k, off],
            recv_sem=got_sem.at[k, off],
            device_id={"sp": dest},
            device_id_type=pl.DeviceIdType.MESH,
        )

    def keeping(k):
        return pltpu.make_async_copy(sent_ref.at[k, me], got_ref.at[k, me], got_sem.at[k, 0])

    block = per_src * n_chan

    def part_of(k, dest):
        return done_ref.at[k, pl.ds(pl.multiple_of(dest * block, block), block), :]

    def returning(k, off):
        dest = lax.rem(me + off, n_dev)
        return pltpu.make_async_remote_copy(
            src_ref=part_of(k, dest),
            dst_ref=back_ref.at[k, me],
            send_sem=done_sem.at[k, off],
            recv_sem=back_sem.at[k, off],
            device_id={"sp": dest},
            device_id_type=pl.DeviceIdType.MESH,
        )

    def storing(k):
        return pltpu.make_async_copy(part_of(k, me), back_ref.at[k, me], done_sem.at[k, 0])

    @pl.loop(0, n_chunks)
    def _(k):
        own_share(k).start()
        keeping(k).start()
        for off in range(1, n_groups):
            sharing(k, off).start()
        for off in range(1, n_dev):
            sending(k, off).start()

    @pl.loop(0, n_chunks)
    def _(k):
        all_shares(k).wait()
        keeping(k).wait()
        for off in range(1, n_dev):
            sending(k, off).wait_recv()

        @pl.loop(0, n_chan // group)
        def _(i):
            first = i * group

            def load_h(which, g):
                start = pl.multiple_of((which * n_chan + first + g) * per_src, per_src)
                return filt_ref[k, :, pl.ds(start, per_src), :].reshape(n_high, LANES)

            def load_x(which, g):
                start = pl.multiple_of((first + g) * per_src, per_src)
                return got_ref[k, :, which, pl.ds(start, per_src), :].reshape(n_high, LANES)

            chan = k * n_chan + first
            spec_one_ref[...] = spectrum([load_h(0, g) for g in range(group)], False)
            spec_two_ref[...] = spectrum([load_h(1, g) for g in range(group)], False)
            values = [load_x(0, g) for g in range(group)]
            conv = signal(spectrum(values, True), spec_one_ref)
            gated = [load_x(1, g) * (conv[g] + skip_ref[0, chan + g] * values[g]) for g in range(group)]
            conv = signal(spectrum(gated, False), spec_two_ref)
            for g in range(group):
                done_ref[k, pl.ds(first + g, n_high, stride=n_chan), :] = conv[g] + skip_ref[1, chan + g] * gated[g]

        storing(k).start()
        for off in range(1, n_dev):
            returning(k, off).start()

    @pl.loop(0, n_chunks)
    def _(k):
        for off in range(1, n_dev):
            sending(k, off).wait_send()
            returning(k, off).wait()
        storing(k).wait()
        for off in range(1, n_groups):
            sharing(k, off).wait_send()


def exchange(skips, share, sent, tables, n_dev, n_groups, group=4):
    n_chunks, _, _, chunk_rows, _ = sent.shape
    n_high = tables[-1].shape[1]
    n_chan = chunk_rows // (n_high // n_dev)
    any_spec = pl.BlockSpec(memory_space=pl.ANY)
    vmem_spec = pl.BlockSpec(memory_space=pltpu.VMEM)
    return pl.pallas_call(
        functools.partial(exchange_body, n_dev, n_groups, group),
        in_specs=[pl.BlockSpec(memory_space=pltpu.SMEM), any_spec, any_spec] + [vmem_spec] * len(tables),
        out_specs=any_spec,
        out_shape=jax.ShapeDtypeStruct((n_chunks, n_dev, chunk_rows, LANES), F32),
        scratch_shapes=[
            pltpu.VMEM((n_chunks, n_dev, 2, chunk_rows, LANES), F32),
            pltpu.VMEM((n_chunks, n_dev, 2 * chunk_rows, LANES), F32),
            pltpu.VMEM((n_chunks, n_high * n_chan, LANES), F32),
            pltpu.VMEM((group * n_high, 6 * LANES), BF16),
            pltpu.VMEM((group * n_high, 2 * LANES), F32),
            pltpu.VMEM((group * n_high, 2 * LANES), F32),
            pltpu.SemaphoreType.DMA((n_chunks, n_dev)),
            pltpu.SemaphoreType.DMA((n_chunks, n_dev)),
            pltpu.SemaphoreType.DMA((n_chunks,)),
            pltpu.SemaphoreType.DMA((n_chunks,)),
            pltpu.SemaphoreType.DMA((n_chunks, n_dev)),
            pltpu.SemaphoreType.DMA((n_chunks, n_dev)),
        ],
        cost_estimate=pl.CostEstimate(flops=10**11, bytes_accessed=40 * 2**20, transcendentals=0),
        compiler_params=pltpu.CompilerParams(collective_id=0, has_side_effects=True, vmem_limit_bytes=60 * 2**20),
        name="exchange",
    )(skips, share, sent, *tables)


def finish_body(gate_ref, u_ref, w_ref, back_ref, out_ref, y_ref):
    n_chunks, n_src, n_rows, _, _ = back_ref.shape
    for r in range(n_rows):
        for s in range(n_src):
            full = jnp.concatenate([back_ref[k, s, r] for k in range(n_chunks)], axis=0)
            rows, cols = slice(r * LANES, (r + 1) * LANES), slice(s * LANES, (s + 1) * LANES)
            y_ref[rows, cols] = (gate_ref[rows, cols].astype(F32) * full.T).astype(BF16)
    out_ref[...] = (u_ref[...].astype(F32) + dot32(y_ref[...], w_ref[...])).astype(BF16)


def finish(gate, u, w_out, back, n_rows=2):
    rows, model = u.shape
    n_chunks, n_src, _, per_chunk, _ = back.shape
    tile = n_rows * LANES
    return pl.pallas_call(
        finish_body,
        grid=(rows // tile,),
        in_specs=[
            pl.BlockSpec((tile, model), lambda i: (i, 0)),
            pl.BlockSpec((tile, model), lambda i: (i, 0)),
            pl.BlockSpec(w_out.shape, lambda i: (0, 0)),
            pl.BlockSpec((n_chunks, n_src, n_rows, per_chunk, LANES), lambda i: (0, 0, i, 0, 0)),
        ],
        out_specs=pl.BlockSpec((tile, model), lambda i: (i, 0)),
        out_shape=jax.ShapeDtypeStruct((rows, model), BF16),
        scratch_shapes=[pltpu.VMEM((tile, model), BF16)],
        cost_estimate=pl.CostEstimate(flops=2 * rows * model * model, bytes_accessed=20 * 2**20, transcendentals=0),
        compiler_params=pltpu.CompilerParams(dimension_semantics=("arbitrary",), vmem_limit_bytes=48 * 2**20),
        name="finish",
    )(gate, u, w_out, back)


def solution(mesh):
    n_dev, n_groups = mesh.shape["sp"], mesh.shape["dp"]
    n_chunks = 8
    n_chan = LANES // n_chunks
    if (2 * n_chan) % n_groups:
        raise ValueError("uneven groups")
    units = 2 * n_chan // n_groups
    halo_perm = list(zip(range(n_dev - 1), range(1, n_dev)))

    def local_step(u_in, w_in, b_in, conv_taps, w_out, skip_one, skip_two, filt_one, filt_two):
        rank = lax.axis_index("sp")
        u = u_in[0]
        rows = u.shape[0]
        tables = [jnp.asarray(t) for t in transform_tables(rows * n_dev)]

        halo = lax.ppermute(u[-8:].astype(F32), "sp", halo_perm)
        has_prev = (rank > 0).astype(jnp.int32)[None]
        first_unit = lax.axis_index("dp") * units
        place = jnp.stack([first_unit // n_chan, first_unit % n_chan])
        share = turn_share(place, filt_one, filt_two, n_dev, n_chunks, units)
        share, halo = lax.optimization_barrier((share, halo))
        share = lax.all_to_all(share, "sp", 0, 0, tiled=True)
        sent, gate = project(has_prev, u, halo, w_in, b_in[None], conv_taps, n_dev, n_chunks)
        skips = lax.dynamic_slice_in_dim(jnp.stack([skip_one, skip_two]), rank * LANES, LANES, axis=1)
        back = exchange(skips, share, sent, tables, n_dev, n_groups)
        back = back.reshape(n_chunks, n_dev, rows // LANES, LANES // n_chunks, LANES)
        return finish(gate, u, w_out, back)[None]

    seq_spec = P("dp", "sp", None)
    filt_spec = P("sp", None)
    return jax.shard_map(
        local_step,
        mesh=mesh,
        in_specs=(seq_spec, P(), P(), P(), P(), P(), P(), filt_spec, filt_spec),
        out_specs=seq_spec,
        check_vma=False,
    )
```

```python
import functools
import jax
import jax.numpy as jnp
import numpy as np
from jax import lax
from jax.experimental import pallas as pl
from jax.experimental.pallas import tpu as pltpu
from jax.sharding import PartitionSpec as P

LANES = 128
F32 = jnp.float32
BF16 = jnp.bfloat16


def split_table(table, n_parts=3):
    parts, rest = [], np.asarray(table, np.float64)
    for _ in range(n_parts):
        part = rest.astype(jnp.bfloat16)
        parts.append(part)
        rest = rest - part.astype(np.float64)
    return parts


def transform_tables(seq_len):
    n_high = seq_len // LANES
    quarter = np.arange(n_high)[:, None] + 0.25
    high = 2.0 * np.pi * quarter * np.arange(n_high)[None, :] / n_high
    twist = 2.0 * np.pi * quarter * np.arange(LANES)[None, :] / seq_len
    low = 2.0 * np.pi * np.outer(np.arange(LANES), np.arange(LANES)) / LANES
    first = np.concatenate([np.cos(high), -np.sin(high)], axis=0)
    last = np.concatenate([np.cos(high.T), -np.sin(high.T)], axis=1)
    er, ei = np.cos(low), -np.sin(low)
    fwd = np.block([[er, ei], [-ei, er]])
    inv = np.block([[er, -ei], [ei, er]])
    a, b, c = split_table(first)
    first_wide = np.concatenate([a, a, a, b, b, c], axis=1)
    first_thin = np.concatenate([a, b, c], axis=1)
    fwd_parts = np.concatenate(split_table(fwd), axis=0)
    inv_parts = np.concatenate(split_table(inv), axis=0)
    last_parts = np.concatenate(split_table(last), axis=0)
    twist_tab = np.stack([np.cos(twist), -np.sin(twist)]).astype(np.float32)
    return first_wide, first_thin, fwd_parts, inv_parts, last_parts, twist_tab


def split3(x):
    hi = x.astype(BF16)
    rest = x - hi.astype(F32)
    mid = rest.astype(BF16)
    low = (rest - mid.astype(F32)).astype(BF16)
    return hi, mid, low


def dot32(a, b):
    return jnp.dot(a, b, preferred_element_type=F32)


def turn_rows(block, into_ref, n_chunks, row, n_rows):
    turned = block.T
    n_chan = LANES // n_chunks
    for k in range(n_chunks):
        into_ref[k, pl.ds(row, n_chan, stride=n_rows), :] = turned[k * n_chan : (k + 1) * n_chan]


def share_filters(n_dev, n_groups, n_chunks, units, filt_refs, u_ref, share_ref, halo_ref, tail_ref, stage_ref, hold_ref, full_ref, sems):
    stage_sem, sent_sem, share_sem, halo_sem = sems
    me, my_group = lax.axis_index("sp"), lax.axis_index("dp")
    rows = stage_ref.shape[1]
    n_rows = rows // LANES
    n_chan = LANES // n_chunks
    first_unit = my_group * units
    which_mine = first_unit // n_chan
    per_dest = 2 if units == 2 * n_chan else 1
    n_items = n_dev * per_dest

    def target(off):
        return lax.rem(me + off, n_dev)

    def load(item, start):
        slot = lax.rem(item, 2)
        dest = target(item // per_dest + 1)
        cols = pl.ds(pl.multiple_of(dest * LANES, LANES), LANES)

        def copy(ref):
            return pltpu.make_async_copy(ref.at[:, cols], stage_ref.at[slot], stage_sem.at[slot])

        if not start:
            copy(filt_refs[0]).wait()
            return
        which = lax.rem(item, 2) if per_dest == 2 else which_mine
        for w, ref in enumerate(filt_refs):

            @pl.when(which == w)
            def _():
                copy(ref).start()

    load(0, True)
    tail_ref[...] = u_ref[u_ref.shape[0] - tail_ref.shape[0] :, :].astype(F32)

    barrier = pltpu.get_barrier_semaphore()
    for off in range(1, n_dev):
        pl.semaphore_signal(barrier, inc=1, device_id={"sp": target(off)}, device_id_type=pl.DeviceIdType.MESH)
    pl.semaphore_wait(barrier, n_dev - 1)
    halo_send(target, tail_ref, halo_ref, halo_sem).start()

    @pl.loop(0, n_items)
    def _(item):
        slot = lax.rem(item, 2)
        off = item // per_dest + 1
        dest = target(off)

        @pl.when(item + 1 < n_items)
        def _():
            load(item + 1, True)

        load(item, False)
        into = hold_ref.at[dest] if units >= n_chan else full_ref
        base = lax.rem(item, per_dest) * (n_chan * n_rows)

        @pl.loop(0, n_rows)
        def _(r):
            turn_rows(stage_ref[slot, pl.ds(pl.multiple_of(r * LANES, LANES), LANES), :], into, n_chunks, base + r, n_rows)

        if units < n_chan:
            start = pl.multiple_of(lax.rem(first_unit, n_chan) * n_rows, n_rows)
            hold_ref[dest] = full_ref[:, pl.ds(start, units * n_rows), :]

        @pl.when(jnp.logical_and(lax.rem(item, per_dest) == per_dest - 1, off < n_dev))
        def _():
            share_send(me, target, hold_ref, share_ref, sent_sem, share_sem, off).start()

    pltpu.make_async_copy(hold_ref.at[me], share_ref.at[me], sent_sem.at[0]).start()


def share_send(me, target, hold_ref, share_ref, sent_sem, share_sem, off):
    dest = target(off)
    return pltpu.make_async_remote_copy(
        src_ref=hold_ref.at[dest],
        dst_ref=share_ref.at[me],
        send_sem=sent_sem.at[off],
        recv_sem=share_sem.at[off],
        device_id={"sp": dest},
        device_id_type=pl.DeviceIdType.MESH,
    )


def halo_send(target, tail_ref, halo_ref, halo_sem):
    return pltpu.make_async_remote_copy(
        src_ref=tail_ref,
        dst_ref=halo_ref,
        send_sem=halo_sem.at[0],
        recv_sem=halo_sem.at[1],
        device_id={"sp": target(1)},
        device_id_type=pl.DeviceIdType.MESH,
    )


def project_body(n_dev, n_groups, n_chunks, units, u_ref, one_ref, two_ref, *refs):
    w_refs, b_refs, tap_refs = refs[:3], refs[3:6], refs[6:9]
    sent_ref, gate_ref, share_ref, p_ref, halo_ref, tail_ref, stage_ref, hold_ref, full_ref, *sems = refs[9:]
    stage_sem, sent_sem, share_sem, halo_sem = sems
    rows = u_ref.shape[0]
    n_rows = rows // LANES
    width = w_refs[0].shape[1]
    me = lax.axis_index("sp")
    step_idx = pl.program_id(0)

    def target(off):
        return lax.rem(me + off, n_dev)

    @pl.when(step_idx == 0)
    def _():
        share_filters(n_dev, n_groups, n_chunks, units, (one_ref, two_ref), u_ref, share_ref, halo_ref, tail_ref, stage_ref, hold_ref, full_ref, sems)
        halo_send(target, tail_ref, halo_ref, halo_sem).wait()

    for which in range(3):
        w = w_refs[which][...]
        bias = b_refs[which][...]
        halo = (dot32(halo_ref[...].astype(BF16), w) + bias).astype(BF16).astype(F32)
        p_ref[0:8, :] = jnp.where(me > 0, halo, 0.0)
        step = 2 * LANES

        @pl.loop(0, rows // step)
        def _(i):
            start = pl.multiple_of(i * step, step)
            proj = dot32(u_ref[pl.ds(start, step), :], w) + bias
            p_ref[pl.ds(start + 8, step), :] = proj.astype(BF16).astype(F32)

        c0, c1, c2 = (tap_refs[which][t : t + 1, :] for t in range(3))

        @pl.loop(0, n_rows)
        def _(r):
            start = pl.multiple_of(r * LANES, LANES)
            window = p_ref[pl.ds(start, LANES + 8), :]
            mixed = c0 * window[8:] + c1 * window[7:-1] + c2 * window[6:-2]
            mixed = mixed.astype(BF16)
            if which == 1:
                gate_ref[pl.ds(start, LANES), :] = mixed
            else:
                slot = 1 if which == 0 else 0
                for d in range(width // LANES):
                    block = mixed[:, d * LANES : (d + 1) * LANES].astype(F32)
                    turn_rows(block, sent_ref.at[:, d, slot], n_chunks, r, n_rows)

    @pl.when(step_idx == pl.num_programs(0) - 1)
    def _():
        pltpu.make_async_copy(hold_ref.at[me], share_ref.at[me], sent_sem.at[0]).wait()
        for off in range(1, n_dev):
            share_send(me, target, hold_ref, share_ref, sent_sem, share_sem, off).wait()


def project(u, filt_one, filt_two, w_in, b_in, taps, n_dev, n_groups, n_chunks, units):
    rows, depth = u.shape
    model = w_in.shape[1] // 3
    width = 2 * LANES
    steps = model // width
    n_rows = rows // LANES
    n_chan = LANES // n_chunks
    chunk_rows = n_chan * n_rows
    any_spec = pl.BlockSpec(memory_space=pl.ANY)

    def third(height):
        return [pl.BlockSpec((height, width), functools.partial(lambda off, j: (0, off + j), t * steps)) for t in range(3)]

    full_shape = (n_chunks, chunk_rows, LANES) if units < n_chan else (1, 8, LANES)
    return pl.pallas_call(
        functools.partial(project_body, n_dev, n_groups, n_chunks, units),
        grid=(steps,),
        in_specs=[pl.BlockSpec((rows, depth), lambda j: (0, 0)), any_spec, any_spec, *third(depth), *third(1), *third(3)],
        out_specs=[
            pl.BlockSpec((n_chunks, 2, 2, chunk_rows, LANES), lambda j: (0, j, 0, 0, 0)),
            pl.BlockSpec((rows, width), lambda j: (0, j)),
            any_spec,
        ],
        out_shape=[
            jax.ShapeDtypeStruct((n_chunks, n_dev, 2, chunk_rows, LANES), F32),
            jax.ShapeDtypeStruct((rows, model), BF16),
            jax.ShapeDtypeStruct((n_dev, n_chunks, units * n_rows, LANES), F32),
        ],
        scratch_shapes=[
            pltpu.VMEM((rows + 8, width), F32),
            pltpu.VMEM((8, depth), F32),
            pltpu.VMEM((8, depth), F32),
            pltpu.VMEM((2, rows, LANES), F32),
            pltpu.VMEM((n_dev, n_chunks, units * n_rows, LANES), F32),
            pltpu.VMEM(full_shape, F32),
            pltpu.SemaphoreType.DMA((2,)),
            pltpu.SemaphoreType.DMA((n_dev,)),
            pltpu.SemaphoreType.DMA((n_dev,)),
            pltpu.SemaphoreType.DMA((2,)),
        ],
        cost_estimate=pl.CostEstimate(flops=2 * rows * depth * 3 * model, bytes_accessed=50 * 2**20, transcendentals=0),
        compiler_params=pltpu.CompilerParams(
            dimension_semantics=("arbitrary",), collective_id=0, has_side_effects=True, vmem_limit_bytes=60 * 2**20
        ),
        name="project",
    )(u, filt_one, filt_two, w_in, w_in, w_in, b_in, b_in, b_in, taps, taps, taps)


def spectrum_tools(group, n_high, tables, parts_ref):
    wide_ref, thin_ref, fwd_ref, inv_ref, last_ref, twist_ref = tables
    wide = 2 * LANES
    scale = 1.0 / (n_high * LANES)

    def complex_dot(tab_ref):
        return (
            dot32(parts_ref[:, 2 * wide :], tab_ref[:wide])
            + dot32(parts_ref[:, wide : 2 * wide], tab_ref[:wide])
            + dot32(parts_ref[:, :wide], tab_ref[wide : 2 * wide])
            + dot32(parts_ref[:, wide : 2 * wide], tab_ref[wide : 2 * wide])
            + dot32(parts_ref[:, :wide], tab_ref[2 * wide :])
            + dot32(parts_ref[:, :wide], tab_ref[:wide])
        )

    def store_parts(g, real, imag):
        for t, (re, im) in enumerate(zip(split3(real), split3(imag))):
            parts_ref[g * n_high : (g + 1) * n_high, 2 * t * LANES : (2 * t + 1) * LANES] = re
            parts_ref[g * n_high : (g + 1) * n_high, (2 * t + 1) * LANES : (2 * t + 2) * LANES] = im

    def spectrum(signals, exact):
        tr, ti = twist_ref[0], twist_ref[1]
        for g in range(0, group, 2):
            pair = jnp.concatenate([signals[g], signals[g + 1]], axis=1)
            if exact:
                short = pair.astype(BF16)
                coarse = dot32(thin_ref[...], jnp.concatenate([short, short, short], axis=0))
            else:
                hi, mid, low = split3(pair)
                coarse = dot32(wide_ref[...], jnp.concatenate([hi, mid, low, hi, mid, hi], axis=0))
            for j in range(2):
                re = coarse[:n_high, j * LANES : (j + 1) * LANES]
                im = coarse[n_high:, j * LANES : (j + 1) * LANES]
                store_parts(g + j, re * tr - im * ti, re * ti + im * tr)
        return complex_dot(fwd_ref)

    def signal(spec_a, spec_b):
        tr, ti = twist_ref[0], twist_ref[1]
        for g in range(group):
            rows = slice(g * n_high, (g + 1) * n_high)
            ar, ai = spec_a[rows, :LANES], spec_a[rows, LANES:]
            br, bi = spec_b[rows, :LANES], spec_b[rows, LANES:]
            store_parts(g, ar * br - ai * bi, ar * bi + ai * br)
        fine = complex_dot(inv_ref)
        results = []
        for g in range(0, group, 2):
            halves = []
            for j in range(2):
                rows = slice((g + j) * n_high, (g + j + 1) * n_high)
                re, im = fine[rows, :LANES] * scale, fine[rows, LANES:] * scale
                halves.append(jnp.concatenate([re * tr + im * ti, im * tr - re * ti], axis=0))
            hi, mid, low = split3(jnp.concatenate(halves, axis=1))
            d_hi = dot32(last_ref[...], hi)
            d_mid = dot32(last_ref[: 2 * n_high], mid)
            d_low = dot32(last_ref[:n_high], low)
            small = d_hi[2 * n_high :] + d_mid[n_high:] + d_low
            total = d_hi[:n_high] + ((d_hi[n_high : 2 * n_high] + d_mid[:n_high]) + small)
            results += [total[:, :LANES], total[:, LANES:]]
        return results

    return spectrum, signal


def exchange_body(n_dev, n_groups, group, skip_one_ref, skip_two_ref, share_ref, sent_ref, wide_ref, thin_ref, fwd_ref, inv_ref, last_ref, twist_ref, back_ref, got_ref, filt_ref, done_ref, parts_ref, spec_one_ref, spec_two_ref, sent_sem, got_sem, share_sem, filt_sem, back_sem, done_sem):
    n_chunks, _, _, chunk_rows, _ = sent_ref.shape
    n_high = twist_ref.shape[1]
    per_src = n_high // n_dev
    n_chan = chunk_rows // per_src
    me, my_group = lax.axis_index("sp"), lax.axis_index("dp")
    share_rows = share_ref.shape[2]
    spectrum, signal = spectrum_tools(group, n_high, (wide_ref, thin_ref, fwd_ref, inv_ref, last_ref, twist_ref), parts_ref)

    barrier = pltpu.get_barrier_semaphore()
    for off in range(1, n_dev):
        pl.semaphore_signal(barrier, inc=1, device_id={"sp": lax.rem(me + off, n_dev)}, device_id_type=pl.DeviceIdType.MESH)
    for off in range(1, n_groups):
        pl.semaphore_signal(barrier, inc=1, device_id={"dp": lax.rem(my_group + off, n_groups)}, device_id_type=pl.DeviceIdType.MESH)
    pl.semaphore_wait(barrier, n_dev + n_groups - 2)

    def sharing(k, off):
        return pltpu.make_async_remote_copy(
            src_ref=share_ref.at[:, k],
            dst_ref=share_of(k),
            send_sem=share_sem.at[k],
            recv_sem=filt_sem.at[k],
            device_id={"dp": lax.rem(my_group + off, n_groups)},
            device_id_type=pl.DeviceIdType.MESH,
        )

    def share_of(k):
        return filt_ref.at[k, :, pl.ds(pl.multiple_of(my_group * share_rows, share_rows), share_rows), :]

    def own_share(k):
        return pltpu.make_async_copy(share_ref.at[:, k], share_of(k), filt_sem.at[k])

    def all_shares(k):
        return pltpu.make_async_copy(filt_ref.at[k], filt_ref.at[k], filt_sem.at[k])

    def sending(k, off):
        dest = lax.rem(me + off, n_dev)
        return pltpu.make_async_remote_copy(
            src_ref=sent_ref.at[k, dest],
            dst_ref=got_ref.at[k, me],
            send_sem=sent_sem.at[k, off],
            recv_sem=got_sem.at[k, off],
            device_id={"sp": dest},
            device_id_type=pl.DeviceIdType.MESH,
        )

    def keeping(k):
        return pltpu.make_async_copy(sent_ref.at[k, me], got_ref.at[k, me], got_sem.at[k, 0])

    block = per_src * n_chan

    def part_of(k, dest):
        return done_ref.at[k, pl.ds(pl.multiple_of(dest * block, block), block), :]

    def returning(k, off):
        dest = lax.rem(me + off, n_dev)
        return pltpu.make_async_remote_copy(
            src_ref=part_of(k, dest),
            dst_ref=back_ref.at[k, me],
            send_sem=done_sem.at[k, off],
            recv_sem=back_sem.at[k, off],
            device_id={"sp": dest},
            device_id_type=pl.DeviceIdType.MESH,
        )

    def storing(k):
        return pltpu.make_async_copy(part_of(k, me), back_ref.at[k, me], done_sem.at[k, 0])

    @pl.loop(0, n_chunks)
    def _(k):
        own_share(k).start()
        keeping(k).start()
        for off in range(1, n_groups):
            sharing(k, off).start()
        for off in range(1, n_dev):
            sending(k, off).start()

    @pl.loop(0, n_chunks)
    def _(k):
        all_shares(k).wait()
        keeping(k).wait()
        for off in range(1, n_dev):
            sending(k, off).wait_recv()

        @pl.loop(0, n_chan // group)
        def _(i):
            first = i * group

            def load_h(which, g):
                start = pl.multiple_of((which * n_chan + first + g) * per_src, per_src)
                return filt_ref[k, :, pl.ds(start, per_src), :].reshape(n_high, LANES)

            def load_x(which, g):
                start = pl.multiple_of((first + g) * per_src, per_src)
                return got_ref[k, :, which, pl.ds(start, per_src), :].reshape(n_high, LANES)

            chan = me * LANES + k * n_chan + first
            spec_one_ref[...] = spectrum([load_h(0, g) for g in range(group)], False)
            spec_two_ref[...] = spectrum([load_h(1, g) for g in range(group)], False)
            values = [load_x(0, g) for g in range(group)]
            conv = signal(spectrum(values, True), spec_one_ref)
            gated = [load_x(1, g) * (conv[g] + skip_one_ref[chan + g] * values[g]) for g in range(group)]
            conv = signal(spectrum(gated, False), spec_two_ref)
            for g in range(group):
                done_ref[k, pl.ds(first + g, n_high, stride=n_chan), :] = conv[g] + skip_two_ref[chan + g] * gated[g]

        storing(k).start()
        for off in range(1, n_dev):
            returning(k, off).start()

    @pl.loop(0, n_chunks)
    def _(k):
        for off in range(1, n_dev):
            sending(k, off).wait_send()
            returning(k, off).wait()
        storing(k).wait()
        for off in range(1, n_groups):
            sharing(k, off).wait_send()


def exchange(skip_one, skip_two, share, sent, tables, n_dev, n_groups, group=4):
    n_chunks, _, _, chunk_rows, _ = sent.shape
    n_high = tables[-1].shape[1]
    n_chan = chunk_rows // (n_high // n_dev)
    any_spec = pl.BlockSpec(memory_space=pl.ANY)
    vmem_spec = pl.BlockSpec(memory_space=pltpu.VMEM)
    return pl.pallas_call(
        functools.partial(exchange_body, n_dev, n_groups, group),
        in_specs=[pl.BlockSpec(memory_space=pltpu.SMEM)] * 2 + [any_spec, any_spec] + [vmem_spec] * len(tables),
        out_specs=any_spec,
        out_shape=jax.ShapeDtypeStruct((n_chunks, n_dev, chunk_rows, LANES), F32),
        scratch_shapes=[
            pltpu.VMEM((n_chunks, n_dev, 2, chunk_rows, LANES), F32),
            pltpu.VMEM((n_chunks, n_dev, 2 * chunk_rows, LANES), F32),
            pltpu.VMEM((n_chunks, n_high * n_chan, LANES), F32),
            pltpu.VMEM((group * n_high, 6 * LANES), BF16),
            pltpu.VMEM((group * n_high, 2 * LANES), F32),
            pltpu.VMEM((group * n_high, 2 * LANES), F32),
            pltpu.SemaphoreType.DMA((n_chunks, n_dev)),
            pltpu.SemaphoreType.DMA((n_chunks, n_dev)),
            pltpu.SemaphoreType.DMA((n_chunks,)),
            pltpu.SemaphoreType.DMA((n_chunks,)),
            pltpu.SemaphoreType.DMA((n_chunks, n_dev)),
            pltpu.SemaphoreType.DMA((n_chunks, n_dev)),
        ],
        cost_estimate=pl.CostEstimate(flops=10**11, bytes_accessed=40 * 2**20, transcendentals=0),
        compiler_params=pltpu.CompilerParams(collective_id=1, has_side_effects=True, vmem_limit_bytes=60 * 2**20),
        name="exchange",
    )(skip_one, skip_two, share, sent, *tables)


def finish_body(gate_ref, u_ref, w_ref, back_ref, out_ref, y_ref):
    n_chunks, n_src, n_rows, _, _ = back_ref.shape
    for r in range(n_rows):
        for s in range(n_src):
            full = jnp.concatenate([back_ref[k, s, r] for k in range(n_chunks)], axis=0)
            rows, cols = slice(r * LANES, (r + 1) * LANES), slice(s * LANES, (s + 1) * LANES)
            y_ref[rows, cols] = (gate_ref[rows, cols].astype(F32) * full.T).astype(BF16)
    out_ref[...] = (u_ref[...].astype(F32) + dot32(y_ref[...], w_ref[...])).astype(BF16)


def finish(gate, u, w_out, back, n_rows=2):
    rows, model = u.shape
    n_chunks, n_src, _, per_chunk, _ = back.shape
    tile = n_rows * LANES
    return pl.pallas_call(
        finish_body,
        grid=(rows // tile,),
        in_specs=[
            pl.BlockSpec((tile, model), lambda i: (i, 0)),
            pl.BlockSpec((tile, model), lambda i: (i, 0)),
            pl.BlockSpec(w_out.shape, lambda i: (0, 0)),
            pl.BlockSpec((n_chunks, n_src, n_rows, per_chunk, LANES), lambda i: (0, 0, i, 0, 0)),
        ],
        out_specs=pl.BlockSpec((tile, model), lambda i: (i, 0)),
        out_shape=jax.ShapeDtypeStruct((rows, model), BF16),
        scratch_shapes=[pltpu.VMEM((tile, model), BF16)],
        cost_estimate=pl.CostEstimate(flops=2 * rows * model * model, bytes_accessed=20 * 2**20, transcendentals=0),
        compiler_params=pltpu.CompilerParams(dimension_semantics=("arbitrary",), vmem_limit_bytes=48 * 2**20),
        name="finish",
    )(gate, u, w_out, back)


def solution(mesh):
    n_dev, n_groups = mesh.shape["sp"], mesh.shape["dp"]
    n_chunks = 8
    n_chan = LANES // n_chunks
    if (2 * n_chan) % n_groups:
        raise ValueError("uneven groups")
    units = 2 * n_chan // n_groups
    def local_step(u_in, w_in, b_in, conv_taps, w_out, skip_one, skip_two, filt_one, filt_two):
        u = u_in[0]
        rows = u.shape[0]
        tables = [jnp.asarray(t) for t in transform_tables(rows * n_dev)]
        sent, gate, share = project(u, filt_one, filt_two, w_in, b_in[None], conv_taps, n_dev, n_groups, n_chunks, units)
        back = exchange(skip_one, skip_two, share, sent, tables, n_dev, n_groups)
        back = back.reshape(n_chunks, n_dev, rows // LANES, LANES // n_chunks, LANES)
        return finish(gate, u, w_out, back)[None]

    seq_spec = P("dp", "sp", None)
    filt_spec = P("sp", None)
    return jax.shard_map(
        local_step,
        mesh=mesh,
        in_specs=(seq_spec, P(), P(), P(), P(), P(), P(), filt_spec, filt_spec),
        out_specs=seq_spec,
        check_vma=False,
    )
```

```python
import functools
import math
import jax
import jax.numpy as jnp
import numpy as np
from jax import lax
from jax.experimental import pallas as pl
from jax.experimental.pallas import tpu as pltpu
from jax.sharding import PartitionSpec as P

LANES = 128
F32 = jnp.float32
BF16 = jnp.bfloat16


def split_table(table, n_parts=3):
    parts, rest = [], np.asarray(table, np.float64)
    for _ in range(n_parts):
        part = rest.astype(jnp.bfloat16)
        parts.append(part)
        rest = rest - part.astype(np.float64)
    return parts


def transform_tables(seq_len):
    n_high = seq_len // LANES
    quarter = np.arange(n_high)[:, None] + 0.25
    high = 2.0 * np.pi * quarter * np.arange(n_high)[None, :] / n_high
    twist = 2.0 * np.pi * quarter * np.arange(LANES)[None, :] / seq_len
    low = 2.0 * np.pi * np.outer(np.arange(LANES), np.arange(LANES)) / LANES
    first = np.concatenate([np.cos(high), -np.sin(high)], axis=0)
    last = np.concatenate([np.cos(high.T), -np.sin(high.T)], axis=1)
    er, ei = np.cos(low), -np.sin(low)
    fwd = np.block([[er, ei], [-ei, er]])
    inv = np.block([[er, -ei], [ei, er]])
    a, b, c = split_table(first)
    first_wide = np.concatenate([a, a, a, b, b, c], axis=1)
    first_thin = np.concatenate([a, b, c], axis=1)
    fwd_parts = np.concatenate(split_table(fwd), axis=0)
    inv_parts = np.concatenate(split_table(inv), axis=0)
    last_parts = np.concatenate(split_table(last), axis=0)
    twist_tab = np.stack([np.cos(twist), -np.sin(twist)]).astype(np.float32)
    return first_wide, first_thin, fwd_parts, inv_parts, last_parts, twist_tab


def split3(x):
    hi = x.astype(BF16)
    rest = x - hi.astype(F32)
    mid = rest.astype(BF16)
    low = (rest - mid.astype(F32)).astype(BF16)
    return hi, mid, low


def dot32(a, b):
    return jnp.dot(a, b, preferred_element_type=F32)


def turn_rows(block, into_ref, n_chunks, row, n_rows):
    turned = block.T
    n_chan = LANES // n_chunks
    for k in range(n_chunks):
        into_ref[k, pl.ds(row, n_chan, stride=n_rows), :] = turned[k * n_chan : (k + 1) * n_chan]


def spread_offsets(n_dev):
    pairs = [off for near in range(2, n_dev, 4) for off in (near, n_dev - near)]
    rest = [off for off in range(1, n_dev) if off not in pairs]
    rest.sort(key=lambda off: -min(off, n_dev - off))
    order = list(dict.fromkeys(pairs)) + rest
    return order


def share_filters(n_dev, n_groups, n_chunks, units, filt_refs, u_hbm_ref, u_ref, share_ref, halo_ref, tail_ref, stage_ref, hold_ref, full_ref, sems):
    stage_sem, sent_sem, share_sem, halo_sem, u_sem = sems
    me, my_group = lax.axis_index("sp"), lax.axis_index("dp")
    rows = stage_ref.shape[1]
    n_rows = rows // LANES
    n_chan = LANES // n_chunks
    first_unit = my_group * units
    which_mine = first_unit // n_chan
    both = units == 2 * n_chan
    items = [(off, which) for off in spread_offsets(n_dev) + [0] for which in ((0, 1) if both else (None,))]

    def target(off):
        return lax.rem(me + off, n_dev)

    def loading(item, which):
        cols = pl.ds(pl.multiple_of(target(items[item][0]) * LANES, LANES), LANES)
        return pltpu.make_async_copy(filt_refs[which].at[:, cols], stage_ref.at[item % 2], stage_sem.at[item % 2])

    def load(item):
        if both:
            loading(item, items[item][1]).start()
            return
        for which in range(2):

            @pl.when(which_mine == which)
            def _():
                loading(item, which).start()

    tail_rows = u_ref.at[pl.ds(rows - 16, 16), :]
    tail_copy = pltpu.make_async_copy(u_hbm_ref.at[pl.ds(rows - 16, 16), :], tail_rows, u_sem.at[1])
    head_copy = u_head(u_hbm_ref, u_ref, u_sem)
    barrier = pltpu.get_barrier_semaphore()
    for off in range(1, n_dev):
        pl.semaphore_signal(barrier, inc=1, device_id={"sp": target(off)}, device_id_type=pl.DeviceIdType.MESH)
    load(0)
    tail_copy.start()
    for item, (off, which) in enumerate(items):
        if item + 1 < len(items):
            load(item + 1)
        if item == 0:
            head_copy.start()
        loading(item, 0).wait()
        dest = target(off)
        into = hold_ref.at[dest] if units >= n_chan else full_ref
        base = n_chan * n_rows if which == 1 else 0
        together = math.gcd(n_rows, 4)

        @pl.loop(0, n_rows // together)
        def _(i):
            for j in range(together):
                r = i * together + j
                turn_rows(stage_ref[item % 2, pl.ds(pl.multiple_of(r * LANES, LANES), LANES), :], into, n_chunks, base + r, n_rows)

        if units < n_chan:
            start = pl.multiple_of(lax.rem(first_unit, n_chan) * n_rows, n_rows)
            hold_ref[dest] = full_ref[:, pl.ds(start, units * n_rows), :]
        if item == 0:
            tail_copy.wait()
            tail_ref[...] = tail_rows[...].astype(F32)[8:]
            pl.semaphore_wait(barrier, n_dev - 1)
            halo_send(target, tail_ref, halo_ref, halo_sem).start()
        if off and which != 0:
            share_send(me, target, hold_ref, share_ref, sent_sem, share_sem, off).start()
    pltpu.make_async_copy(hold_ref.at[me], share_ref.at[me], sent_sem.at[0]).start()


def u_head(u_hbm_ref, u_ref, u_sem):
    rows = u_ref.shape[0] - 16
    return pltpu.make_async_copy(u_hbm_ref.at[pl.ds(0, rows), :], u_ref.at[pl.ds(0, rows), :], u_sem.at[0])


def share_send(me, target, hold_ref, share_ref, sent_sem, share_sem, off):
    dest = target(off)
    return pltpu.make_async_remote_copy(
        src_ref=hold_ref.at[dest],
        dst_ref=share_ref.at[me],
        send_sem=sent_sem.at[off],
        recv_sem=share_sem.at[off],
        device_id={"sp": dest},
        device_id_type=pl.DeviceIdType.MESH,
    )


def halo_send(target, tail_ref, halo_ref, halo_sem):
    return pltpu.make_async_remote_copy(
        src_ref=tail_ref,
        dst_ref=halo_ref,
        send_sem=halo_sem.at[0],
        recv_sem=halo_sem.at[1],
        device_id={"sp": target(1)},
        device_id_type=pl.DeviceIdType.MESH,
    )


def project_body(n_dev, n_groups, n_chunks, units, u_hbm_ref, one_ref, two_ref, *refs):
    w_refs, b_refs, tap_refs = refs[:3], refs[3:6], refs[6:9]
    sent_ref, gate_ref, share_ref, u_ref, p_ref, halo_ref, tail_ref, stage_ref, hold_ref, full_ref, *sems = refs[9:]
    stage_sem, sent_sem, share_sem, halo_sem, u_sem = sems
    rows = u_ref.shape[0]
    n_rows = rows // LANES
    width = w_refs[0].shape[1]
    me = lax.axis_index("sp")
    step_idx = pl.program_id(0)

    def target(off):
        return lax.rem(me + off, n_dev)

    @pl.when(step_idx == 0)
    def _():
        share_filters(n_dev, n_groups, n_chunks, units, (one_ref, two_ref), u_hbm_ref, u_ref, share_ref, halo_ref, tail_ref, stage_ref, hold_ref, full_ref, sems)
        u_head(u_hbm_ref, u_ref, u_sem).wait()
        halo_send(target, tail_ref, halo_ref, halo_sem).wait()

    for which in range(3):
        w = w_refs[which][...]
        bias = b_refs[which][...]
        halo = (dot32(halo_ref[...].astype(BF16), w) + bias).astype(BF16).astype(F32)
        p_ref[0:8, :] = jnp.where(me > 0, halo, 0.0)
        step = 2 * LANES

        @pl.loop(0, rows // step)
        def _(i):
            start = pl.multiple_of(i * step, step)
            proj = dot32(u_ref[pl.ds(start, step), :], w) + bias
            p_ref[pl.ds(start + 8, step), :] = proj.astype(BF16).astype(F32)

        c0, c1, c2 = (tap_refs[which][t : t + 1, :] for t in range(3))

        @pl.loop(0, n_rows)
        def _(r):
            start = pl.multiple_of(r * LANES, LANES)
            window = p_ref[pl.ds(start, LANES + 8), :]
            mixed = c0 * window[8:] + c1 * window[7:-1] + c2 * window[6:-2]
            mixed = mixed.astype(BF16)
            if which == 1:
                gate_ref[pl.ds(start, LANES), :] = mixed
            else:
                slot = 1 if which == 0 else 0
                for d in range(width // LANES):
                    block = mixed[:, d * LANES : (d + 1) * LANES].astype(F32)
                    turn_rows(block, sent_ref.at[:, d, slot], n_chunks, r, n_rows)

    @pl.when(step_idx == pl.num_programs(0) - 1)
    def _():
        pltpu.make_async_copy(hold_ref.at[me], share_ref.at[me], sent_sem.at[0]).wait()
        for off in range(1, n_dev):
            share_send(me, target, hold_ref, share_ref, sent_sem, share_sem, off).wait()


def project(u, filt_one, filt_two, w_in, b_in, taps, n_dev, n_groups, n_chunks, units):
    rows, depth = u.shape
    model = w_in.shape[1] // 3
    width = 2 * LANES
    steps = model // width
    n_rows = rows // LANES
    n_chan = LANES // n_chunks
    chunk_rows = n_chan * n_rows
    any_spec = pl.BlockSpec(memory_space=pl.ANY)

    def third(height):
        return [pl.BlockSpec((height, width), functools.partial(lambda off, j: (0, off + j), t * steps)) for t in range(3)]

    full_shape = (n_chunks, chunk_rows, LANES) if units < n_chan else (1, 8, LANES)
    return pl.pallas_call(
        functools.partial(project_body, n_dev, n_groups, n_chunks, units),
        grid=(steps,),
        in_specs=[any_spec, any_spec, any_spec, *third(depth), *third(1), *third(3)],
        out_specs=[
            pl.BlockSpec((n_chunks, 2, 2, chunk_rows, LANES), lambda j: (0, j, 0, 0, 0)),
            pl.BlockSpec((rows, width), lambda j: (0, j)),
            any_spec,
        ],
        out_shape=[
            jax.ShapeDtypeStruct((n_chunks, n_dev, 2, chunk_rows, LANES), F32),
            jax.ShapeDtypeStruct((rows, model), BF16),
            jax.ShapeDtypeStruct((n_dev, n_chunks, units * n_rows, LANES), F32),
        ],
        scratch_shapes=[
            pltpu.VMEM((rows, depth), BF16),
            pltpu.VMEM((rows + 8, width), F32),
            pltpu.VMEM((8, depth), F32),
            pltpu.VMEM((8, depth), F32),
            pltpu.VMEM((2, rows, LANES), F32),
            pltpu.VMEM((n_dev, n_chunks, units * n_rows, LANES), F32),
            pltpu.VMEM(full_shape, F32),
            pltpu.SemaphoreType.DMA((2,)),
            pltpu.SemaphoreType.DMA((n_dev,)),
            pltpu.SemaphoreType.DMA((n_dev,)),
            pltpu.SemaphoreType.DMA((2,)),
            pltpu.SemaphoreType.DMA((2,)),
        ],
        cost_estimate=pl.CostEstimate(flops=2 * rows * depth * 3 * model, bytes_accessed=50 * 2**20, transcendentals=0),
        compiler_params=pltpu.CompilerParams(
            dimension_semantics=("arbitrary",), collective_id=0, has_side_effects=True, vmem_limit_bytes=60 * 2**20
        ),
        name="project",
    )(u, filt_one, filt_two, w_in, w_in, w_in, b_in, b_in, b_in, taps, taps, taps)


def spectrum_tools(group, n_high, tables, parts_ref):
    wide_ref, thin_ref, fwd_ref, inv_ref, last_ref, twist_ref = tables
    wide = 2 * LANES
    scale = 1.0 / (n_high * LANES)

    def complex_dot(tab_ref):
        return (
            dot32(parts_ref[:, 2 * wide :], tab_ref[:wide])
            + dot32(parts_ref[:, wide : 2 * wide], tab_ref[:wide])
            + dot32(parts_ref[:, :wide], tab_ref[wide : 2 * wide])
            + dot32(parts_ref[:, wide : 2 * wide], tab_ref[wide : 2 * wide])
            + dot32(parts_ref[:, :wide], tab_ref[2 * wide :])
            + dot32(parts_ref[:, :wide], tab_ref[:wide])
        )

    def store_parts(g, real, imag):
        for t, (re, im) in enumerate(zip(split3(real), split3(imag))):
            parts_ref[g * n_high : (g + 1) * n_high, 2 * t * LANES : (2 * t + 1) * LANES] = re
            parts_ref[g * n_high : (g + 1) * n_high, (2 * t + 1) * LANES : (2 * t + 2) * LANES] = im

    def spectrum(signals, exact):
        tr, ti = twist_ref[0], twist_ref[1]
        for g in range(0, group, 2):
            pair = jnp.concatenate([signals[g], signals[g + 1]], axis=1)
            if exact:
                short = pair.astype(BF16)
                coarse = dot32(thin_ref[...], jnp.concatenate([short, short, short], axis=0))
            else:
                hi, mid, low = split3(pair)
                coarse = dot32(wide_ref[...], jnp.concatenate([hi, mid, low, hi, mid, hi], axis=0))
            for j in range(2):
                re = coarse[:n_high, j * LANES : (j + 1) * LANES]
                im = coarse[n_high:, j * LANES : (j + 1) * LANES]
                store_parts(g + j, re * tr - im * ti, re * ti + im * tr)
        return complex_dot(fwd_ref)

    def signal(spec_a, spec_b):
        tr, ti = twist_ref[0], twist_ref[1]
        for g in range(group):
            rows = slice(g * n_high, (g + 1) * n_high)
            ar, ai = spec_a[rows, :LANES], spec_a[rows, LANES:]
            br, bi = spec_b[rows, :LANES], spec_b[rows, LANES:]
            store_parts(g, ar * br - ai * bi, ar * bi + ai * br)
        fine = complex_dot(inv_ref)
        results = []
        for g in range(0, group, 2):
            halves = []
            for j in range(2):
                rows = slice((g + j) * n_high, (g + j + 1) * n_high)
                re, im = fine[rows, :LANES] * scale, fine[rows, LANES:] * scale
                halves.append(jnp.concatenate([re * tr + im * ti, im * tr - re * ti], axis=0))
            hi, mid, low = split3(jnp.concatenate(halves, axis=1))
            d_hi = dot32(last_ref[...], hi)
            d_mid = dot32(last_ref[: 2 * n_high], mid)
            d_low = dot32(last_ref[:n_high], low)
            small = d_hi[2 * n_high :] + d_mid[n_high:] + d_low
            total = d_hi[:n_high] + ((d_hi[n_high : 2 * n_high] + d_mid[:n_high]) + small)
            results += [total[:, :LANES], total[:, LANES:]]
        return results

    return spectrum, signal


def exchange_body(n_dev, n_groups, group, skip_one_ref, skip_two_ref, share_ref, sent_ref, wide_ref, thin_ref, fwd_ref, inv_ref, last_ref, twist_ref, back_ref, got_ref, filt_ref, done_ref, parts_ref, spec_one_ref, spec_two_ref, sent_sem, got_sem, share_sem, filt_sem, back_sem, done_sem):
    n_chunks, _, _, chunk_rows, _ = sent_ref.shape
    n_high = twist_ref.shape[1]
    per_src = n_high // n_dev
    n_chan = chunk_rows // per_src
    me, my_group = lax.axis_index("sp"), lax.axis_index("dp")
    share_rows = share_ref.shape[2]
    spectrum, signal = spectrum_tools(group, n_high, (wide_ref, thin_ref, fwd_ref, inv_ref, last_ref, twist_ref), parts_ref)

    barrier = pltpu.get_barrier_semaphore()
    for off in range(1, n_dev):
        pl.semaphore_signal(barrier, inc=1, device_id={"sp": lax.rem(me + off, n_dev)}, device_id_type=pl.DeviceIdType.MESH)
    for off in range(1, n_groups):
        pl.semaphore_signal(barrier, inc=1, device_id={"dp": lax.rem(my_group + off, n_groups)}, device_id_type=pl.DeviceIdType.MESH)
    pl.semaphore_wait(barrier, n_dev + n_groups - 2)

    def sharing(k, off):
        return pltpu.make_async_remote_copy(
            src_ref=share_ref.at[:, k],
            dst_ref=share_of(k),
            send_sem=share_sem.at[k],
            recv_sem=filt_sem.at[k],
            device_id={"dp": lax.rem(my_group + off, n_groups)},
            device_id_type=pl.DeviceIdType.MESH,
        )

    def share_of(k):
        return filt_ref.at[k, :, pl.ds(pl.multiple_of(my_group * share_rows, share_rows), share_rows), :]

    def own_share(k):
        return pltpu.make_async_copy(share_ref.at[:, k], share_of(k), filt_sem.at[k])

    def all_shares(k):
        return pltpu.make_async_copy(filt_ref.at[k], filt_ref.at[k], filt_sem.at[k])

    def sending(k, off):
        dest = lax.rem(me + off, n_dev)
        return pltpu.make_async_remote_copy(
            src_ref=sent_ref.at[k, dest],
            dst_ref=got_ref.at[k, me],
            send_sem=sent_sem.at[k, off],
            recv_sem=got_sem.at[k, off],
            device_id={"sp": dest},
            device_id_type=pl.DeviceIdType.MESH,
        )

    def keeping(k):
        return pltpu.make_async_copy(sent_ref.at[k, me], got_ref.at[k, me], got_sem.at[k, 0])

    block = per_src * n_chan

    def part_of(k, dest):
        return done_ref.at[k, pl.ds(pl.multiple_of(dest * block, block), block), :]

    def returning(k, off):
        dest = lax.rem(me + off, n_dev)
        return pltpu.make_async_remote_copy(
            src_ref=part_of(k, dest),
            dst_ref=back_ref.at[k, me],
            send_sem=done_sem.at[k, off],
            recv_sem=back_sem.at[k, off],
            device_id={"sp": dest},
            device_id_type=pl.DeviceIdType.MESH,
        )

    def storing(k):
        return pltpu.make_async_copy(part_of(k, me), back_ref.at[k, me], done_sem.at[k, 0])

    @pl.loop(0, n_chunks)
    def _(k):
        own_share(k).start()
        keeping(k).start()
        for off in range(1, n_groups):
            sharing(k, off).start()
        for off in range(1, n_dev):
            sending(k, off).start()

    @pl.loop(0, n_chunks)
    def _(k):
        all_shares(k).wait()
        keeping(k).wait()
        for off in range(1, n_dev):
            sending(k, off).wait_recv()

        @pl.loop(0, n_chan // group)
        def _(i):
            first = i * group

            def load_h(which, g):
                start = pl.multiple_of((which * n_chan + first + g) * per_src, per_src)
                return filt_ref[k, :, pl.ds(start, per_src), :].reshape(n_high, LANES)

            def load_x(which, g):
                start = pl.multiple_of((first + g) * per_src, per_src)
                return got_ref[k, :, which, pl.ds(start, per_src), :].reshape(n_high, LANES)

            chan = me * LANES + k * n_chan + first
            spec_one_ref[...] = spectrum([load_h(0, g) for g in range(group)], False)
            spec_two_ref[...] = spectrum([load_h(1, g) for g in range(group)], False)
            values = [load_x(0, g) for g in range(group)]
            conv = signal(spectrum(values, True), spec_one_ref)
            gated = [load_x(1, g) * (conv[g] + skip_one_ref[chan + g] * values[g]) for g in range(group)]
            conv = signal(spectrum(gated, False), spec_two_ref)
            for g in range(group):
                done_ref[k, pl.ds(first + g, n_high, stride=n_chan), :] = conv[g] + skip_two_ref[chan + g] * gated[g]

        storing(k).start()
        for off in range(1, n_dev):
            returning(k, off).start()

    @pl.loop(0, n_chunks)
    def _(k):
        for off in range(1, n_dev):
            sending(k, off).wait_send()
            returning(k, off).wait()
        storing(k).wait()
        for off in range(1, n_groups):
            sharing(k, off).wait_send()


def exchange(skip_one, skip_two, share, sent, tables, n_dev, n_groups, group=4):
    n_chunks, _, _, chunk_rows, _ = sent.shape
    n_high = tables[-1].shape[1]
    n_chan = chunk_rows // (n_high // n_dev)
    any_spec = pl.BlockSpec(memory_space=pl.ANY)
    vmem_spec = pl.BlockSpec(memory_space=pltpu.VMEM)
    return pl.pallas_call(
        functools.partial(exchange_body, n_dev, n_groups, group),
        in_specs=[pl.BlockSpec(memory_space=pltpu.SMEM)] * 2 + [any_spec, any_spec] + [vmem_spec] * len(tables),
        out_specs=any_spec,
        out_shape=jax.ShapeDtypeStruct((n_chunks, n_dev, chunk_rows, LANES), F32),
        scratch_shapes=[
            pltpu.VMEM((n_chunks, n_dev, 2, chunk_rows, LANES), F32),
            pltpu.VMEM((n_chunks, n_dev, 2 * chunk_rows, LANES), F32),
            pltpu.VMEM((n_chunks, n_high * n_chan, LANES), F32),
            pltpu.VMEM((group * n_high, 6 * LANES), BF16),
            pltpu.VMEM((group * n_high, 2 * LANES), F32),
            pltpu.VMEM((group * n_high, 2 * LANES), F32),
            pltpu.SemaphoreType.DMA((n_chunks, n_dev)),
            pltpu.SemaphoreType.DMA((n_chunks, n_dev)),
            pltpu.SemaphoreType.DMA((n_chunks,)),
            pltpu.SemaphoreType.DMA((n_chunks,)),
            pltpu.SemaphoreType.DMA((n_chunks, n_dev)),
            pltpu.SemaphoreType.DMA((n_chunks, n_dev)),
        ],
        cost_estimate=pl.CostEstimate(flops=10**11, bytes_accessed=40 * 2**20, transcendentals=0),
        compiler_params=pltpu.CompilerParams(collective_id=1, has_side_effects=True, vmem_limit_bytes=60 * 2**20),
        name="exchange",
    )(skip_one, skip_two, share, sent, *tables)


def finish_body(gate_ref, u_ref, w_ref, back_ref, out_ref, y_ref):
    n_chunks, n_src, n_rows, _, _ = back_ref.shape
    for r in range(n_rows):
        for s in range(n_src):
            full = jnp.concatenate([back_ref[k, s, r] for k in range(n_chunks)], axis=0)
            rows, cols = slice(r * LANES, (r + 1) * LANES), slice(s * LANES, (s + 1) * LANES)
            y_ref[rows, cols] = (gate_ref[rows, cols].astype(F32) * full.T).astype(BF16)
    out_ref[...] = (u_ref[...].astype(F32) + dot32(y_ref[...], w_ref[...])).astype(BF16)


def finish(gate, u, w_out, back, n_rows=2):
    rows, model = u.shape
    n_chunks, n_src, _, per_chunk, _ = back.shape
    tile = n_rows * LANES
    return pl.pallas_call(
        finish_body,
        grid=(rows // tile,),
        in_specs=[
            pl.BlockSpec((tile, model), lambda i: (i, 0)),
            pl.BlockSpec((tile, model), lambda i: (i, 0)),
            pl.BlockSpec(w_out.shape, lambda i: (0, 0)),
            pl.BlockSpec((n_chunks, n_src, n_rows, per_chunk, LANES), lambda i: (0, 0, i, 0, 0)),
        ],
        out_specs=pl.BlockSpec((tile, model), lambda i: (i, 0)),
        out_shape=jax.ShapeDtypeStruct((rows, model), BF16),
        scratch_shapes=[pltpu.VMEM((tile, model), BF16)],
        cost_estimate=pl.CostEstimate(flops=2 * rows * model * model, bytes_accessed=20 * 2**20, transcendentals=0),
        compiler_params=pltpu.CompilerParams(dimension_semantics=("arbitrary",), vmem_limit_bytes=48 * 2**20),
        name="finish",
    )(gate, u, w_out, back)


def solution(mesh):
    n_dev, n_groups = mesh.shape["sp"], mesh.shape["dp"]
    n_chunks = 8
    n_chan = LANES // n_chunks
    if (2 * n_chan) % n_groups:
        raise ValueError("uneven groups")
    units = 2 * n_chan // n_groups
    def local_step(u_in, w_in, b_in, conv_taps, w_out, skip_one, skip_two, filt_one, filt_two):
        u = u_in[0]
        rows = u.shape[0]
        tables = [jnp.asarray(t) for t in transform_tables(rows * n_dev)]
        sent, gate, share = project(u, filt_one, filt_two, w_in, b_in[None], conv_taps, n_dev, n_groups, n_chunks, units)
        back = exchange(skip_one, skip_two, share, sent, tables, n_dev, n_groups)
        back = back.reshape(n_chunks, n_dev, rows // LANES, LANES // n_chunks, LANES)
        return finish(gate, u, w_out, back)[None]

    seq_spec = P("dp", "sp", None)
    filt_spec = P("sp", None)
    return jax.shard_map(
        local_step,
        mesh=mesh,
        in_specs=(seq_spec, P(), P(), P(), P(), P(), P(), filt_spec, filt_spec),
        out_specs=seq_spec,
        check_vma=False,
    )
```

```python
import functools
import math
import jax
import jax.numpy as jnp
import numpy as np
from jax import lax
from jax.experimental import pallas as pl
from jax.experimental.pallas import tpu as pltpu
from jax.sharding import PartitionSpec as P

LANES = 128
F32 = jnp.float32
BF16 = jnp.bfloat16


def split_table(table, n_parts=3):
    parts, rest = [], np.asarray(table, np.float64)
    for _ in range(n_parts):
        part = rest.astype(jnp.bfloat16)
        parts.append(part)
        rest = rest - part.astype(np.float64)
    return parts


def transform_tables(seq_len):
    n_high = seq_len // LANES
    quarter = np.arange(n_high)[:, None] + 0.25
    high = 2.0 * np.pi * quarter * np.arange(n_high)[None, :] / n_high
    twist = 2.0 * np.pi * quarter * np.arange(LANES)[None, :] / seq_len
    low = 2.0 * np.pi * np.outer(np.arange(LANES), np.arange(LANES)) / LANES
    first = np.concatenate([np.cos(high), -np.sin(high)], axis=0)
    last = np.concatenate([np.cos(high.T), -np.sin(high.T)], axis=1)
    er, ei = np.cos(low), -np.sin(low)
    fwd = np.block([[er, ei], [-ei, er]])
    inv = np.block([[er, -ei], [ei, er]])
    a, b, c = split_table(first)
    first_wide = np.concatenate([a, a, a, b, b, c], axis=1)
    first_thin = np.concatenate([a, b, c], axis=1)
    fwd_parts = np.concatenate(split_table(fwd), axis=0)
    inv_parts = np.concatenate(split_table(inv), axis=0)
    last_parts = np.concatenate(split_table(last), axis=0)
    twist_tab = np.stack([np.cos(twist), -np.sin(twist)]).astype(np.float32)
    return first_wide, first_thin, fwd_parts, inv_parts, last_parts, twist_tab


def split3(x):
    hi = x.astype(BF16)
    rest = x - hi.astype(F32)
    mid = rest.astype(BF16)
    low = (rest - mid.astype(F32)).astype(BF16)
    return hi, mid, low


def dot32(a, b):
    return jnp.dot(a, b, preferred_element_type=F32)


def turn_rows(block, into_ref, n_chunks, row, n_rows):
    turned = block.T
    n_chan = LANES // n_chunks
    for k in range(n_chunks):
        into_ref[k, pl.ds(row, n_chan, stride=n_rows), :] = turned[k * n_chan : (k + 1) * n_chan]


def spread_offsets(n_dev):
    pairs = [off for near in range(2, n_dev, 4) for off in (near, n_dev - near)]
    rest = [off for off in range(1, n_dev) if off not in pairs]
    rest.sort(key=lambda off: -min(off, n_dev - off))
    order = list(dict.fromkeys(pairs)) + rest
    return order


def share_filters(n_dev, n_groups, n_chunks, units, filt_refs, u_hbm_ref, u_ref, share_ref, halo_ref, tail_ref, stage_ref, hold_ref, full_ref, sems):
    stage_sem, sent_sem, share_sem, halo_sem, u_sem = sems
    me, my_group = lax.axis_index("sp"), lax.axis_index("dp")
    rows = stage_ref.shape[1]
    n_rows = rows // LANES
    n_chan = LANES // n_chunks
    first_unit = my_group * units
    which_mine = first_unit // n_chan
    both = units == 2 * n_chan
    items = [(off, which) for off in spread_offsets(n_dev) + [0] for which in ((0, 1) if both else (None,))]

    def target(off):
        return lax.rem(me + off, n_dev)

    def loading(item, which):
        cols = pl.ds(pl.multiple_of(target(items[item][0]) * LANES, LANES), LANES)
        return pltpu.make_async_copy(filt_refs[which].at[:, cols], stage_ref.at[item % 2], stage_sem.at[item % 2])

    def load(item):
        if both:
            loading(item, items[item][1]).start()
            return
        for which in range(2):

            @pl.when(which_mine == which)
            def _():
                loading(item, which).start()

    tail_rows = u_ref.at[pl.ds(rows - 16, 16), :]
    tail_copy = pltpu.make_async_copy(u_hbm_ref.at[pl.ds(rows - 16, 16), :], tail_rows, u_sem.at[1])
    head_copy = u_head(u_hbm_ref, u_ref, u_sem)
    barrier = pltpu.get_barrier_semaphore()
    for off in range(1, n_dev):
        pl.semaphore_signal(barrier, inc=1, device_id={"sp": target(off)}, device_id_type=pl.DeviceIdType.MESH)
    load(0)
    tail_copy.start()
    for item, (off, which) in enumerate(items):
        if item + 1 < len(items):
            load(item + 1)
        if item == 0:
            head_copy.start()
        loading(item, 0).wait()
        dest = target(off)
        into = hold_ref.at[dest] if units >= n_chan else full_ref
        base = n_chan * n_rows if which == 1 else 0
        together = math.gcd(n_rows, 4)

        @pl.loop(0, n_rows // together)
        def _(i):
            for j in range(together):
                r = i * together + j
                turn_rows(stage_ref[item % 2, pl.ds(pl.multiple_of(r * LANES, LANES), LANES), :], into, n_chunks, base + r, n_rows)

        if units < n_chan:
            start = pl.multiple_of(lax.rem(first_unit, n_chan) * n_rows, n_rows)
            hold_ref[dest] = full_ref[:, pl.ds(start, units * n_rows), :]
        if item == 0:
            tail_copy.wait()
            tail_ref[...] = tail_rows[...].astype(F32)[8:]
            pl.semaphore_wait(barrier, n_dev - 1)
            halo_send(target, tail_ref, halo_ref, halo_sem).start()
        if off and which != 0:
            share_send(me, target, hold_ref, share_ref, sent_sem, share_sem, off).start()
    pltpu.make_async_copy(hold_ref.at[me], share_ref.at[me], sent_sem.at[0]).start()


def u_head(u_hbm_ref, u_ref, u_sem):
    rows = u_ref.shape[0] - 16
    return pltpu.make_async_copy(u_hbm_ref.at[pl.ds(0, rows), :], u_ref.at[pl.ds(0, rows), :], u_sem.at[0])


def share_send(me, target, hold_ref, share_ref, sent_sem, share_sem, off):
    dest = target(off)
    return pltpu.make_async_remote_copy(
        src_ref=hold_ref.at[dest],
        dst_ref=share_ref.at[me],
        send_sem=sent_sem.at[off],
        recv_sem=share_sem.at[off],
        device_id={"sp": dest},
        device_id_type=pl.DeviceIdType.MESH,
    )


def halo_send(target, tail_ref, halo_ref, halo_sem):
    return pltpu.make_async_remote_copy(
        src_ref=tail_ref,
        dst_ref=halo_ref,
        send_sem=halo_sem.at[0],
        recv_sem=halo_sem.at[1],
        device_id={"sp": target(1)},
        device_id_type=pl.DeviceIdType.MESH,
    )


def project_body(n_dev, n_groups, n_chunks, units, u_hbm_ref, one_ref, two_ref, *refs):
    w_refs, b_refs, tap_refs = refs[:3], refs[3:6], refs[6:9]
    sent_ref, gate_ref, share_ref, u_ref, p_ref, halo_ref, tail_ref, stage_ref, hold_ref, full_ref, *sems = refs[9:]
    stage_sem, sent_sem, share_sem, halo_sem, u_sem = sems
    rows = u_ref.shape[0]
    n_rows = rows // LANES
    width = w_refs[0].shape[1]
    me = lax.axis_index("sp")
    step_idx = pl.program_id(0)

    def target(off):
        return lax.rem(me + off, n_dev)

    @pl.when(step_idx == 0)
    def _():
        share_filters(n_dev, n_groups, n_chunks, units, (one_ref, two_ref), u_hbm_ref, u_ref, share_ref, halo_ref, tail_ref, stage_ref, hold_ref, full_ref, sems)
        u_head(u_hbm_ref, u_ref, u_sem).wait()
        halo_send(target, tail_ref, halo_ref, halo_sem).wait()

    for which in range(3):
        w = w_refs[which][...]
        bias = b_refs[which][...]
        halo = (dot32(halo_ref[...].astype(BF16), w) + bias).astype(BF16).astype(F32)
        p_ref[0:8, :] = jnp.where(me > 0, halo, 0.0)
        step = 2 * LANES

        @pl.loop(0, rows // step)
        def _(i):
            start = pl.multiple_of(i * step, step)
            proj = dot32(u_ref[pl.ds(start, step), :], w) + bias
            p_ref[pl.ds(start + 8, step), :] = proj.astype(BF16).astype(F32)

        c0, c1, c2 = (tap_refs[which][t : t + 1, :] for t in range(3))

        @pl.loop(0, n_rows)
        def _(r):
            start = pl.multiple_of(r * LANES, LANES)
            window = p_ref[pl.ds(start, LANES + 8), :]
            mixed = c0 * window[8:] + c1 * window[7:-1] + c2 * window[6:-2]
            mixed = mixed.astype(BF16)
            if which == 1:
                gate_ref[pl.ds(start, LANES), :] = mixed
            else:
                slot = 1 if which == 0 else 0
                for d in range(width // LANES):
                    block = mixed[:, d * LANES : (d + 1) * LANES].astype(F32)
                    turn_rows(block, sent_ref.at[:, d, slot], n_chunks, r, n_rows)

    @pl.when(step_idx == pl.num_programs(0) - 1)
    def _():
        pltpu.make_async_copy(hold_ref.at[me], share_ref.at[me], sent_sem.at[0]).wait()
        for off in range(1, n_dev):
            share_send(me, target, hold_ref, share_ref, sent_sem, share_sem, off).wait()


def project(u, filt_one, filt_two, w_in, b_in, taps, n_dev, n_groups, n_chunks, units):
    rows, depth = u.shape
    model = w_in.shape[1] // 3
    width = 2 * LANES
    steps = model // width
    n_rows = rows // LANES
    n_chan = LANES // n_chunks
    chunk_rows = n_chan * n_rows
    any_spec = pl.BlockSpec(memory_space=pl.ANY)

    def third(height):
        return [pl.BlockSpec((height, width), functools.partial(lambda off, j: (0, off + j), t * steps)) for t in range(3)]

    full_shape = (n_chunks, chunk_rows, LANES) if units < n_chan else (1, 8, LANES)
    return pl.pallas_call(
        functools.partial(project_body, n_dev, n_groups, n_chunks, units),
        grid=(steps,),
        in_specs=[any_spec, any_spec, any_spec, *third(depth), *third(1), *third(3)],
        out_specs=[
            pl.BlockSpec((n_chunks, 2, 2, chunk_rows, LANES), lambda j: (0, j, 0, 0, 0)),
            pl.BlockSpec((rows, width), lambda j: (0, j)),
            any_spec,
        ],
        out_shape=[
            jax.ShapeDtypeStruct((n_chunks, n_dev, 2, chunk_rows, LANES), F32),
            jax.ShapeDtypeStruct((rows, model), BF16),
            jax.ShapeDtypeStruct((n_dev, n_chunks, units * n_rows, LANES), F32),
        ],
        scratch_shapes=[
            pltpu.VMEM((rows, depth), BF16),
            pltpu.VMEM((rows + 8, width), F32),
            pltpu.VMEM((8, depth), F32),
            pltpu.VMEM((8, depth), F32),
            pltpu.VMEM((2, rows, LANES), F32),
            pltpu.VMEM((n_dev, n_chunks, units * n_rows, LANES), F32),
            pltpu.VMEM(full_shape, F32),
            pltpu.SemaphoreType.DMA((2,)),
            pltpu.SemaphoreType.DMA((n_dev,)),
            pltpu.SemaphoreType.DMA((n_dev,)),
            pltpu.SemaphoreType.DMA((2,)),
            pltpu.SemaphoreType.DMA((2,)),
        ],
        cost_estimate=pl.CostEstimate(flops=2 * rows * depth * 3 * model, bytes_accessed=50 * 2**20, transcendentals=0),
        compiler_params=pltpu.CompilerParams(
            dimension_semantics=("arbitrary",), collective_id=0, has_side_effects=True, vmem_limit_bytes=60 * 2**20
        ),
        name="project",
    )(u, filt_one, filt_two, w_in, w_in, w_in, b_in, b_in, b_in, taps, taps, taps)


def spectrum_tools(group, n_high, tables, parts_ref):
    wide_ref, thin_ref, fwd_ref, inv_ref, last_ref, twist_ref = tables
    wide = 2 * LANES
    scale = 1.0 / (n_high * LANES)

    def complex_dot(tab_ref):
        return (
            dot32(parts_ref[:, 2 * wide :], tab_ref[:wide])
            + dot32(parts_ref[:, wide : 2 * wide], tab_ref[:wide])
            + dot32(parts_ref[:, :wide], tab_ref[wide : 2 * wide])
            + dot32(parts_ref[:, wide : 2 * wide], tab_ref[wide : 2 * wide])
            + dot32(parts_ref[:, :wide], tab_ref[2 * wide :])
            + dot32(parts_ref[:, :wide], tab_ref[:wide])
        )

    def store_parts(g, real, imag):
        for t, (re, im) in enumerate(zip(split3(real), split3(imag))):
            parts_ref[g * n_high : (g + 1) * n_high, 2 * t * LANES : (2 * t + 1) * LANES] = re
            parts_ref[g * n_high : (g + 1) * n_high, (2 * t + 1) * LANES : (2 * t + 2) * LANES] = im

    def spectrum(signals, exact):
        tr, ti = twist_ref[0], twist_ref[1]
        for g in range(0, group, 2):
            pair = jnp.concatenate([signals[g], signals[g + 1]], axis=1)
            if exact:
                short = pair.astype(BF16)
                coarse = dot32(thin_ref[...], jnp.concatenate([short, short, short], axis=0))
            else:
                hi, mid, low = split3(pair)
                coarse = dot32(wide_ref[...], jnp.concatenate([hi, mid, low, hi, mid, hi], axis=0))
            for j in range(2):
                re = coarse[:n_high, j * LANES : (j + 1) * LANES]
                im = coarse[n_high:, j * LANES : (j + 1) * LANES]
                store_parts(g + j, re * tr - im * ti, re * ti + im * tr)
        return complex_dot(fwd_ref)

    def signal(spec_a, spec_b):
        tr, ti = twist_ref[0], twist_ref[1]
        for g in range(group):
            rows = slice(g * n_high, (g + 1) * n_high)
            ar, ai = spec_a[rows, :LANES], spec_a[rows, LANES:]
            br, bi = spec_b[rows, :LANES], spec_b[rows, LANES:]
            store_parts(g, ar * br - ai * bi, ar * bi + ai * br)
        fine = complex_dot(inv_ref)
        results = []
        for g in range(0, group, 2):
            halves = []
            for j in range(2):
                rows = slice((g + j) * n_high, (g + j + 1) * n_high)
                re, im = fine[rows, :LANES] * scale, fine[rows, LANES:] * scale
                halves.append(jnp.concatenate([re * tr + im * ti, im * tr - re * ti], axis=0))
            hi, mid, low = split3(jnp.concatenate(halves, axis=1))
            d_hi = dot32(last_ref[...], hi)
            d_mid = dot32(last_ref[: 2 * n_high], mid)
            d_low = dot32(last_ref[:n_high], low)
            small = d_hi[2 * n_high :] + d_mid[n_high:] + d_low
            total = d_hi[:n_high] + ((d_hi[n_high : 2 * n_high] + d_mid[:n_high]) + small)
            results += [total[:, :LANES], total[:, LANES:]]
        return results

    return spectrum, signal


def exchange_body(n_dev, n_groups, group, skip_one_ref, skip_two_ref, share_ref, sent_ref, wide_ref, thin_ref, fwd_ref, inv_ref, last_ref, twist_ref, back_ref, got_ref, filt_ref, done_ref, parts_ref, spec_one_ref, spec_two_ref, sent_sem, got_sem, share_sem, filt_sem, back_sem, done_sem):
    n_chunks, _, _, chunk_rows, _ = sent_ref.shape
    n_high = twist_ref.shape[1]
    per_src = n_high // n_dev
    n_chan = chunk_rows // per_src
    me, my_group = lax.axis_index("sp"), lax.axis_index("dp")
    share_rows = share_ref.shape[2]
    spectrum, signal = spectrum_tools(group, n_high, (wide_ref, thin_ref, fwd_ref, inv_ref, last_ref, twist_ref), parts_ref)

    barrier = pltpu.get_barrier_semaphore()
    for off in range(1, n_dev):
        pl.semaphore_signal(barrier, inc=1, device_id={"sp": lax.rem(me + off, n_dev)}, device_id_type=pl.DeviceIdType.MESH)
    for off in range(1, n_groups):
        pl.semaphore_signal(barrier, inc=1, device_id={"dp": lax.rem(my_group + off, n_groups)}, device_id_type=pl.DeviceIdType.MESH)
    pl.semaphore_wait(barrier, n_dev + n_groups - 2)

    def sharing(k, off):
        return pltpu.make_async_remote_copy(
            src_ref=share_ref.at[:, k],
            dst_ref=share_of(k),
            send_sem=share_sem.at[k],
            recv_sem=filt_sem.at[k],
            device_id={"dp": lax.rem(my_group + off, n_groups)},
            device_id_type=pl.DeviceIdType.MESH,
        )

    def share_of(k):
        return filt_ref.at[k, :, pl.ds(pl.multiple_of(my_group * share_rows, share_rows), share_rows), :]

    def own_share(k):
        return pltpu.make_async_copy(share_ref.at[:, k], share_of(k), filt_sem.at[k])

    def all_shares(k):
        return pltpu.make_async_copy(filt_ref.at[k], filt_ref.at[k], filt_sem.at[k])

    def sending(k, off):
        dest = lax.rem(me + off, n_dev)
        return pltpu.make_async_remote_copy(
            src_ref=sent_ref.at[k, dest],
            dst_ref=got_ref.at[k, me],
            send_sem=sent_sem.at[k, off],
            recv_sem=got_sem.at[k, off],
            device_id={"sp": dest},
            device_id_type=pl.DeviceIdType.MESH,
        )

    def keeping(k):
        return pltpu.make_async_copy(sent_ref.at[k, me], got_ref.at[k, me], got_sem.at[k, 0])

    block = per_src * n_chan

    def part_of(k, dest):
        return done_ref.at[k, pl.ds(pl.multiple_of(dest * block, block), block), :]

    def returning(k, off):
        dest = lax.rem(me + off, n_dev)
        return pltpu.make_async_remote_copy(
            src_ref=part_of(k, dest),
            dst_ref=back_ref.at[k, me],
            send_sem=done_sem.at[k, off],
            recv_sem=back_sem.at[k, off],
            device_id={"sp": dest},
            device_id_type=pl.DeviceIdType.MESH,
        )

    def storing(k):
        return pltpu.make_async_copy(part_of(k, me), back_ref.at[k, me], done_sem.at[k, 0])

    @pl.loop(0, n_chunks)
    def _(k):
        own_share(k).start()
        keeping(k).start()
        for off in range(1, n_groups):
            sharing(k, off).start()
        for off in range(1, n_dev):
            sending(k, off).start()

    @pl.loop(0, n_chunks)
    def _(k):
        all_shares(k).wait()
        keeping(k).wait()
        for off in range(1, n_dev):
            sending(k, off).wait_recv()

        @pl.loop(0, n_chan // group)
        def _(i):
            first = i * group

            def load_h(which, g):
                start = pl.multiple_of((which * n_chan + first + g) * per_src, per_src)
                return filt_ref[k, :, pl.ds(start, per_src), :].reshape(n_high, LANES)

            def load_x(which, g):
                start = pl.multiple_of((first + g) * per_src, per_src)
                return got_ref[k, :, which, pl.ds(start, per_src), :].reshape(n_high, LANES)

            chan = me * LANES + k * n_chan + first
            spec_one_ref[...] = spectrum([load_h(0, g) for g in range(group)], False)
            spec_two_ref[...] = spectrum([load_h(1, g) for g in range(group)], False)
            values = [load_x(0, g) for g in range(group)]
            conv = signal(spectrum(values, True), spec_one_ref)
            gated = [load_x(1, g) * (conv[g] + skip_one_ref[chan + g] * values[g]) for g in range(group)]
            conv = signal(spectrum(gated, False), spec_two_ref)
            for g in range(group):
                done_ref[k, pl.ds(first + g, n_high, stride=n_chan), :] = conv[g] + skip_two_ref[chan + g] * gated[g]

        storing(k).start()
        for off in range(1, n_dev):
            returning(k, off).start()

    @pl.loop(0, n_chunks)
    def _(k):
        for off in range(1, n_dev):
            sending(k, off).wait_send()
            returning(k, off).wait()
        storing(k).wait()
        for off in range(1, n_groups):
            sharing(k, off).wait_send()


def exchange(skip_one, skip_two, share, sent, tables, n_dev, n_groups, group=4):
    n_chunks, _, _, chunk_rows, _ = sent.shape
    n_high = tables[-1].shape[1]
    n_chan = chunk_rows // (n_high // n_dev)
    any_spec = pl.BlockSpec(memory_space=pl.ANY)
    vmem_spec = pl.BlockSpec(memory_space=pltpu.VMEM)
    return pl.pallas_call(
        functools.partial(exchange_body, n_dev, n_groups, group),
        in_specs=[pl.BlockSpec(memory_space=pltpu.SMEM)] * 2 + [any_spec, any_spec] + [vmem_spec] * len(tables),
        out_specs=any_spec,
        out_shape=jax.ShapeDtypeStruct((n_chunks, n_dev, chunk_rows, LANES), F32),
        scratch_shapes=[
            pltpu.VMEM((n_chunks, n_dev, 2, chunk_rows, LANES), F32),
            pltpu.VMEM((n_chunks, n_dev, 2 * chunk_rows, LANES), F32),
            pltpu.VMEM((n_chunks, n_high * n_chan, LANES), F32),
            pltpu.VMEM((group * n_high, 6 * LANES), BF16),
            pltpu.VMEM((group * n_high, 2 * LANES), F32),
            pltpu.VMEM((group * n_high, 2 * LANES), F32),
            pltpu.SemaphoreType.DMA((n_chunks, n_dev)),
            pltpu.SemaphoreType.DMA((n_chunks, n_dev)),
            pltpu.SemaphoreType.DMA((n_chunks,)),
            pltpu.SemaphoreType.DMA((n_chunks,)),
            pltpu.SemaphoreType.DMA((n_chunks, n_dev)),
            pltpu.SemaphoreType.DMA((n_chunks, n_dev)),
        ],
        cost_estimate=pl.CostEstimate(flops=10**11, bytes_accessed=40 * 2**20, transcendentals=0),
        compiler_params=pltpu.CompilerParams(collective_id=1, has_side_effects=True, vmem_limit_bytes=50 * 2**20),
        name="exchange",
    )(skip_one, skip_two, share, sent, *tables)


def finish_body(gate_ref, all_back_ref, u_ref, w_ref, out_ref, y_ref, back_bufs, back_sem):
    _, n_chunks, n_src, n_rows, _, _ = back_bufs.shape
    step = pl.program_id(0)

    def fetch(idx, slot):
        rows = pl.ds(pl.multiple_of(idx * n_rows, n_rows), n_rows)
        return pltpu.make_async_copy(all_back_ref.at[:, :, rows], back_bufs.at[slot], back_sem.at[slot])

    def gather(slot):
        back_ref = back_bufs.at[slot]
        for r in range(n_rows):
            for s in range(n_src):
                full = jnp.concatenate([back_ref[k, s, r] for k in range(n_chunks)], axis=0)
                rows, cols = slice(r * LANES, (r + 1) * LANES), slice(s * LANES, (s + 1) * LANES)
                y_ref[slot, rows, cols] = (gate_ref[rows, cols].astype(F32) * full.T).astype(BF16)

    def emit(slot):
        out_ref[...] = (u_ref[...].astype(F32) + dot32(y_ref[slot], w_ref[...])).astype(BF16)

    last = pl.num_programs(0) - 1

    @pl.when(step == 0)
    def _():
        fetch(0, 0).start()

    for slot in range(2):
        mine = lax.rem(step, 2) == slot

        @pl.when(jnp.logical_and(mine, step + 1 < last))
        def _():
            fetch(step + 1, 1 - slot).start()

        @pl.when(jnp.logical_and(mine, step < last))
        def _():
            fetch(step, slot).wait()

        @pl.when(jnp.logical_and(mine, jnp.logical_and(step > 0, step < last)))
        def _():
            gather(slot)
            emit(1 - slot)

    @pl.when(step == 0)
    def _():
        gather(0)

    @pl.when(step == last)
    def _():
        emit((last - 1) % 2)


def finish(gate, u, w_out, back, n_rows=2):
    rows, model = u.shape
    n_chunks, n_src, _, per_chunk, _ = back.shape
    tile = n_rows * LANES
    steps = rows // tile

    def now(i):
        return jnp.minimum(i, steps - 1)

    def before(i):
        return jnp.maximum(i - 1, 0)

    return pl.pallas_call(
        finish_body,
        grid=(steps + 1,),
        in_specs=[
            pl.BlockSpec((tile, model), lambda i: (now(i), 0)),
            pl.BlockSpec(memory_space=pltpu.HBM),
            pl.BlockSpec((tile, model), lambda i: (before(i), 0)),
            pl.BlockSpec(w_out.shape, lambda i: (0, 0)),
        ],
        out_specs=pl.BlockSpec((tile, model), lambda i: (before(i), 0)),
        out_shape=jax.ShapeDtypeStruct((rows, model), BF16),
        scratch_shapes=[
            pltpu.VMEM((2, tile, model), BF16),
            pltpu.VMEM((2, n_chunks, n_src, n_rows, per_chunk, LANES), F32),
            pltpu.SemaphoreType.DMA((2,)),
        ],
        cost_estimate=pl.CostEstimate(flops=2 * rows * model * model, bytes_accessed=20 * 2**20, transcendentals=0),
        compiler_params=pltpu.CompilerParams(dimension_semantics=("arbitrary",), vmem_limit_bytes=40 * 2**20),
        name="finish",
    )(gate, back, u, w_out)


def solution(mesh):
    n_dev, n_groups = mesh.shape["sp"], mesh.shape["dp"]
    n_chunks = 8
    n_chan = LANES // n_chunks
    if (2 * n_chan) % n_groups:
        raise ValueError("uneven groups")
    units = 2 * n_chan // n_groups
    def local_step(u_in, w_in, b_in, conv_taps, w_out, skip_one, skip_two, filt_one, filt_two):
        u = u_in[0]
        rows = u.shape[0]
        tables = [jnp.asarray(t) for t in transform_tables(rows * n_dev)]
        sent, gate, share = project(u, filt_one, filt_two, w_in, b_in[None], conv_taps, n_dev, n_groups, n_chunks, units)
        back = exchange(skip_one, skip_two, share, sent, tables, n_dev, n_groups)
        back = back.reshape(n_chunks, n_dev, rows // LANES, LANES // n_chunks, LANES)
        return finish(gate, u, w_out, back)[None]

    seq_spec = P("dp", "sp", None)
    filt_spec = P("sp", None)
    return jax.shard_map(
        local_step,
        mesh=mesh,
        in_specs=(seq_spec, P(), P(), P(), P(), P(), P(), filt_spec, filt_spec),
        out_specs=seq_spec,
        check_vma=False,
    )
```

```python
import functools
import math
import jax
import jax.numpy as jnp
import numpy as np
from jax import lax
from jax.experimental import pallas as pl
from jax.experimental.pallas import tpu as pltpu
from jax.sharding import PartitionSpec as P

LANES = 128
F32 = jnp.float32
BF16 = jnp.bfloat16


def split_table(table, n_parts=3):
    parts, rest = [], np.asarray(table, np.float64)
    for _ in range(n_parts):
        part = rest.astype(jnp.bfloat16)
        parts.append(part)
        rest = rest - part.astype(np.float64)
    return parts


def transform_tables(seq_len):
    n_high = seq_len // LANES
    quarter = np.arange(n_high)[:, None] + 0.25
    high = 2.0 * np.pi * quarter * np.arange(n_high)[None, :] / n_high
    twist = 2.0 * np.pi * quarter * np.arange(LANES)[None, :] / seq_len
    low = 2.0 * np.pi * np.outer(np.arange(LANES), np.arange(LANES)) / LANES
    first = np.concatenate([np.cos(high), -np.sin(high)], axis=0)
    last = np.concatenate([np.cos(high.T), -np.sin(high.T)], axis=1)
    er, ei = np.cos(low), -np.sin(low)
    fwd = np.block([[er, ei], [-ei, er]])
    inv = np.block([[er, -ei], [ei, er]])
    a, b, c = split_table(first)
    first_wide = np.concatenate([a, a, a, b, b, c], axis=1)
    first_thin = np.concatenate([a, b, c], axis=1)
    fwd_parts = np.concatenate(split_table(fwd), axis=0)
    inv_parts = np.concatenate(split_table(inv), axis=0)
    last_parts = np.concatenate(split_table(last), axis=0)
    twist_tab = np.stack([np.cos(twist), -np.sin(twist)]).astype(np.float32)
    return first_wide, first_thin, fwd_parts, inv_parts, last_parts, twist_tab


def split3(x):
    hi = x.astype(BF16)
    rest = x - hi.astype(F32)
    mid = rest.astype(BF16)
    low = (rest - mid.astype(F32)).astype(BF16)
    return hi, mid, low


def dot32(a, b):
    return jnp.dot(a, b, preferred_element_type=F32)


def turn_rows(block, into_ref, n_chunks, row, n_rows):
    turned = block.T
    n_chan = LANES // n_chunks
    for k in range(n_chunks):
        into_ref[k, pl.ds(row, n_chan, stride=n_rows), :] = turned[k * n_chan : (k + 1) * n_chan]


def spread_offsets(n_dev):
    pairs = [off for near in range(2, n_dev, 4) for off in (near, n_dev - near)]
    rest = [off for off in range(1, n_dev) if off not in pairs]
    rest.sort(key=lambda off: -min(off, n_dev - off))
    return list(dict.fromkeys(pairs)) + rest


def spectrum_tools(group, n_high, tables, parts_ref):
    wide_ref, thin_ref, fwd_ref, inv_ref, last_ref, twist_ref = tables
    wide = 2 * LANES
    scale = 1.0 / (n_high * LANES)

    def complex_dot(tab_ref):
        return (
            dot32(parts_ref[:, 2 * wide :], tab_ref[:wide])
            + dot32(parts_ref[:, wide : 2 * wide], tab_ref[:wide])
            + dot32(parts_ref[:, :wide], tab_ref[wide : 2 * wide])
            + dot32(parts_ref[:, wide : 2 * wide], tab_ref[wide : 2 * wide])
            + dot32(parts_ref[:, :wide], tab_ref[2 * wide :])
            + dot32(parts_ref[:, :wide], tab_ref[:wide])
        )

    def store_parts(g, real, imag):
        for t, (re, im) in enumerate(zip(split3(real), split3(imag))):
            parts_ref[g * n_high : (g + 1) * n_high, 2 * t * LANES : (2 * t + 1) * LANES] = re
            parts_ref[g * n_high : (g + 1) * n_high, (2 * t + 1) * LANES : (2 * t + 2) * LANES] = im

    def spectrum(signals, exact):
        tr, ti = twist_ref[0], twist_ref[1]
        for g in range(0, group, 2):
            pair = jnp.concatenate([signals[g], signals[g + 1]], axis=1)
            if exact:
                short = pair.astype(BF16)
                coarse = dot32(thin_ref[...], jnp.concatenate([short, short, short], axis=0))
            else:
                hi, mid, low = split3(pair)
                coarse = dot32(wide_ref[...], jnp.concatenate([hi, mid, low, hi, mid, hi], axis=0))
            for j in range(2):
                re = coarse[:n_high, j * LANES : (j + 1) * LANES]
                im = coarse[n_high:, j * LANES : (j + 1) * LANES]
                store_parts(g + j, re * tr - im * ti, re * ti + im * tr)
        return complex_dot(fwd_ref)

    def signal(spec_a, spec_b):
        tr, ti = twist_ref[0], twist_ref[1]
        for g in range(group):
            rows = slice(g * n_high, (g + 1) * n_high)
            ar, ai = spec_a[rows, :LANES], spec_a[rows, LANES:]
            br, bi = spec_b[rows, :LANES], spec_b[rows, LANES:]
            store_parts(g, ar * br - ai * bi, ar * bi + ai * br)
        fine = complex_dot(inv_ref)
        results = []
        for g in range(0, group, 2):
            halves = []
            for j in range(2):
                rows = slice((g + j) * n_high, (g + j + 1) * n_high)
                re, im = fine[rows, :LANES] * scale, fine[rows, LANES:] * scale
                halves.append(jnp.concatenate([re * tr + im * ti, im * tr - re * ti], axis=0))
            hi, mid, low = split3(jnp.concatenate(halves, axis=1))
            d_hi = dot32(last_ref[...], hi)
            d_mid = dot32(last_ref[: 2 * n_high], mid)
            d_low = dot32(last_ref[:n_high], low)
            small = d_hi[2 * n_high :] + d_mid[n_high:] + d_low
            total = d_hi[:n_high] + ((d_hi[n_high : 2 * n_high] + d_mid[:n_high]) + small)
            results += [total[:, :LANES], total[:, LANES:]]
        return results

    return spectrum, signal


def hyena_body(n_dev, n_groups, units, group, u_hbm_ref, one_ref, two_ref, w_hbm_ref, *refs):
    consts_in, refs = refs[:10], refs[10:]
    consts, const_sem, refs = refs[4:14], refs[14], refs[:4] + refs[15:]
    skip_one_ref, skip_two_ref, bias_ref, taps_ref, *tables = consts
    sent_ref, gate_ref, got_ref, back_ref = refs[:4]
    u_ref, w_ref, p_ref, stage_ref, turned_ref, mixed_ref, halo_ref, tail_ref = refs[4:12]
    filt_ref, block_ref, done_ref, parts_ref, spec_one_ref, spec_two_ref = refs[12:18]
    (u_sem, w_sem, stage_sem, out_sem, halo_sem, hold_sem, share_sem, group_sem, filt_sem, sent_sem, got_sem, block_sem, done_sem, back_sem) = refs[18:]
    me, my_group = lax.axis_index("sp"), lax.axis_index("dp")
    rows, depth = u_ref.shape
    n_rows = rows // LANES
    n_chunks = n_dev
    n_chan = LANES // n_chunks
    n_high = n_dev * n_rows
    model = w_hbm_ref.shape[1] // 3
    width = w_ref.shape[2]
    steps = model // width
    share_rows = units * n_rows
    first_unit = my_group * units
    which_mine = first_unit // n_chan
    mesh_id = pl.DeviceIdType.MESH

    def target(off):
        return lax.rem(me + off, n_dev)

    def own_rows(first):
        return pl.ds(pl.multiple_of(first * share_rows, share_rows), share_rows)


    def loading(item, off, which):
        cols = pl.ds(pl.multiple_of(target(off) * LANES, LANES), LANES)
        return pltpu.make_async_copy((one_ref, two_ref)[which].at[:, cols], stage_ref.at[item % 2], stage_sem.at[item % 2])

    def weights(which, step):
        cols = pl.ds(pl.multiple_of(which * model + step * width, width), width)
        slot = lax.rem(which + step, 2)
        return pltpu.make_async_copy(w_hbm_ref.at[:, cols], w_ref.at[slot], w_sem.at[slot])

    def u_part(start, size, idx):
        return pltpu.make_async_copy(u_hbm_ref.at[pl.ds(start, size), :], u_ref.at[pl.ds(start, size), :], u_sem.at[idx])

    def halo_send():
        return pltpu.make_async_remote_copy(tail_ref, halo_ref, halo_sem.at[0], halo_sem.at[1], device_id={"sp": target(1)}, device_id_type=mesh_id)

    def hold_of(dest):
        return done_ref.at[dest, :, pl.ds(0, share_rows), :]

    def share_send(off):
        dest = target(off)
        return pltpu.make_async_remote_copy(
            hold_of(dest), filt_ref.at[:, me, own_rows(my_group), :], hold_sem.at[off], share_sem.at[off], device_id={"sp": dest}, device_id_type=mesh_id
        )

    def group_send(k, off):
        mine = filt_ref.at[k, :, own_rows(my_group), :]
        return pltpu.make_async_remote_copy(
            mine, mine, group_sem.at[k], filt_sem.at[k], device_id={"dp": lax.rem(my_group + off, n_groups)}, device_id_type=mesh_id
        )

    def other_groups(k):
        same_size = filt_ref.at[k, :, pl.ds(0, (n_groups - 1) * share_rows), :]
        return pltpu.make_async_copy(same_size, same_size, filt_sem.at[k])

    def turned_out(slot, step):
        return pltpu.make_async_copy(turned_ref.at[slot], sent_ref.at[:, pl.ds(step * (width // LANES), width // LANES), slot], out_sem.at[slot])

    def mixed_out(step):
        cols = pl.ds(pl.multiple_of(step * width, width), width)
        return pltpu.make_async_copy(mixed_ref, gate_ref.at[:, cols], out_sem.at[2])

    def sending(k, off):
        dest = target(off)
        return pltpu.make_async_remote_copy(
            sent_ref.at[k, dest], got_ref.at[k, me], sent_sem.at[k, off], got_sem.at[k, off], device_id={"sp": dest}, device_id_type=mesh_id
        )

    def block_in(k, off):
        src = lax.rem(me - off + n_dev, n_dev)
        from_ref = got_ref if off else sent_ref
        return pltpu.make_async_copy(from_ref.at[k, src], block_ref.at[src], block_sem.at[off])

    def returning(k, off):
        dest = target(off)
        return pltpu.make_async_remote_copy(
            done_ref.at[k, dest], back_ref.at[k, me], done_sem.at[k, off], back_sem.at[k, off], device_id={"sp": dest}, device_id_type=mesh_id
        )

    def storing(k):
        return pltpu.make_async_copy(done_ref.at[k, me], back_ref.at[k, me], done_sem.at[k, 0])

    def constant(idx):
        return pltpu.make_async_copy(consts_in[idx], consts[idx], const_sem.at[idx])


    barrier = pltpu.get_barrier_semaphore()
    for off in range(1, n_dev):
        pl.semaphore_signal(barrier, inc=1, device_id={"sp": target(off)}, device_id_type=mesh_id)
    for off in range(1, n_groups):
        pl.semaphore_signal(barrier, inc=1, device_id={"dp": lax.rem(my_group + off, n_groups)}, device_id_type=mesh_id)

    order = spread_offsets(n_dev) + [0]

    def load(item):
        for which in range(2):

            @pl.when(which_mine == which)
            def _():
                loading(item, order[item], which).start()

    load(0)
    u_part(rows - 16, 16, 1).start()
    for item, off in enumerate(order):
        if item + 1 < len(order):
            load(item + 1)
        if item == 0:
            u_part(0, rows - 16, 0).start()
            weights(0, 0).start()
            for idx in range(len(consts)):
                constant(idx).start()
        loading(item, off, 0).wait()
        if units < n_chan:
            into = turned_ref.at[0, :, 0]
        elif off:
            into = done_ref.at[target(off)]
        else:
            into = filt_ref.at[:, me, own_rows(my_group), :]
        together = math.gcd(n_rows, 4)

        @pl.loop(0, n_rows // together)
        def _(i):
            for j in range(together):
                r = i * together + j
                turn_rows(stage_ref[item % 2, pl.ds(pl.multiple_of(r * LANES, LANES), LANES), :], into, n_chunks, r, n_rows)

        if units < n_chan:
            start = pl.multiple_of(lax.rem(first_unit, n_chan) * n_rows, n_rows)
            share = turned_ref[0, :, 0, pl.ds(start, share_rows), :]
            if off:
                done_ref[target(off), :, pl.ds(0, share_rows), :] = share
            else:
                filt_ref[:, me, own_rows(my_group), :] = share
        if item == 0:
            u_part(rows - 16, 16, 1).wait()
            tail_ref[...] = u_ref[pl.ds(rows - 16, 16), :].astype(F32)[8:]
            pl.semaphore_wait(barrier, n_dev + n_groups - 2)
            halo_send().start()
        if off:
            share_send(off).start()


    for idx in range(len(consts)):
        constant(idx).wait()
    u_part(0, rows - 16, 0).wait()
    halo_send().wait()

    @pl.loop(0, steps)
    def _(step):
        for which in range(3):
            if which < 2:
                weights(which + 1, step).start()
            else:

                @pl.when(step + 1 < steps)
                def _():
                    weights(0, step + 1).start()

            weights(which, step).wait()
            w_now = w_ref.at[lax.rem(which + step, 2)]
            cols = pl.ds(pl.multiple_of(which * model + step * width, width), width)
            bias = bias_ref[:, cols]
            halo = (dot32(halo_ref[...].astype(BF16), w_now[...]) + bias).astype(BF16).astype(F32)
            p_ref[0:8, :] = jnp.where(me > 0, halo, 0.0)
            tile = 2 * LANES

            @pl.loop(0, rows // tile)
            def _(i):
                start = pl.multiple_of(i * tile, tile)
                proj = dot32(u_ref[pl.ds(start, tile), :], w_now[...]) + bias
                p_ref[pl.ds(start + 8, tile), :] = proj.astype(BF16).astype(F32)

            c0, c1, c2 = (taps_ref[t : t + 1, cols] for t in range(3))
            slot = 1 if which == 0 else 0

            @pl.when(step > 0)
            def _():
                if which == 1:
                    mixed_out(step - 1).wait()
                else:
                    turned_out(slot, step - 1).wait()

            @pl.loop(0, n_rows)
            def _(r):
                start = pl.multiple_of(r * LANES, LANES)
                window = p_ref[pl.ds(start, LANES + 8), :]
                mixed = c0 * window[8:] + c1 * window[7:-1] + c2 * window[6:-2]
                mixed = mixed.astype(BF16)
                if which == 1:
                    mixed_ref[pl.ds(start, LANES), :] = mixed
                else:
                    for d in range(width // LANES):
                        block = mixed[:, d * LANES : (d + 1) * LANES].astype(F32)
                        turn_rows(block, turned_ref.at[slot, :, d], n_chunks, r, n_rows)

            if which == 1:
                mixed_out(step).start()
            else:
                turned_out(slot, step).start()

    turned_out(0, steps - 1).wait()
    turned_out(1, steps - 1).wait()
    mixed_out(steps - 1).wait()

    @pl.loop(0, n_chunks)
    def _(k):
        for off in range(1, n_dev):
            sending(k, off).start()


    for off in range(1, n_dev):
        share_send(off).wait()

    @pl.loop(0, n_chunks)
    def _(k):
        for off in range(1, n_groups):
            group_send(k, off).start()


    spectrum, signal = spectrum_tools(group, n_high, tables, parts_ref)

    @pl.loop(0, n_chunks)
    def _(k):
        block_in(k, 0).start()
        for off in range(1, n_dev):
            sending(k, off).wait_recv()
            block_in(k, off).start()
        other_groups(k).wait()
        for off in range(n_dev):
            block_in(k, off).wait()

        @pl.loop(0, n_chan // group)
        def _(i):
            first = i * group

            def load_h(which, g):
                start = pl.multiple_of((which * n_chan + first + g) * n_rows, n_rows)
                return filt_ref[k, :, pl.ds(start, n_rows), :].reshape(n_high, LANES)

            def load_x(which, g):
                start = pl.multiple_of((first + g) * n_rows, n_rows)
                return block_ref[:, which, pl.ds(start, n_rows), :].reshape(n_high, LANES)

            chan = me * LANES + k * n_chan + first
            spec_one_ref[...] = spectrum([load_h(0, g) for g in range(group)], False)
            spec_two_ref[...] = spectrum([load_h(1, g) for g in range(group)], False)
            values = [load_x(0, g) for g in range(group)]
            conv = signal(spectrum(values, True), spec_one_ref)
            gated = [load_x(1, g) * (conv[g] + skip_one_ref[chan + g] * values[g]) for g in range(group)]
            conv = signal(spectrum(gated, False), spec_two_ref)
            for g in range(group):
                result = conv[g] + skip_two_ref[chan + g] * gated[g]
                done_ref[k, :, pl.ds(first + g, n_rows, stride=n_chan), :] = result.reshape(n_dev, n_rows, LANES)

        storing(k).start()
        for off in range(1, n_dev):
            returning(k, off).start()

    @pl.loop(0, n_chunks)
    def _(k):
        for off in range(1, n_dev):
            sending(k, off).wait_send()
            returning(k, off).wait()
        storing(k).wait()
        for off in range(1, n_groups):
            group_send(k, off).wait_send()


def hyena(skip_one, skip_two, u, filt_one, filt_two, w_in, bias, taps, tables, n_dev, n_groups, units, group=4):
    rows, depth = u.shape
    model = w_in.shape[1] // 3
    width = 2 * LANES
    n_rows = rows // LANES
    n_chunks = n_dev
    n_high = n_dev * n_rows
    chunk_rows = LANES // n_chunks * n_rows
    hbm_spec = pl.BlockSpec(memory_space=pltpu.HBM)
    consts = (bias, taps, *tables)
    dma = pltpu.SemaphoreType.DMA
    return pl.pallas_call(
        functools.partial(hyena_body, n_dev, n_groups, units, group),
        in_specs=[hbm_spec] * (6 + len(consts)),
        out_specs=[hbm_spec] * 4,
        out_shape=[
            jax.ShapeDtypeStruct((n_chunks, n_dev, 2, chunk_rows, LANES), F32),
            jax.ShapeDtypeStruct((rows, model), BF16),
            jax.ShapeDtypeStruct((n_chunks, n_dev, 2, chunk_rows, LANES), F32),
            jax.ShapeDtypeStruct((n_chunks, n_dev, chunk_rows, LANES), F32),
        ],
        scratch_shapes=[
            pltpu.SMEM(skip_one.shape, F32),
            pltpu.SMEM(skip_two.shape, F32),
            *[pltpu.VMEM(c.shape, c.dtype) for c in consts],
            dma((2 + len(consts),)),
            pltpu.VMEM((rows, depth), BF16),
            pltpu.VMEM((2, depth, width), BF16),
            pltpu.VMEM((rows + 8, width), F32),
            pltpu.VMEM((2, rows, LANES), F32),
            pltpu.VMEM((2, n_chunks, width // LANES, chunk_rows, LANES), F32),
            pltpu.VMEM((rows, width), BF16),
            pltpu.VMEM((8, depth), F32),
            pltpu.VMEM((8, depth), F32),
            pltpu.VMEM((n_chunks, n_dev, 2 * chunk_rows, LANES), F32),
            pltpu.VMEM((n_dev, 2, chunk_rows, LANES), F32),
            pltpu.VMEM((n_chunks, n_dev, chunk_rows, LANES), F32),
            pltpu.VMEM((group * n_high, 6 * LANES), BF16),
            pltpu.VMEM((group * n_high, 2 * LANES), F32),
            pltpu.VMEM((group * n_high, 2 * LANES), F32),
            dma((2,)),
            dma((2,)),
            dma((2,)),
            dma((3,)),
            dma((2,)),
            dma((n_dev,)),
            dma((n_dev,)),
            dma((n_chunks,)),
            dma((n_chunks,)),
            dma((n_chunks, n_dev)),
            dma((n_chunks, n_dev)),
            dma((n_dev,)),
            dma((n_chunks, n_dev)),
            dma((n_chunks, n_dev)),
        ],
        cost_estimate=pl.CostEstimate(flops=10**11, bytes_accessed=100 * 2**20, transcendentals=0),
        compiler_params=pltpu.CompilerParams(collective_id=0, has_side_effects=True, vmem_limit_bytes=54 * 2**20),
        name="hyena",
    )(u, filt_one, filt_two, w_in, skip_one, skip_two, *consts)


def finish_body(all_gate_ref, all_back_ref, u_ref, w_ref, out_ref, y_ref, gate_bufs, back_bufs, back_sem):
    _, n_chunks, n_src, n_rows, _, _ = back_bufs.shape
    step = pl.program_id(0)

    def fetch(idx, slot):
        rows = pl.ds(pl.multiple_of(idx * n_rows, n_rows), n_rows)
        tile = pl.ds(pl.multiple_of(idx * n_rows * LANES, n_rows * LANES), n_rows * LANES)
        return (
            pltpu.make_async_copy(all_back_ref.at[:, :, rows], back_bufs.at[slot], back_sem.at[slot, 0]),
            pltpu.make_async_copy(all_gate_ref.at[tile, :], gate_bufs.at[slot], back_sem.at[slot, 1]),
        )

    def gather(slot):
        back_ref, gate_ref = back_bufs.at[slot], gate_bufs.at[slot]
        for r in range(n_rows):
            for s in range(n_src):
                full = jnp.concatenate([back_ref[k, s, r] for k in range(n_chunks)], axis=0)
                rows, cols = slice(r * LANES, (r + 1) * LANES), slice(s * LANES, (s + 1) * LANES)
                y_ref[slot, rows, cols] = (gate_ref[rows, cols].astype(F32) * full.T).astype(BF16)

    def emit(slot):
        out_ref[...] = (u_ref[...].astype(F32) + dot32(y_ref[slot], w_ref[...])).astype(BF16)

    last = pl.num_programs(0) - 1

    @pl.when(step == 0)
    def _():
        for copy in fetch(0, 0):
            copy.start()

    for slot in range(2):
        mine = lax.rem(step, 2) == slot

        @pl.when(jnp.logical_and(mine, step + 1 < last))
        def _():
            for copy in fetch(step + 1, 1 - slot):
                copy.start()

        @pl.when(jnp.logical_and(mine, step < last))
        def _():
            for copy in fetch(step, slot):
                copy.wait()

        @pl.when(jnp.logical_and(mine, jnp.logical_and(step > 0, step < last)))
        def _():
            gather(slot)
            emit(1 - slot)

    @pl.when(step == 0)
    def _():
        gather(0)

    @pl.when(step == last)
    def _():
        emit((last - 1) % 2)


def finish(gate, u, w_out, back, n_rows=2):
    rows, model = u.shape
    n_chunks, n_src, _, per_chunk, _ = back.shape
    tile = n_rows * LANES
    steps = rows // tile

    def before(i):
        return jnp.maximum(i - 1, 0)

    return pl.pallas_call(
        finish_body,
        grid=(steps + 1,),
        in_specs=[
            pl.BlockSpec(memory_space=pltpu.HBM),
            pl.BlockSpec(memory_space=pltpu.HBM),
            pl.BlockSpec((tile, model), lambda i: (before(i), 0)),
            pl.BlockSpec(w_out.shape, lambda i: (0, 0)),
        ],
        out_specs=pl.BlockSpec((tile, model), lambda i: (before(i), 0)),
        out_shape=jax.ShapeDtypeStruct((rows, model), BF16),
        scratch_shapes=[
            pltpu.VMEM((2, tile, model), BF16),
            pltpu.VMEM((2, tile, model), BF16),
            pltpu.VMEM((2, n_chunks, n_src, n_rows, per_chunk, LANES), F32),
            pltpu.SemaphoreType.DMA((2, 2)),
        ],
        cost_estimate=pl.CostEstimate(flops=2 * rows * model * model, bytes_accessed=20 * 2**20, transcendentals=0),
        compiler_params=pltpu.CompilerParams(dimension_semantics=("arbitrary",), vmem_limit_bytes=48 * 2**20),
        name="finish",
    )(gate, back, u, w_out)


def solution(mesh):
    n_dev, n_groups = mesh.shape["sp"], mesh.shape["dp"]
    n_chunks = n_dev
    n_chan = LANES // n_chunks
    if n_groups < 2 or (2 * n_chan) % n_groups:
        raise ValueError("uneven groups")
    units = 2 * n_chan // n_groups

    def local_step(u_in, w_in, b_in, conv_taps, w_out, skip_one, skip_two, filt_one, filt_two):
        u = u_in[0]
        rows = u.shape[0]
        tables = [jnp.asarray(t) for t in transform_tables(rows * n_dev)]
        _, gate, _, back = hyena(skip_one, skip_two, u, filt_one, filt_two, w_in, b_in[None], conv_taps, tables, n_dev, n_groups, units)
        back = back.reshape(n_chunks, n_dev, rows // LANES, LANES // n_chunks, LANES)
        return finish(gate, u, w_out, back)[None]

    seq_spec = P("dp", "sp", None)
    filt_spec = P("sp", None)
    return jax.shard_map(
        local_step,
        mesh=mesh,
        in_specs=(seq_spec, P(), P(), P(), P(), P(), P(), filt_spec, filt_spec),
        out_specs=seq_spec,
        check_vma=False,
    )
```

```python
import functools
import math
import jax
import jax.numpy as jnp
import numpy as np
from jax import lax
from jax.experimental import pallas as pl
from jax.experimental.pallas import tpu as pltpu
from jax.sharding import PartitionSpec as P

LANES = 128
F32 = jnp.float32
BF16 = jnp.bfloat16


def split_table(table, n_parts=3):
    parts, rest = [], np.asarray(table, np.float64)
    for _ in range(n_parts):
        part = rest.astype(jnp.bfloat16)
        parts.append(part)
        rest = rest - part.astype(np.float64)
    return parts


def transform_tables(seq_len):
    n_high = seq_len // LANES
    quarter = np.arange(n_high)[:, None] + 0.25
    high = 2.0 * np.pi * quarter * np.arange(n_high)[None, :] / n_high
    twist = 2.0 * np.pi * quarter * np.arange(LANES)[None, :] / seq_len
    low = 2.0 * np.pi * np.outer(np.arange(LANES), np.arange(LANES)) / LANES
    first = np.concatenate([np.cos(high), -np.sin(high)], axis=0)
    last = np.concatenate([np.cos(high.T), -np.sin(high.T)], axis=1)
    er, ei = np.cos(low), -np.sin(low)
    fwd = np.block([[er, ei], [-ei, er]])
    inv = np.block([[er, -ei], [ei, er]])
    a, b, c = split_table(first)
    first_wide = np.concatenate([a, a, a, b, b, c], axis=1)
    first_thin = np.concatenate([a, b, c], axis=1)
    fwd_parts = np.concatenate(split_table(fwd), axis=0)
    inv_parts = np.concatenate(split_table(inv), axis=0)
    last_parts = np.concatenate(split_table(last), axis=0)
    twist_tab = np.stack([np.cos(twist), -np.sin(twist)]).astype(np.float32)
    return first_wide, first_thin, fwd_parts, inv_parts, last_parts, twist_tab


def split3(x):
    hi = x.astype(BF16)
    rest = x - hi.astype(F32)
    mid = rest.astype(BF16)
    low = (rest - mid.astype(F32)).astype(BF16)
    return hi, mid, low


def dot32(a, b):
    return jnp.dot(a, b, preferred_element_type=F32)


def turn_rows(block, into_ref, n_chunks, row, n_rows):
    turned = block.T
    n_chan = LANES // n_chunks
    for k in range(n_chunks):
        into_ref[k, pl.ds(row, n_chan, stride=n_rows), :] = turned[k * n_chan : (k + 1) * n_chan]


def spread_offsets(n_dev):
    pairs = [off for near in range(2, n_dev, 4) for off in (near, n_dev - near)]
    rest = [off for off in range(1, n_dev) if off not in pairs]
    rest.sort(key=lambda off: -min(off, n_dev - off))
    return list(dict.fromkeys(pairs)) + rest


def spectrum_tools(group, n_high, tables, parts_ref):
    wide_ref, thin_ref, fwd_ref, inv_ref, last_ref, twist_ref = tables
    wide = 2 * LANES
    scale = 1.0 / (n_high * LANES)

    def complex_dot(tab_ref):
        return (
            dot32(parts_ref[:, 2 * wide :], tab_ref[:wide])
            + dot32(parts_ref[:, wide : 2 * wide], tab_ref[:wide])
            + dot32(parts_ref[:, :wide], tab_ref[wide : 2 * wide])
            + dot32(parts_ref[:, wide : 2 * wide], tab_ref[wide : 2 * wide])
            + dot32(parts_ref[:, :wide], tab_ref[2 * wide :])
            + dot32(parts_ref[:, :wide], tab_ref[:wide])
        )

    def store_parts(g, real, imag):
        for t, (re, im) in enumerate(zip(split3(real), split3(imag))):
            parts_ref[g * n_high : (g + 1) * n_high, 2 * t * LANES : (2 * t + 1) * LANES] = re
            parts_ref[g * n_high : (g + 1) * n_high, (2 * t + 1) * LANES : (2 * t + 2) * LANES] = im

    def spectrum(signals, exact):
        tr, ti = twist_ref[0], twist_ref[1]
        for g in range(0, group, 2):
            pair = jnp.concatenate([signals[g], signals[g + 1]], axis=1)
            if exact:
                short = pair.astype(BF16)
                coarse = dot32(thin_ref[...], jnp.concatenate([short, short, short], axis=0))
            else:
                hi, mid, low = split3(pair)
                coarse = dot32(wide_ref[...], jnp.concatenate([hi, mid, low, hi, mid, hi], axis=0))
            for j in range(2):
                re = coarse[:n_high, j * LANES : (j + 1) * LANES]
                im = coarse[n_high:, j * LANES : (j + 1) * LANES]
                store_parts(g + j, re * tr - im * ti, re * ti + im * tr)
        return complex_dot(fwd_ref)

    def signal(spec_a, spec_b):
        tr, ti = twist_ref[0], twist_ref[1]
        for g in range(group):
            rows = slice(g * n_high, (g + 1) * n_high)
            ar, ai = spec_a[rows, :LANES], spec_a[rows, LANES:]
            br, bi = spec_b[rows, :LANES], spec_b[rows, LANES:]
            store_parts(g, ar * br - ai * bi, ar * bi + ai * br)
        fine = complex_dot(inv_ref)
        results = []
        for g in range(0, group, 2):
            halves = []
            for j in range(2):
                rows = slice((g + j) * n_high, (g + j + 1) * n_high)
                re, im = fine[rows, :LANES] * scale, fine[rows, LANES:] * scale
                halves.append(jnp.concatenate([re * tr + im * ti, im * tr - re * ti], axis=0))
            hi, mid, low = split3(jnp.concatenate(halves, axis=1))
            d_hi = dot32(last_ref[...], hi)
            d_mid = dot32(last_ref[: 2 * n_high], mid)
            d_low = dot32(last_ref[:n_high], low)
            small = d_hi[2 * n_high :] + d_mid[n_high:] + d_low
            total = d_hi[:n_high] + ((d_hi[n_high : 2 * n_high] + d_mid[:n_high]) + small)
            results += [total[:, :LANES], total[:, LANES:]]
        return results

    return spectrum, signal


def hyena_body(n_dev, n_groups, units, group, u_hbm_ref, one_ref, two_ref, w_hbm_ref, w_out_ref, *refs):
    consts_in, refs = refs[:10], refs[10:]
    consts, const_sem, refs = refs[5:15], refs[15], refs[:5] + refs[16:]
    skip_one_ref, skip_two_ref, bias_ref, taps_ref, *tables = consts
    sent_ref, gate_ref, got_ref, back_ref, sum_ref = refs[:5]
    u_ref, w_ref, p_ref, stage_ref, turned_ref, mixed_ref, halo_ref, tail_ref = refs[5:13]
    filt_ref, block_ref, done_ref, parts_ref, spec_one_ref, spec_two_ref, gated_ref, w_pair_ref = refs[13:21]
    (u_sem, w_sem, stage_sem, out_sem, halo_sem, hold_sem, share_sem, group_sem, filt_sem, sent_sem, got_sem, block_sem, done_sem, back_sem, pair_sem) = refs[21:]
    me, my_group = lax.axis_index("sp"), lax.axis_index("dp")
    rows, depth = u_ref.shape
    n_rows = rows // LANES
    n_chunks = n_dev
    n_chan = LANES // n_chunks
    n_high = n_dev * n_rows
    model = w_hbm_ref.shape[1] // 3
    width = w_ref.shape[2]
    steps = model // width
    share_rows = units * n_rows
    first_unit = my_group * units
    which_mine = first_unit // n_chan
    mesh_id = pl.DeviceIdType.MESH

    def target(off):
        return lax.rem(me + off, n_dev)

    def own_rows(first):
        return pl.ds(pl.multiple_of(first * share_rows, share_rows), share_rows)


    def loading(item, off, which):
        cols = pl.ds(pl.multiple_of(target(off) * LANES, LANES), LANES)
        return pltpu.make_async_copy((one_ref, two_ref)[which].at[:, cols], stage_ref.at[item % 2], stage_sem.at[item % 2])

    def weights(which, step):
        cols = pl.ds(pl.multiple_of(which * model + step * width, width), width)
        slot = lax.rem(which + step, 2)
        return pltpu.make_async_copy(w_hbm_ref.at[:, cols], w_ref.at[slot], w_sem.at[slot])

    def u_part(start, size, idx):
        return pltpu.make_async_copy(u_hbm_ref.at[pl.ds(start, size), :], u_ref.at[pl.ds(start, size), :], u_sem.at[idx])

    def halo_send():
        return pltpu.make_async_remote_copy(tail_ref, halo_ref, halo_sem.at[0], halo_sem.at[1], device_id={"sp": target(1)}, device_id_type=mesh_id)

    def hold_of(dest):
        return done_ref.at[dest, :, pl.ds(0, share_rows), :]

    def share_send(off):
        dest = target(off)
        return pltpu.make_async_remote_copy(
            hold_of(dest), filt_ref.at[:, me, own_rows(my_group), :], hold_sem.at[off], share_sem.at[off], device_id={"sp": dest}, device_id_type=mesh_id
        )

    def group_send(k, off):
        mine = filt_ref.at[k, :, own_rows(my_group), :]
        return pltpu.make_async_remote_copy(
            mine, mine, group_sem.at[k], filt_sem.at[k], device_id={"dp": lax.rem(my_group + off, n_groups)}, device_id_type=mesh_id
        )

    def other_groups(k):
        same_size = filt_ref.at[k, :, pl.ds(0, (n_groups - 1) * share_rows), :]
        return pltpu.make_async_copy(same_size, same_size, filt_sem.at[k])

    def turned_out(slot, step):
        return pltpu.make_async_copy(turned_ref.at[slot], sent_ref.at[:, pl.ds(step * (width // LANES), width // LANES), slot], out_sem.at[slot])

    def mixed_out(step):
        return pltpu.make_async_copy(mixed_ref, gate_ref.at[:, pl.ds(step * (width // LANES), width // LANES)], out_sem.at[2])

    def sending(k, off):
        dest = target(off)
        return pltpu.make_async_remote_copy(
            sent_ref.at[k, dest], got_ref.at[k, me], sent_sem.at[k, off], got_sem.at[k, off], device_id={"sp": dest}, device_id_type=mesh_id
        )

    def block_in(k, off):
        src = lax.rem(me - off + n_dev, n_dev)
        from_ref = got_ref if off else sent_ref
        return pltpu.make_async_copy(from_ref.at[k, src], block_ref.at[src], block_sem.at[off])

    def returning(k, off):
        dest = target(off)
        return pltpu.make_async_remote_copy(
            done_ref.at[k, dest], back_ref.at[k, me], done_sem.at[k, off], back_sem.at[k, off], device_id={"sp": dest}, device_id_type=mesh_id
        )

    def storing(k):
        return pltpu.make_async_copy(done_ref.at[k, me], back_ref.at[k, me], done_sem.at[k, 0])

    def constant(idx):
        return pltpu.make_async_copy(consts_in[idx], consts[idx], const_sem.at[idx])


    barrier = pltpu.get_barrier_semaphore()
    for off in range(1, n_dev):
        pl.semaphore_signal(barrier, inc=1, device_id={"sp": target(off)}, device_id_type=mesh_id)
    for off in range(1, n_groups):
        pl.semaphore_signal(barrier, inc=1, device_id={"dp": lax.rem(my_group + off, n_groups)}, device_id_type=mesh_id)

    order = spread_offsets(n_dev) + [0]

    def load(item):
        for which in range(2):

            @pl.when(which_mine == which)
            def _():
                loading(item, order[item], which).start()

    load(0)
    u_part(rows - 16, 16, 1).start()
    for item, off in enumerate(order):
        if item + 1 < len(order):
            load(item + 1)
        if item == 0:
            u_part(0, rows - 16, 0).start()
            weights(0, 0).start()
            for idx in range(len(consts)):
                constant(idx).start()
        loading(item, off, 0).wait()
        if units < n_chan:
            into = turned_ref.at[0, :, 0]
        elif off:
            into = done_ref.at[target(off)]
        else:
            into = filt_ref.at[:, me, own_rows(my_group), :]
        together = math.gcd(n_rows, 4)

        @pl.loop(0, n_rows // together)
        def _(i):
            for j in range(together):
                r = i * together + j
                turn_rows(stage_ref[item % 2, pl.ds(pl.multiple_of(r * LANES, LANES), LANES), :], into, n_chunks, r, n_rows)

        if units < n_chan:
            start = pl.multiple_of(lax.rem(first_unit, n_chan) * n_rows, n_rows)
            share = turned_ref[0, :, 0, pl.ds(start, share_rows), :]
            if off:
                done_ref[target(off), :, pl.ds(0, share_rows), :] = share
            else:
                filt_ref[:, me, own_rows(my_group), :] = share
        if item == 0:
            u_part(rows - 16, 16, 1).wait()
            tail_ref[...] = u_ref[pl.ds(rows - 16, 16), :].astype(F32)[8:]
            pl.semaphore_wait(barrier, n_dev + n_groups - 2)
            halo_send().start()
        if off:
            share_send(off).start()


    for idx in range(len(consts)):
        constant(idx).wait()
    u_part(0, rows - 16, 0).wait()
    halo_send().wait()

    @pl.loop(0, steps)
    def _(step):
        for which in range(3):
            if which < 2:
                weights(which + 1, step).start()
            else:

                @pl.when(step + 1 < steps)
                def _():
                    weights(0, step + 1).start()

            weights(which, step).wait()
            w_now = w_ref.at[lax.rem(which + step, 2)]
            cols = pl.ds(pl.multiple_of(which * model + step * width, width), width)
            bias = bias_ref[:, cols]
            halo = (dot32(halo_ref[...].astype(BF16), w_now[...]) + bias).astype(BF16).astype(F32)
            p_ref[0:8, :] = jnp.where(me > 0, halo, 0.0)
            tile = 2 * LANES

            @pl.loop(0, rows // tile)
            def _(i):
                start = pl.multiple_of(i * tile, tile)
                proj = dot32(u_ref[pl.ds(start, tile), :], w_now[...]) + bias
                p_ref[pl.ds(start + 8, tile), :] = proj.astype(BF16).astype(F32)

            c0, c1, c2 = (taps_ref[t : t + 1, cols] for t in range(3))
            slot = 1 if which == 0 else 0

            @pl.when(step > 0)
            def _():
                if which == 1:
                    mixed_out(step - 1).wait()
                else:
                    turned_out(slot, step - 1).wait()

            @pl.loop(0, n_rows)
            def _(r):
                start = pl.multiple_of(r * LANES, LANES)
                window = p_ref[pl.ds(start, LANES + 8), :]
                mixed = c0 * window[8:] + c1 * window[7:-1] + c2 * window[6:-2]
                mixed = mixed.astype(BF16)
                for d in range(width // LANES):
                    block = mixed[:, d * LANES : (d + 1) * LANES].astype(F32)
                    if which != 1:
                        turn_rows(block, turned_ref.at[slot, :, d], n_chunks, r, n_rows)
                        continue
                    turned = block.T.astype(BF16)
                    for k in range(n_chunks):
                        at = pl.ds(pl.multiple_of(r * n_chan, n_chan), n_chan)
                        mixed_ref[k, d, at, :] = turned[k * n_chan : (k + 1) * n_chan]

            if which == 1:
                mixed_out(step).start()
            else:
                turned_out(slot, step).start()

    turned_out(0, steps - 1).wait()
    turned_out(1, steps - 1).wait()
    mixed_out(steps - 1).wait()

    @pl.loop(0, n_chunks)
    def _(k):
        for off in range(1, n_dev):
            sending(k, off).start()


    for off in range(1, n_dev):
        share_send(off).wait()

    @pl.loop(0, n_chunks)
    def _(k):
        for off in range(1, n_groups):
            group_send(k, off).start()


    spectrum, signal = spectrum_tools(group, n_high, tables, parts_ref)

    @pl.loop(0, n_chunks)
    def _(k):
        block_in(k, 0).start()
        for off in range(1, n_dev):
            sending(k, off).wait_recv()
            block_in(k, off).start()
        other_groups(k).wait()
        for off in range(n_dev):
            block_in(k, off).wait()

        @pl.loop(0, n_chan // group)
        def _(i):
            first = i * group

            def load_h(which, g):
                start = pl.multiple_of((which * n_chan + first + g) * n_rows, n_rows)
                return filt_ref[k, :, pl.ds(start, n_rows), :].reshape(n_high, LANES)

            def load_x(which, g):
                start = pl.multiple_of((first + g) * n_rows, n_rows)
                return block_ref[:, which, pl.ds(start, n_rows), :].reshape(n_high, LANES)

            chan = me * LANES + k * n_chan + first
            spec_one_ref[...] = spectrum([load_h(0, g) for g in range(group)], False)
            spec_two_ref[...] = spectrum([load_h(1, g) for g in range(group)], False)
            values = [load_x(0, g) for g in range(group)]
            conv = signal(spectrum(values, True), spec_one_ref)
            gated = [load_x(1, g) * (conv[g] + skip_one_ref[chan + g] * values[g]) for g in range(group)]
            conv = signal(spectrum(gated, False), spec_two_ref)
            for g in range(group):
                result = conv[g] + skip_two_ref[chan + g] * gated[g]
                done_ref[k, :, pl.ds(first + g, n_rows, stride=n_chan), :] = result.reshape(n_dev, n_rows, LANES)

        storing(k).start()
        for off in range(1, n_dev):
            returning(k, off).start()

    @pl.loop(0, n_chunks)
    def _(k):
        for off in range(1, n_dev):
            sending(k, off).wait_send()
        for off in range(1, n_groups):
            group_send(k, off).wait_send()


    tile = filt_ref.shape[2]
    n_tiles = rows // tile

    @pl.loop(0, n_tiles)
    def _(q):
        for e in range(model // LANES):
            part = u_ref[pl.ds(pl.multiple_of(q * tile, tile), tile), e * LANES : (e + 1) * LANES]
            filt_ref[e, q] = part.astype(F32)

    def returned(k):
        for off in range(1, n_dev):
            returning(k, off).wait()
        storing(k).wait()

    def pair_in(k, j):
        return (
            pltpu.make_async_copy(back_ref.at[k], block_ref.at[:, j], pair_sem.at[j, 0]),
            pltpu.make_async_copy(gate_ref.at[k], mixed_ref.at[:, j], pair_sem.at[j, 1]),
            pltpu.make_async_copy(w_out_ref.at[:, k], w_pair_ref.at[j], pair_sem.at[j, 2]),
        )

    @pl.loop(0, n_chunks // 2 - 1)
    def _(p):
        for j in range(2):
            returned(2 * p + j)
            for copy in pair_in(2 * p + j, j):
                copy.start()
        for j in range(2):
            for copy in pair_in(2 * p + j, j):
                copy.wait()

        @pl.loop(0, n_tiles)
        def _(q):
            for t in range(tile // LANES):
                for j in range(2):
                    at = pl.ds(pl.multiple_of((q * (tile // LANES) + t) * n_chan, n_chan), n_chan)
                    gated = block_ref[:, j, at, :] * mixed_ref[:, j, at, :].astype(F32)
                    gated_ref[t * LANES : (t + 1) * LANES, j * LANES : (j + 1) * LANES] = gated.reshape(LANES, LANES).T.astype(BF16)
            added = dot32(gated_ref[...], w_pair_ref[...].reshape(2 * LANES, model))
            for e in range(model // LANES):
                filt_ref[e, q] = filt_ref[e, q] + added[:, e * LANES : (e + 1) * LANES]

    sum_out = pltpu.make_async_copy(filt_ref.at[:, pl.ds(0, n_tiles)], sum_ref, pair_sem.at[0, 0])
    sum_out.start()
    for k in range(n_chunks - 2, n_chunks):
        returned(k)
    sum_out.wait()


def hyena(skip_one, skip_two, u, filt_one, filt_two, w_in, w_out, bias, taps, tables, n_dev, n_groups, units, group=4):
    rows, depth = u.shape
    model = w_in.shape[1] // 3
    width = 2 * LANES
    n_rows = rows // LANES
    n_chunks = n_dev
    n_high = n_dev * n_rows
    chunk_rows = LANES // n_chunks * n_rows
    hbm_spec = pl.BlockSpec(memory_space=pltpu.HBM)
    consts = (bias, taps, *tables)
    dma = pltpu.SemaphoreType.DMA
    return pl.pallas_call(
        functools.partial(hyena_body, n_dev, n_groups, units, group),
        in_specs=[hbm_spec] * (7 + len(consts)),
        out_specs=[hbm_spec] * 5,
        out_shape=[
            jax.ShapeDtypeStruct((n_chunks, n_dev, 2, chunk_rows, LANES), F32),
            jax.ShapeDtypeStruct((n_chunks, n_dev, chunk_rows, LANES), BF16),
            jax.ShapeDtypeStruct((n_chunks, n_dev, 2, chunk_rows, LANES), F32),
            jax.ShapeDtypeStruct((n_chunks, n_dev, chunk_rows, LANES), F32),
            jax.ShapeDtypeStruct((n_chunks, rows // (2 * chunk_rows), 2 * chunk_rows, LANES), F32),
        ],
        scratch_shapes=[
            pltpu.SMEM(skip_one.shape, F32),
            pltpu.SMEM(skip_two.shape, F32),
            *[pltpu.VMEM(c.shape, c.dtype) for c in consts],
            dma((2 + len(consts),)),
            pltpu.VMEM((rows, depth), BF16),
            pltpu.VMEM((2, depth, width), BF16),
            pltpu.VMEM((rows + 8, width), F32),
            pltpu.VMEM((2, rows, LANES), F32),
            pltpu.VMEM((2, n_chunks, width // LANES, chunk_rows, LANES), F32),
            pltpu.VMEM((n_chunks, width // LANES, chunk_rows, LANES), BF16),
            pltpu.VMEM((8, depth), F32),
            pltpu.VMEM((8, depth), F32),
            pltpu.VMEM((n_chunks, n_dev, 2 * chunk_rows, LANES), F32),
            pltpu.VMEM((n_dev, 2, chunk_rows, LANES), F32),
            pltpu.VMEM((n_chunks, n_dev, chunk_rows, LANES), F32),
            pltpu.VMEM((group * n_high, 6 * LANES), BF16),
            pltpu.VMEM((group * n_high, 2 * LANES), F32),
            pltpu.VMEM((group * n_high, 2 * LANES), F32),
            pltpu.VMEM((2 * chunk_rows, 2 * LANES), BF16),
            pltpu.VMEM((2, n_dev, LANES // n_chunks, model), BF16),
            dma((2,)),
            dma((2,)),
            dma((2,)),
            dma((3,)),
            dma((2,)),
            dma((n_dev,)),
            dma((n_dev,)),
            dma((n_chunks,)),
            dma((n_chunks,)),
            dma((n_chunks, n_dev)),
            dma((n_chunks, n_dev)),
            dma((n_dev,)),
            dma((n_chunks, n_dev)),
            dma((n_chunks, n_dev)),
            dma((2, 3)),
        ],
        cost_estimate=pl.CostEstimate(flops=10**11, bytes_accessed=100 * 2**20, transcendentals=0),
        compiler_params=pltpu.CompilerParams(collective_id=0, has_side_effects=True, vmem_limit_bytes=54 * 2**20),
        name="hyena",
    )(u, filt_one, filt_two, w_in, w_out, skip_one, skip_two, *consts)


def finish_body(sum_ref, gate_ref, back_ref, w_ref, out_ref, gated_ref):
    n_rows = back_ref.shape[2]
    for r in range(n_rows):
        for j in range(2):
            gated = back_ref[j, :, r] * gate_ref[j, :, r].astype(F32)
            gated_ref[r * LANES : (r + 1) * LANES, j * LANES : (j + 1) * LANES] = gated.reshape(LANES, LANES).T.astype(BF16)
    w_pair = jnp.concatenate([w_ref[:, j].reshape(LANES, w_ref.shape[3]) for j in range(2)], axis=0)
    added = dot32(gated_ref[...], w_pair)
    for e in range(sum_ref.shape[0]):
        cols = slice(e * LANES, (e + 1) * LANES)
        out_ref[:, cols] = (sum_ref[e] + added[:, cols]).astype(BF16)


def finish(partial, gate, back, w_out, n_rows=2):
    n_chunks, n_src, all_rows, n_chan, _ = back.shape
    rows, model = all_rows * LANES, w_out.shape[3]
    tile = n_rows * LANES
    last = n_chunks // 2 - 1
    pair = pl.BlockSpec((2, n_src, n_rows, n_chan, LANES), lambda i: (last, 0, i, 0, 0))
    return pl.pallas_call(
        finish_body,
        grid=(rows // tile,),
        in_specs=[
            pl.BlockSpec((model // LANES, tile, LANES), lambda i: (0, i, 0)),
            pair,
            pair,
            pl.BlockSpec((n_src, 2, n_chan, model), lambda i: (0, last, 0, 0)),
        ],
        out_specs=pl.BlockSpec((tile, model), lambda i: (i, 0)),
        out_shape=jax.ShapeDtypeStruct((rows, model), BF16),
        scratch_shapes=[pltpu.VMEM((tile, 2 * LANES), BF16)],
        cost_estimate=pl.CostEstimate(flops=4 * rows * model * LANES, bytes_accessed=16 * 2**20, transcendentals=0),
        compiler_params=pltpu.CompilerParams(dimension_semantics=("arbitrary",), vmem_limit_bytes=56 * 2**20),
        name="finish",
    )(partial, gate, back, w_out)


def solution(mesh):
    n_dev, n_groups = mesh.shape["sp"], mesh.shape["dp"]
    n_chunks = n_dev
    n_chan = LANES // n_chunks
    if n_groups < 2 or (2 * n_chan) % n_groups:
        raise ValueError("uneven groups")
    units = 2 * n_chan // n_groups

    def local_step(u_in, w_in, b_in, conv_taps, w_out, skip_one, skip_two, filt_one, filt_two):
        u = u_in[0]
        rows = u.shape[0]
        tables = [jnp.asarray(t) for t in transform_tables(rows * n_dev)]
        w_blocks = w_out.reshape(n_dev, n_chunks, n_chan, w_out.shape[1])
        _, gate, _, back, partial = hyena(
            skip_one, skip_two, u, filt_one, filt_two, w_in, w_blocks, b_in[None], conv_taps, tables, n_dev, n_groups, units
        )
        by_row = (n_chunks, n_dev, rows // LANES, n_chan, LANES)
        return finish(partial.reshape(-1, rows, LANES), gate.reshape(by_row), back.reshape(by_row), w_blocks)[None]

    seq_spec = P("dp", "sp", None)
    filt_spec = P("sp", None)
    return jax.shard_map(
        local_step,
        mesh=mesh,
        in_specs=(seq_spec, P(), P(), P(), P(), P(), P(), filt_spec, filt_spec),
        out_specs=seq_spec,
        check_vma=False,
    )
```

```python
import functools
import math
import jax
import jax.numpy as jnp
import numpy as np
from jax import lax
from jax.experimental import pallas as pl
from jax.experimental.pallas import tpu as pltpu
from jax.sharding import PartitionSpec as P

LANES = 128
F32 = jnp.float32
BF16 = jnp.bfloat16


def split_table(table, n_parts=3):
    parts, rest = [], np.asarray(table, np.float64)
    for _ in range(n_parts):
        part = rest.astype(jnp.bfloat16)
        parts.append(part)
        rest = rest - part.astype(np.float64)
    return parts


def transform_tables(seq_len):
    n_high = seq_len // LANES
    quarter = np.arange(n_high)[:, None] + 0.25
    high = 2.0 * np.pi * quarter * np.arange(n_high)[None, :] / n_high
    twist = 2.0 * np.pi * quarter * np.arange(LANES)[None, :] / seq_len
    low = 2.0 * np.pi * np.outer(np.arange(LANES), np.arange(LANES)) / LANES
    first = np.concatenate([np.cos(high), -np.sin(high)], axis=0)
    last = np.concatenate([np.cos(high.T), -np.sin(high.T)], axis=1)
    er, ei = np.cos(low), -np.sin(low)
    fwd = np.block([[er, ei], [-ei, er]])
    inv = np.block([[er, -ei], [ei, er]])
    a, b, c = split_table(first)
    first_wide = np.concatenate([a, a, a, b, b, c], axis=1)
    first_thin = np.concatenate([a, b, c], axis=1)
    fwd_parts = np.concatenate(split_table(fwd), axis=0)
    inv_parts = np.concatenate(split_table(inv), axis=0)
    last_parts = np.concatenate(split_table(last), axis=0)
    twist_tab = np.stack([np.cos(twist), -np.sin(twist)]).astype(np.float32)
    return first_wide, first_thin, fwd_parts, inv_parts, last_parts, twist_tab


def split3(x):
    hi = x.astype(BF16)
    rest = x - hi.astype(F32)
    mid = rest.astype(BF16)
    low = (rest - mid.astype(F32)).astype(BF16)
    return hi, mid, low


def dot32(a, b):
    return jnp.dot(a, b, preferred_element_type=F32)


def turn_rows(block, into_ref, n_chunks, row, n_rows):
    turned = block.T
    n_chan = LANES // n_chunks
    for k in range(n_chunks):
        into_ref[k, pl.ds(row, n_chan, stride=n_rows), :] = turned[k * n_chan : (k + 1) * n_chan]


def spread_offsets(n_dev):
    pairs = [off for near in range(2, n_dev, 4) for off in (near, n_dev - near)]
    rest = [off for off in range(1, n_dev) if off not in pairs]
    rest.sort(key=lambda off: -min(off, n_dev - off))
    return list(dict.fromkeys(pairs)) + rest


def spectrum_tools(group, n_high, tables, parts_ref):
    wide_ref, thin_ref, fwd_ref, inv_ref, last_ref, twist_ref = tables
    wide = 2 * LANES
    scale = 1.0 / (n_high * LANES)

    def complex_dot(tab_ref):
        return (
            dot32(parts_ref[:, 2 * wide :], tab_ref[:wide])
            + dot32(parts_ref[:, wide : 2 * wide], tab_ref[:wide])
            + dot32(parts_ref[:, :wide], tab_ref[wide : 2 * wide])
            + dot32(parts_ref[:, wide : 2 * wide], tab_ref[wide : 2 * wide])
            + dot32(parts_ref[:, :wide], tab_ref[2 * wide :])
            + dot32(parts_ref[:, :wide], tab_ref[:wide])
        )

    def store_parts(g, real, imag):
        for t, (re, im) in enumerate(zip(split3(real), split3(imag))):
            parts_ref[g * n_high : (g + 1) * n_high, 2 * t * LANES : (2 * t + 1) * LANES] = re
            parts_ref[g * n_high : (g + 1) * n_high, (2 * t + 1) * LANES : (2 * t + 2) * LANES] = im

    def spectrum(signals, exact):
        tr, ti = twist_ref[0], twist_ref[1]
        for g in range(0, group, 2):
            pair = jnp.concatenate([signals[g], signals[g + 1]], axis=1)
            if exact:
                short = pair.astype(BF16)
                coarse = dot32(thin_ref[...], jnp.concatenate([short, short, short], axis=0))
            else:
                hi, mid, low = split3(pair)
                coarse = dot32(wide_ref[...], jnp.concatenate([hi, mid, low, hi, mid, hi], axis=0))
            for j in range(2):
                re = coarse[:n_high, j * LANES : (j + 1) * LANES]
                im = coarse[n_high:, j * LANES : (j + 1) * LANES]
                store_parts(g + j, re * tr - im * ti, re * ti + im * tr)
        return complex_dot(fwd_ref)

    def signal(spec_a, spec_b):
        tr, ti = twist_ref[0], twist_ref[1]
        for g in range(group):
            rows = slice(g * n_high, (g + 1) * n_high)
            ar, ai = spec_a[rows, :LANES], spec_a[rows, LANES:]
            br, bi = spec_b[rows, :LANES], spec_b[rows, LANES:]
            store_parts(g, ar * br - ai * bi, ar * bi + ai * br)
        fine = complex_dot(inv_ref)
        results = []
        for g in range(0, group, 2):
            halves = []
            for j in range(2):
                rows = slice((g + j) * n_high, (g + j + 1) * n_high)
                re, im = fine[rows, :LANES] * scale, fine[rows, LANES:] * scale
                halves.append(jnp.concatenate([re * tr + im * ti, im * tr - re * ti], axis=0))
            hi, mid, low = split3(jnp.concatenate(halves, axis=1))
            d_hi = dot32(last_ref[...], hi)
            d_mid = dot32(last_ref[: 2 * n_high], mid)
            d_low = dot32(last_ref[:n_high], low)
            small = d_hi[2 * n_high :] + d_mid[n_high:] + d_low
            total = d_hi[:n_high] + ((d_hi[n_high : 2 * n_high] + d_mid[:n_high]) + small)
            results += [total[:, :LANES], total[:, LANES:]]
        return results

    return spectrum, signal


def hyena_body(n_dev, n_groups, units, group, u_hbm_ref, one_ref, two_ref, w_hbm_ref, w_out_ref, *refs):
    consts_in, refs = refs[:10], refs[10:]
    consts, const_sem, refs = refs[5:15], refs[15], refs[:5] + refs[16:]
    skip_one_ref, skip_two_ref, bias_ref, taps_ref, *tables = consts
    sent_ref, gate_ref, got_ref, back_ref, sum_ref = refs[:5]
    u_ref, w_ref, p_ref, stage_ref, turned_ref, mixed_ref, halo_ref, tail_ref = refs[5:13]
    filt_ref, block_ref, done_ref, parts_ref, spec_one_ref, spec_two_ref, gated_ref, w_pair_ref = refs[13:21]
    (u_sem, w_sem, stage_sem, out_sem, halo_sem, hold_sem, share_sem, group_sem, filt_sem, sent_sem, got_sem, block_sem, done_sem, back_sem, pair_sem, sum_sem) = refs[21:]
    me, my_group = lax.axis_index("sp"), lax.axis_index("dp")
    rows, depth = u_ref.shape
    n_rows = rows // LANES
    n_chunks = n_dev
    n_chan = LANES // n_chunks
    n_high = n_dev * n_rows
    model = w_hbm_ref.shape[1] // 3
    width = w_ref.shape[2]
    steps = model // width
    share_rows = units * n_rows
    first_unit = my_group * units
    which_mine = first_unit // n_chan
    mesh_id = pl.DeviceIdType.MESH

    def target(off):
        return lax.rem(me + off, n_dev)

    def own_rows(first):
        return pl.ds(pl.multiple_of(first * share_rows, share_rows), share_rows)


    def loading(item, off, which):
        cols = pl.ds(pl.multiple_of(target(off) * LANES, LANES), LANES)
        return pltpu.make_async_copy((one_ref, two_ref)[which].at[:, cols], stage_ref.at[item % 2], stage_sem.at[item % 2])

    def weights(which, step):
        cols = pl.ds(pl.multiple_of(which * model + step * width, width), width)
        slot = lax.rem(which + step, 2)
        return pltpu.make_async_copy(w_hbm_ref.at[:, cols], w_ref.at[slot], w_sem.at[slot])

    def u_part(start, size, idx):
        return pltpu.make_async_copy(u_hbm_ref.at[pl.ds(start, size), :], u_ref.at[pl.ds(start, size), :], u_sem.at[idx])

    def halo_send():
        return pltpu.make_async_remote_copy(tail_ref, halo_ref, halo_sem.at[0], halo_sem.at[1], device_id={"sp": target(1)}, device_id_type=mesh_id)

    def hold_of(dest):
        return done_ref.at[dest, :, pl.ds(0, share_rows), :]

    def share_send(off):
        dest = target(off)
        return pltpu.make_async_remote_copy(
            hold_of(dest), filt_ref.at[:, me, own_rows(my_group), :], hold_sem.at[off], share_sem.at[off], device_id={"sp": dest}, device_id_type=mesh_id
        )

    def group_send(k, off):
        mine = filt_ref.at[k, :, own_rows(my_group), :]
        return pltpu.make_async_remote_copy(
            mine, mine, group_sem.at[k], filt_sem.at[k], device_id={"dp": lax.rem(my_group + off, n_groups)}, device_id_type=mesh_id
        )

    def other_groups(k):
        same_size = filt_ref.at[k, :, pl.ds(0, (n_groups - 1) * share_rows), :]
        return pltpu.make_async_copy(same_size, same_size, filt_sem.at[k])

    def turned_out(slot, step):
        return pltpu.make_async_copy(turned_ref.at[slot], sent_ref.at[:, pl.ds(step * (width // LANES), width // LANES), slot], out_sem.at[slot])

    def mixed_out(step):
        return pltpu.make_async_copy(mixed_ref, gate_ref.at[:, pl.ds(step * (width // LANES), width // LANES)], out_sem.at[2])

    def sending(k, off):
        dest = target(off)
        return pltpu.make_async_remote_copy(
            sent_ref.at[k, dest], got_ref.at[k, me], sent_sem.at[k, off], got_sem.at[k, off], device_id={"sp": dest}, device_id_type=mesh_id
        )

    def block_in(k, off):
        src = lax.rem(me - off + n_dev, n_dev)
        from_ref = got_ref if off else sent_ref
        return pltpu.make_async_copy(from_ref.at[k, src], block_ref.at[src], block_sem.at[off])

    def returning(k, off):
        dest = target(off)
        return pltpu.make_async_remote_copy(
            done_ref.at[k, dest], back_ref.at[k, me], done_sem.at[k, off], back_sem.at[k, off], device_id={"sp": dest}, device_id_type=mesh_id
        )

    def storing(k):
        return pltpu.make_async_copy(done_ref.at[k, me], back_ref.at[k, me], done_sem.at[k, 0])

    def constant(idx):
        return pltpu.make_async_copy(consts_in[idx], consts[idx], const_sem.at[idx])


    barrier = pltpu.get_barrier_semaphore()
    for off in range(1, n_dev):
        pl.semaphore_signal(barrier, inc=1, device_id={"sp": target(off)}, device_id_type=mesh_id)
    for off in range(1, n_groups):
        pl.semaphore_signal(barrier, inc=1, device_id={"dp": lax.rem(my_group + off, n_groups)}, device_id_type=mesh_id)

    order = spread_offsets(n_dev) + [0]

    def load(item):
        for which in range(2):

            @pl.when(which_mine == which)
            def _():
                loading(item, order[item], which).start()

    load(0)
    u_part(rows - 16, 16, 1).start()
    for item, off in enumerate(order):
        if item + 1 < len(order):
            load(item + 1)
        if item == 0:
            u_part(0, rows - 16, 0).start()
            weights(0, 0).start()
            for idx in range(len(consts)):
                constant(idx).start()
        loading(item, off, 0).wait()
        if units < n_chan:
            into = turned_ref.at[0, :, 0]
        elif off:
            into = done_ref.at[target(off)]
        else:
            into = filt_ref.at[:, me, own_rows(my_group), :]
        together = math.gcd(n_rows, 4)

        @pl.loop(0, n_rows // together)
        def _(i):
            for j in range(together):
                r = i * together + j
                turn_rows(stage_ref[item % 2, pl.ds(pl.multiple_of(r * LANES, LANES), LANES), :], into, n_chunks, r, n_rows)

        if units < n_chan:
            start = pl.multiple_of(lax.rem(first_unit, n_chan) * n_rows, n_rows)
            share = turned_ref[0, :, 0, pl.ds(start, share_rows), :]
            if off:
                done_ref[target(off), :, pl.ds(0, share_rows), :] = share
            else:
                filt_ref[:, me, own_rows(my_group), :] = share
        if item == 0:
            u_part(rows - 16, 16, 1).wait()
            tail_ref[...] = u_ref[pl.ds(rows - 16, 16), :].astype(F32)[8:]
            pl.semaphore_wait(barrier, n_dev + n_groups - 2)
            halo_send().start()
        if off:
            share_send(off).start()


    for idx in range(len(consts)):
        constant(idx).wait()
    u_part(0, rows - 16, 0).wait()
    halo_send().wait()

    @pl.loop(0, steps)
    def _(step):
        for which in range(3):
            if which < 2:
                weights(which + 1, step).start()
            else:

                @pl.when(step + 1 < steps)
                def _():
                    weights(0, step + 1).start()

            weights(which, step).wait()
            w_now = w_ref.at[lax.rem(which + step, 2)]
            cols = pl.ds(pl.multiple_of(which * model + step * width, width), width)
            bias = bias_ref[:, cols]
            halo = (dot32(halo_ref[...].astype(BF16), w_now[...]) + bias).astype(BF16).astype(F32)
            p_ref[0:8, :] = jnp.where(me > 0, halo, 0.0)
            tile = 2 * LANES

            @pl.loop(0, rows // tile)
            def _(i):
                start = pl.multiple_of(i * tile, tile)
                proj = dot32(u_ref[pl.ds(start, tile), :], w_now[...]) + bias
                p_ref[pl.ds(start + 8, tile), :] = proj.astype(BF16).astype(F32)

            c0, c1, c2 = (taps_ref[t : t + 1, cols] for t in range(3))
            slot = 1 if which == 0 else 0

            @pl.when(step > 0)
            def _():
                if which == 1:
                    mixed_out(step - 1).wait()
                else:
                    turned_out(slot, step - 1).wait()

            @pl.loop(0, n_rows)
            def _(r):
                start = pl.multiple_of(r * LANES, LANES)
                window = p_ref[pl.ds(start, LANES + 8), :]
                mixed = c0 * window[8:] + c1 * window[7:-1] + c2 * window[6:-2]
                mixed = mixed.astype(BF16)
                for d in range(width // LANES):
                    block = mixed[:, d * LANES : (d + 1) * LANES].astype(F32)
                    if which != 1:
                        turn_rows(block, turned_ref.at[slot, :, d], n_chunks, r, n_rows)
                        continue
                    turned = block.T.astype(BF16)
                    for k in range(n_chunks):
                        at = pl.ds(pl.multiple_of(r * n_chan, n_chan), n_chan)
                        mixed_ref[k, d, at, :] = turned[k * n_chan : (k + 1) * n_chan]

            if which == 1:
                mixed_out(step).start()
            else:
                turned_out(slot, step).start()

    turned_out(0, steps - 1).wait()
    turned_out(1, steps - 1).wait()
    mixed_out(steps - 1).wait()

    @pl.loop(0, n_chunks)
    def _(k):
        for off in range(1, n_dev):
            sending(k, off).start()


    for off in range(1, n_dev):
        share_send(off).wait()

    @pl.loop(0, n_chunks)
    def _(k):
        for off in range(1, n_groups):
            group_send(k, off).start()


    spectrum, signal = spectrum_tools(group, n_high, tables, parts_ref)

    @pl.loop(0, n_chunks)
    def _(k):
        block_in(k, 0).start()
        for off in range(1, n_dev):
            sending(k, off).wait_recv()
            block_in(k, off).start()
        other_groups(k).wait()
        for off in range(n_dev):
            block_in(k, off).wait()

        @pl.loop(0, n_chan // group)
        def _(i):
            first = i * group

            def load_h(which, g):
                start = pl.multiple_of((which * n_chan + first + g) * n_rows, n_rows)
                return filt_ref[k, :, pl.ds(start, n_rows), :].reshape(n_high, LANES)

            def load_x(which, g):
                start = pl.multiple_of((first + g) * n_rows, n_rows)
                return block_ref[:, which, pl.ds(start, n_rows), :].reshape(n_high, LANES)

            chan = me * LANES + k * n_chan + first
            spec_one_ref[...] = spectrum([load_h(0, g) for g in range(group)], False)
            spec_two_ref[...] = spectrum([load_h(1, g) for g in range(group)], False)
            values = [load_x(0, g) for g in range(group)]
            conv = signal(spectrum(values, True), spec_one_ref)
            gated = [load_x(1, g) * (conv[g] + skip_one_ref[chan + g] * values[g]) for g in range(group)]
            conv = signal(spectrum(gated, False), spec_two_ref)
            for g in range(group):
                result = conv[g] + skip_two_ref[chan + g] * gated[g]
                done_ref[k, :, pl.ds(first + g, n_rows, stride=n_chan), :] = result.reshape(n_dev, n_rows, LANES)

        storing(k).start()
        for off in range(1, n_dev):
            returning(k, off).start()

    @pl.loop(0, n_chunks)
    def _(k):
        for off in range(1, n_dev):
            sending(k, off).wait_send()
        for off in range(1, n_groups):
            group_send(k, off).wait_send()


    tile = filt_ref.shape[2]
    n_tiles = rows // tile

    @pl.loop(0, n_tiles)
    def _(q):
        for e in range(model // LANES):
            part = u_ref[pl.ds(pl.multiple_of(q * tile, tile), tile), e * LANES : (e + 1) * LANES]
            filt_ref[e, q] = part.astype(F32)

    def returned(k):
        for off in range(1, n_dev):
            returning(k, off).wait()
        storing(k).wait()

    def pair_in(k, j):
        return (
            pltpu.make_async_copy(back_ref.at[k], block_ref.at[:, j], pair_sem.at[j, 0]),
            pltpu.make_async_copy(gate_ref.at[k], mixed_ref.at[:, j], pair_sem.at[j, 1]),
            pltpu.make_async_copy(w_out_ref.at[:, k], w_pair_ref.at[j], pair_sem.at[j, 2]),
        )

    n_pairs = n_chunks // 2 - 1

    def sum_out(q):
        return pltpu.make_async_copy(filt_ref.at[:, q], sum_ref.at[:, q], sum_sem.at[q])

    @pl.loop(0, n_pairs)
    def _(p):
        for j in range(2):
            returned(2 * p + j)
            for copy in pair_in(2 * p + j, j):
                copy.start()
        for j in range(2):
            for copy in pair_in(2 * p + j, j):
                copy.wait()

        @pl.loop(0, n_tiles)
        def _(q):
            for t in range(tile // LANES):
                for j in range(2):
                    at = pl.ds(pl.multiple_of((q * (tile // LANES) + t) * n_chan, n_chan), n_chan)
                    gated = block_ref[:, j, at, :] * mixed_ref[:, j, at, :].astype(F32)
                    gated_ref[t * LANES : (t + 1) * LANES, j * LANES : (j + 1) * LANES] = gated.reshape(LANES, LANES).T.astype(BF16)
            added = dot32(gated_ref[...], w_pair_ref[...].reshape(2 * LANES, model))
            for e in range(model // LANES):
                filt_ref[e, q] = filt_ref[e, q] + added[:, e * LANES : (e + 1) * LANES]

            @pl.when(p == n_pairs - 1)
            def _():
                sum_out(q).start()

    for k in range(n_chunks - 2, n_chunks):
        returned(k)

    @pl.loop(0, n_tiles)
    def _(q):
        if n_pairs == 0:
            sum_out(q).start()
        sum_out(q).wait()


def hyena(skip_one, skip_two, u, filt_one, filt_two, w_in, w_out, bias, taps, tables, n_dev, n_groups, units, group=4):
    rows, depth = u.shape
    model = w_in.shape[1] // 3
    width = 2 * LANES
    n_rows = rows // LANES
    n_chunks = n_dev
    n_high = n_dev * n_rows
    chunk_rows = LANES // n_chunks * n_rows
    hbm_spec = pl.BlockSpec(memory_space=pltpu.HBM)
    consts = (bias, taps, *tables)
    dma = pltpu.SemaphoreType.DMA
    return pl.pallas_call(
        functools.partial(hyena_body, n_dev, n_groups, units, group),
        in_specs=[hbm_spec] * (7 + len(consts)),
        out_specs=[hbm_spec] * 5,
        out_shape=[
            jax.ShapeDtypeStruct((n_chunks, n_dev, 2, chunk_rows, LANES), F32),
            jax.ShapeDtypeStruct((n_chunks, n_dev, chunk_rows, LANES), BF16),
            jax.ShapeDtypeStruct((n_chunks, n_dev, 2, chunk_rows, LANES), F32),
            jax.ShapeDtypeStruct((n_chunks, n_dev, chunk_rows, LANES), F32),
            jax.ShapeDtypeStruct((n_chunks, rows // (2 * chunk_rows), 2 * chunk_rows, LANES), F32),
        ],
        scratch_shapes=[
            pltpu.SMEM(skip_one.shape, F32),
            pltpu.SMEM(skip_two.shape, F32),
            *[pltpu.VMEM(c.shape, c.dtype) for c in consts],
            dma((2 + len(consts),)),
            pltpu.VMEM((rows, depth), BF16),
            pltpu.VMEM((2, depth, width), BF16),
            pltpu.VMEM((rows + 8, width), F32),
            pltpu.VMEM((2, rows, LANES), F32),
            pltpu.VMEM((2, n_chunks, width // LANES, chunk_rows, LANES), F32),
            pltpu.VMEM((n_chunks, width // LANES, chunk_rows, LANES), BF16),
            pltpu.VMEM((8, depth), F32),
            pltpu.VMEM((8, depth), F32),
            pltpu.VMEM((n_chunks, n_dev, 2 * chunk_rows, LANES), F32),
            pltpu.VMEM((n_dev, 2, chunk_rows, LANES), F32),
            pltpu.VMEM((n_chunks, n_dev, chunk_rows, LANES), F32),
            pltpu.VMEM((group * n_high, 6 * LANES), BF16),
            pltpu.VMEM((group * n_high, 2 * LANES), F32),
            pltpu.VMEM((group * n_high, 2 * LANES), F32),
            pltpu.VMEM((2 * chunk_rows, 2 * LANES), BF16),
            pltpu.VMEM((2, n_dev, LANES // n_chunks, model), BF16),
            dma((2,)),
            dma((2,)),
            dma((2,)),
            dma((3,)),
            dma((2,)),
            dma((n_dev,)),
            dma((n_dev,)),
            dma((n_chunks,)),
            dma((n_chunks,)),
            dma((n_chunks, n_dev)),
            dma((n_chunks, n_dev)),
            dma((n_dev,)),
            dma((n_chunks, n_dev)),
            dma((n_chunks, n_dev)),
            dma((2, 3)),
            dma((rows // (2 * chunk_rows),)),
        ],
        cost_estimate=pl.CostEstimate(flops=10**11, bytes_accessed=100 * 2**20, transcendentals=0),
        compiler_params=pltpu.CompilerParams(collective_id=0, has_side_effects=True, vmem_limit_bytes=54 * 2**20),
        name="hyena",
    )(u, filt_one, filt_two, w_in, w_out, skip_one, skip_two, *consts)


def finish_body(n_rows, sum_hbm_ref, gate_hbm_ref, back_hbm_ref, w_hbm_ref, out_hbm_ref, *refs):
    sum_ref, gate_ref, back_ref, w_ref, out_ref, gated_ref, in_sem, w_sem, out_sem = refs
    first = gate_hbm_ref.shape[0] - 2
    tile = n_rows * LANES
    n_tiles = out_ref.shape[0] // tile

    def rows_of(i):
        return pl.ds(pl.multiple_of(i * tile, tile), tile)

    def tile_in(i):
        narrow = pl.ds(i * n_rows, n_rows)
        return (
            pltpu.make_async_copy(sum_hbm_ref.at[:, rows_of(i)], sum_ref.at[:, rows_of(i)], in_sem.at[i, 0]),
            pltpu.make_async_copy(gate_hbm_ref.at[pl.ds(first, 2), :, narrow], gate_ref.at[:, :, narrow], in_sem.at[i, 1]),
            pltpu.make_async_copy(back_hbm_ref.at[pl.ds(first, 2), :, narrow], back_ref.at[:, :, narrow], in_sem.at[i, 2]),
        )

    def tile_out(i):
        return pltpu.make_async_copy(out_ref.at[rows_of(i)], out_hbm_ref.at[rows_of(i)], out_sem.at[i])

    w_in = pltpu.make_async_copy(w_hbm_ref.at[:, pl.ds(first, 2)], w_ref, w_sem)
    w_in.start()

    @pl.loop(0, n_tiles)
    def _(i):
        for copy in tile_in(i):
            copy.start()

    w_in.wait()

    @pl.loop(0, n_tiles)
    def _(i):
        for copy in tile_in(i):
            copy.wait()
        for r in range(n_rows):
            for j in range(2):
                gated = back_ref[j, :, i * n_rows + r] * gate_ref[j, :, i * n_rows + r].astype(F32)
                gated_ref[r * LANES : (r + 1) * LANES, j * LANES : (j + 1) * LANES] = gated.reshape(LANES, LANES).T.astype(BF16)
        w_pair = jnp.concatenate([w_ref[:, j].reshape(LANES, w_ref.shape[3]) for j in range(2)], axis=0)
        added = dot32(gated_ref[...], w_pair)
        for e in range(sum_ref.shape[0]):
            cols = slice(e * LANES, (e + 1) * LANES)
            out_ref[rows_of(i), cols] = (sum_ref[e, rows_of(i)] + added[:, cols]).astype(BF16)
        tile_out(i).start()

    @pl.loop(0, n_tiles)
    def _(i):
        tile_out(i).wait()


def finish(partial, gate, back, w_out, n_rows=2):
    _, n_src, all_rows, n_chan, _ = back.shape
    rows, model = all_rows * LANES, w_out.shape[3]
    n_tiles = all_rows // n_rows
    hbm_spec = pl.BlockSpec(memory_space=pltpu.HBM)
    return pl.pallas_call(
        functools.partial(finish_body, n_rows),
        in_specs=[hbm_spec] * 4,
        out_specs=hbm_spec,
        out_shape=jax.ShapeDtypeStruct((rows, model), BF16),
        scratch_shapes=[
            pltpu.VMEM(partial.shape, F32),
            pltpu.VMEM((2,) + gate.shape[1:], BF16),
            pltpu.VMEM((2,) + back.shape[1:], F32),
            pltpu.VMEM((n_src, 2, n_chan, model), BF16),
            pltpu.VMEM((rows, model), BF16),
            pltpu.VMEM((n_rows * LANES, 2 * LANES), BF16),
            pltpu.SemaphoreType.DMA((n_tiles, 3)),
            pltpu.SemaphoreType.DMA,
            pltpu.SemaphoreType.DMA((n_tiles,)),
        ],
        cost_estimate=pl.CostEstimate(flops=4 * rows * model * LANES, bytes_accessed=16 * 2**20, transcendentals=0),
        compiler_params=pltpu.CompilerParams(vmem_limit_bytes=56 * 2**20),
        name="finish",
    )(partial, gate, back, w_out)


def solution(mesh):
    n_dev, n_groups = mesh.shape["sp"], mesh.shape["dp"]
    n_chunks = n_dev
    n_chan = LANES // n_chunks
    if n_groups < 2 or (2 * n_chan) % n_groups:
        raise ValueError("uneven groups")
    units = 2 * n_chan // n_groups

    def local_step(u_in, w_in, b_in, conv_taps, w_out, skip_one, skip_two, filt_one, filt_two):
        u = u_in[0]
        rows = u.shape[0]
        tables = [jnp.asarray(t) for t in transform_tables(rows * n_dev)]
        w_blocks = w_out.reshape(n_dev, n_chunks, n_chan, w_out.shape[1])
        _, gate, _, back, partial = hyena(
            skip_one, skip_two, u, filt_one, filt_two, w_in, w_blocks, b_in[None], conv_taps, tables, n_dev, n_groups, units
        )
        by_row = (n_chunks, n_dev, rows // LANES, n_chan, LANES)
        return finish(partial.reshape(-1, rows, LANES), gate.reshape(by_row), back.reshape(by_row), w_blocks)[None]

    seq_spec = P("dp", "sp", None)
    filt_spec = P("sp", None)
    return jax.shard_map(
        local_step,
        mesh=mesh,
        in_specs=(seq_spec, P(), P(), P(), P(), P(), P(), filt_spec, filt_spec),
        out_specs=seq_spec,
        check_vma=False,
    )
```

```python
import functools
import math
import jax
import jax.numpy as jnp
import numpy as np
from jax import lax
from jax.experimental import pallas as pl
from jax.experimental.pallas import tpu as pltpu
from jax.sharding import PartitionSpec as P

LANES = 128
F32 = jnp.float32
BF16 = jnp.bfloat16


def split_table(table, n_parts=3):
    parts, rest = [], np.asarray(table, np.float64)
    for _ in range(n_parts):
        part = rest.astype(jnp.bfloat16)
        parts.append(part)
        rest = rest - part.astype(np.float64)
    return parts


def transform_tables(seq_len):
    n_high = seq_len // LANES
    quarter = np.arange(n_high)[:, None] + 0.25
    high = 2.0 * np.pi * quarter * np.arange(n_high)[None, :] / n_high
    twist = 2.0 * np.pi * quarter * np.arange(LANES)[None, :] / seq_len
    low = 2.0 * np.pi * np.outer(np.arange(LANES), np.arange(LANES)) / LANES
    first = np.concatenate([np.cos(high), -np.sin(high)], axis=0)
    last = np.concatenate([np.cos(high.T), -np.sin(high.T)], axis=1)
    er, ei = np.cos(low), -np.sin(low)
    fwd = np.block([[er, ei], [-ei, er]])
    inv = np.block([[er, -ei], [ei, er]])
    a, b, c = split_table(first)
    first_wide = np.concatenate([a, a, a, b, b, c], axis=1)
    first_thin = np.concatenate([a, b, c], axis=1)
    fwd_parts = np.concatenate(split_table(fwd), axis=0)
    inv_parts = np.concatenate(split_table(inv), axis=0)
    last_parts = np.concatenate(split_table(last), axis=0)
    twist_tab = np.stack([np.cos(twist), -np.sin(twist)]).astype(np.float32)
    return first_wide, first_thin, fwd_parts, inv_parts, last_parts, twist_tab


def split3(x):
    hi = x.astype(BF16)
    rest = x - hi.astype(F32)
    mid = rest.astype(BF16)
    low = (rest - mid.astype(F32)).astype(BF16)
    return hi, mid, low


def dot32(a, b):
    return jnp.dot(a, b, preferred_element_type=F32)


def turn_rows(block, into_ref, n_chunks, row, n_rows):
    turned = block.T
    n_chan = LANES // n_chunks
    for k in range(n_chunks):
        into_ref[k, pl.ds(row, n_chan, stride=n_rows), :] = turned[k * n_chan : (k + 1) * n_chan]


def far_first(n_dev):
    return sorted(range(1, n_dev), key=lambda off: -min(off, n_dev - off))


def spectrum_tools(group, n_high, tables, parts_ref):
    wide_ref, thin_ref, fwd_ref, inv_ref, last_ref, twist_ref = tables
    wide = 2 * LANES
    scale = 1.0 / (n_high * LANES)

    def complex_dot(tab_ref):
        return (
            dot32(parts_ref[:, 2 * wide :], tab_ref[:wide])
            + dot32(parts_ref[:, wide : 2 * wide], tab_ref[:wide])
            + dot32(parts_ref[:, :wide], tab_ref[wide : 2 * wide])
            + dot32(parts_ref[:, wide : 2 * wide], tab_ref[wide : 2 * wide])
            + dot32(parts_ref[:, :wide], tab_ref[2 * wide :])
            + dot32(parts_ref[:, :wide], tab_ref[:wide])
        )

    def store_parts(g, real, imag):
        for t, (re, im) in enumerate(zip(split3(real), split3(imag))):
            parts_ref[g * n_high : (g + 1) * n_high, 2 * t * LANES : (2 * t + 1) * LANES] = re
            parts_ref[g * n_high : (g + 1) * n_high, (2 * t + 1) * LANES : (2 * t + 2) * LANES] = im

    def spectrum(signals, exact):
        tr, ti = twist_ref[0], twist_ref[1]
        for g in range(0, group, 2):
            pair = jnp.concatenate([signals[g], signals[g + 1]], axis=1)
            if exact:
                short = pair.astype(BF16)
                coarse = dot32(thin_ref[...], jnp.concatenate([short, short, short], axis=0))
            else:
                hi, mid, low = split3(pair)
                coarse = dot32(wide_ref[...], jnp.concatenate([hi, mid, low, hi, mid, hi], axis=0))
            for j in range(2):
                re = coarse[:n_high, j * LANES : (j + 1) * LANES]
                im = coarse[n_high:, j * LANES : (j + 1) * LANES]
                store_parts(g + j, re * tr - im * ti, re * ti + im * tr)
        return complex_dot(fwd_ref)

    def signal(spec_a, spec_b):
        tr, ti = twist_ref[0], twist_ref[1]
        for g in range(group):
            rows = slice(g * n_high, (g + 1) * n_high)
            ar, ai = spec_a[rows, :LANES], spec_a[rows, LANES:]
            br, bi = spec_b[rows, :LANES], spec_b[rows, LANES:]
            store_parts(g, ar * br - ai * bi, ar * bi + ai * br)
        fine = complex_dot(inv_ref)
        results = []
        for g in range(0, group, 2):
            halves = []
            for j in range(2):
                rows = slice((g + j) * n_high, (g + j + 1) * n_high)
                re, im = fine[rows, :LANES] * scale, fine[rows, LANES:] * scale
                halves.append(jnp.concatenate([re * tr + im * ti, im * tr - re * ti], axis=0))
            hi, mid, low = split3(jnp.concatenate(halves, axis=1))
            d_hi = dot32(last_ref[...], hi)
            d_mid = dot32(last_ref[: 2 * n_high], mid)
            d_low = dot32(last_ref[:n_high], low)
            small = d_hi[2 * n_high :] + d_mid[n_high:] + d_low
            total = d_hi[:n_high] + ((d_hi[n_high : 2 * n_high] + d_mid[:n_high]) + small)
            results += [total[:, :LANES], total[:, LANES:]]
        return results

    return spectrum, signal


def hyena_body(n_dev, n_groups, units, group, u_hbm_ref, one_ref, two_ref, w_hbm_ref, w_out_ref, *refs):
    consts_in, refs = refs[:10], refs[10:]
    consts, const_sem, refs = refs[5:15], refs[15], refs[:5] + refs[16:]
    skip_one_ref, skip_two_ref, bias_ref, taps_ref, *tables = consts
    sent_ref, gate_ref, got_ref, back_ref, sum_ref = refs[:5]
    u_ref, w_ref, p_ref, stage_ref, turned_ref, mixed_ref, halo_ref, tail_ref = refs[5:13]
    filt_ref, block_ref, done_ref, parts_ref, spec_one_ref, spec_two_ref, gated_ref, w_pair_ref = refs[13:21]
    (u_sem, w_sem, stage_sem, out_sem, halo_sem, hold_sem, share_sem, group_sem, filt_sem, sent_sem, got_sem, block_sem, done_sem, back_sem, pair_sem, sum_sem) = refs[21:]
    me, my_group = lax.axis_index("sp"), lax.axis_index("dp")
    rows, depth = u_ref.shape
    n_rows = rows // LANES
    n_chunks = n_dev
    n_chan = LANES // n_chunks
    n_high = n_dev * n_rows
    model = w_hbm_ref.shape[1] // 3
    width = w_ref.shape[2]
    steps = model // width
    share_rows = units * n_rows
    first_unit = my_group * units
    which_mine = first_unit // n_chan
    mesh_id = pl.DeviceIdType.MESH

    def target(off):
        return lax.rem(me + off, n_dev)

    def own_rows(first):
        return pl.ds(pl.multiple_of(first * share_rows, share_rows), share_rows)


    def loading(item, off, which):
        cols = pl.ds(pl.multiple_of(target(off) * LANES, LANES), LANES)
        return pltpu.make_async_copy((one_ref, two_ref)[which].at[:, cols], stage_ref.at[item % 2], stage_sem.at[item % 2])

    def weights(which, step):
        cols = pl.ds(pl.multiple_of(which * model + step * width, width), width)
        slot = lax.rem(which + step, 2)
        return pltpu.make_async_copy(w_hbm_ref.at[:, cols], w_ref.at[slot], w_sem.at[slot])

    def u_part(start, size, idx):
        return pltpu.make_async_copy(u_hbm_ref.at[pl.ds(start, size), :], u_ref.at[pl.ds(start, size), :], u_sem.at[idx])

    def halo_send():
        return pltpu.make_async_remote_copy(tail_ref, halo_ref, halo_sem.at[0], halo_sem.at[1], device_id={"sp": target(1)}, device_id_type=mesh_id)

    def hold_of(dest):
        return done_ref.at[dest, :, pl.ds(0, share_rows), :]

    def share_send(off):
        dest = target(off)
        return pltpu.make_async_remote_copy(
            hold_of(dest), filt_ref.at[:, me, own_rows(my_group), :], hold_sem.at[off], share_sem.at[off], device_id={"sp": dest}, device_id_type=mesh_id
        )

    def group_send(k, off):
        mine = filt_ref.at[k, :, own_rows(my_group), :]
        return pltpu.make_async_remote_copy(
            mine, mine, group_sem.at[k], filt_sem.at[k], device_id={"dp": lax.rem(my_group + off, n_groups)}, device_id_type=mesh_id
        )

    def other_groups(k):
        same_size = filt_ref.at[k, :, pl.ds(0, (n_groups - 1) * share_rows), :]
        return pltpu.make_async_copy(same_size, same_size, filt_sem.at[k])

    def turned_out(slot, step):
        return pltpu.make_async_copy(turned_ref.at[slot], sent_ref.at[:, pl.ds(step * (width // LANES), width // LANES), slot], out_sem.at[slot])

    def mixed_out(step):
        return pltpu.make_async_copy(mixed_ref, gate_ref.at[:, pl.ds(step * (width // LANES), width // LANES)], out_sem.at[2])

    def sending(k, off):
        dest = target(off)
        return pltpu.make_async_remote_copy(
            sent_ref.at[k, dest], got_ref.at[k, me], sent_sem.at[k, off], got_sem.at[k, off], device_id={"sp": dest}, device_id_type=mesh_id
        )

    def block_in(k, off):
        src = lax.rem(me - off + n_dev, n_dev)
        from_ref = got_ref if off else sent_ref
        return pltpu.make_async_copy(from_ref.at[k, src], block_ref.at[src], block_sem.at[off])

    def returning(k, off):
        dest = target(off)
        return pltpu.make_async_remote_copy(
            done_ref.at[k, dest], back_ref.at[k, me], done_sem.at[k, off], back_sem.at[k, off], device_id={"sp": dest}, device_id_type=mesh_id
        )

    def storing(k):
        return pltpu.make_async_copy(done_ref.at[k, me], back_ref.at[k, me], done_sem.at[k, 0])

    def constant(idx):
        return pltpu.make_async_copy(consts_in[idx], consts[idx], const_sem.at[idx])


    barrier = pltpu.get_barrier_semaphore()
    for off in range(1, n_dev):
        pl.semaphore_signal(barrier, inc=1, device_id={"sp": target(off)}, device_id_type=mesh_id)
    for off in range(1, n_groups):
        pl.semaphore_signal(barrier, inc=1, device_id={"dp": lax.rem(my_group + off, n_groups)}, device_id_type=mesh_id)

    order = far_first(n_dev) + [0]

    def load(item):
        for which in range(2):

            @pl.when(which_mine == which)
            def _():
                loading(item, order[item], which).start()

    load(0)
    u_part(rows - 16, 16, 1).start()
    for item, off in enumerate(order):
        if item + 1 < len(order):
            load(item + 1)
        if item == 0:
            u_part(0, rows - 16, 0).start()
            weights(0, 0).start()
            for idx in range(len(consts)):
                constant(idx).start()
        loading(item, off, 0).wait()
        if units < n_chan:
            into = turned_ref.at[0, :, 0]
        elif off:
            into = done_ref.at[target(off)]
        else:
            into = filt_ref.at[:, me, own_rows(my_group), :]
        together = math.gcd(n_rows, 4)

        @pl.loop(0, n_rows // together)
        def _(i):
            for j in range(together):
                r = i * together + j
                turn_rows(stage_ref[item % 2, pl.ds(pl.multiple_of(r * LANES, LANES), LANES), :], into, n_chunks, r, n_rows)

        if units < n_chan:
            start = pl.multiple_of(lax.rem(first_unit, n_chan) * n_rows, n_rows)
            share = turned_ref[0, :, 0, pl.ds(start, share_rows), :]
            if off:
                done_ref[target(off), :, pl.ds(0, share_rows), :] = share
            else:
                filt_ref[:, me, own_rows(my_group), :] = share
        if item == 0:
            u_part(rows - 16, 16, 1).wait()
            tail_ref[...] = u_ref[pl.ds(rows - 16, 16), :].astype(F32)[8:]
            pl.semaphore_wait(barrier, n_dev + n_groups - 2)
            halo_send().start()
        if off:
            share_send(off).start()


    for idx in range(len(consts)):
        constant(idx).wait()
    u_part(0, rows - 16, 0).wait()
    halo_send().wait()

    @pl.loop(0, steps)
    def _(step):
        for which in range(3):
            if which < 2:
                weights(which + 1, step).start()
            else:

                @pl.when(step + 1 < steps)
                def _():
                    weights(0, step + 1).start()

            weights(which, step).wait()
            w_now = w_ref.at[lax.rem(which + step, 2)]
            cols = pl.ds(pl.multiple_of(which * model + step * width, width), width)
            bias = bias_ref[:, cols]
            halo = (dot32(halo_ref[...].astype(BF16), w_now[...]) + bias).astype(BF16).astype(F32)
            p_ref[0:8, :] = jnp.where(me > 0, halo, 0.0)
            tile = 2 * LANES

            @pl.loop(0, rows // tile)
            def _(i):
                start = pl.multiple_of(i * tile, tile)
                proj = dot32(u_ref[pl.ds(start, tile), :], w_now[...]) + bias
                p_ref[pl.ds(start + 8, tile), :] = proj.astype(BF16).astype(F32)

            c0, c1, c2 = (taps_ref[t : t + 1, cols] for t in range(3))
            slot = 1 if which == 0 else 0

            @pl.when(step > 0)
            def _():
                if which == 1:
                    mixed_out(step - 1).wait()
                else:
                    turned_out(slot, step - 1).wait()

            @pl.loop(0, n_rows)
            def _(r):
                start = pl.multiple_of(r * LANES, LANES)
                window = p_ref[pl.ds(start, LANES + 8), :]
                mixed = c0 * window[8:] + c1 * window[7:-1] + c2 * window[6:-2]
                mixed = mixed.astype(BF16)
                for d in range(width // LANES):
                    block = mixed[:, d * LANES : (d + 1) * LANES].astype(F32)
                    if which != 1:
                        turn_rows(block, turned_ref.at[slot, :, d], n_chunks, r, n_rows)
                        continue
                    turned = block.T.astype(BF16)
                    for k in range(n_chunks):
                        at = pl.ds(pl.multiple_of(r * n_chan, n_chan), n_chan)
                        mixed_ref[k, d, at, :] = turned[k * n_chan : (k + 1) * n_chan]

            if which == 1:
                mixed_out(step).start()
            else:
                turned_out(slot, step).start()

    turned_out(0, steps - 1).wait()
    turned_out(1, steps - 1).wait()
    mixed_out(steps - 1).wait()

    @pl.loop(0, n_chunks)
    def _(k):
        for off in far_first(n_dev):
            sending(k, off).start()


    for off in range(1, n_dev):
        share_send(off).wait()

    @pl.loop(0, n_chunks)
    def _(k):
        for off in range(1, n_groups):
            group_send(k, off).start()


    spectrum, signal = spectrum_tools(group, n_high, tables, parts_ref)

    @pl.loop(0, n_chunks)
    def _(k):
        block_in(k, 0).start()
        for off in range(1, n_dev):
            sending(k, off).wait_recv()
            block_in(k, off).start()
        other_groups(k).wait()
        for off in range(n_dev):
            block_in(k, off).wait()

        @pl.loop(0, n_chan // group)
        def _(i):
            first = i * group

            def load_h(which, g):
                start = pl.multiple_of((which * n_chan + first + g) * n_rows, n_rows)
                return filt_ref[k, :, pl.ds(start, n_rows), :].reshape(n_high, LANES)

            def load_x(which, g):
                start = pl.multiple_of((first + g) * n_rows, n_rows)
                return block_ref[:, which, pl.ds(start, n_rows), :].reshape(n_high, LANES)

            chan = me * LANES + k * n_chan + first
            spec_one_ref[...] = spectrum([load_h(0, g) for g in range(group)], False)
            spec_two_ref[...] = spectrum([load_h(1, g) for g in range(group)], False)
            values = [load_x(0, g) for g in range(group)]
            conv = signal(spectrum(values, True), spec_one_ref)
            gated = [load_x(1, g) * (conv[g] + skip_one_ref[chan + g] * values[g]) for g in range(group)]
            conv = signal(spectrum(gated, False), spec_two_ref)
            for g in range(group):
                result = conv[g] + skip_two_ref[chan + g] * gated[g]
                done_ref[k, :, pl.ds(first + g, n_rows, stride=n_chan), :] = result.reshape(n_dev, n_rows, LANES)

        storing(k).start()
        for off in far_first(n_dev):
            returning(k, off).start()

    @pl.loop(0, n_chunks)
    def _(k):
        for off in range(1, n_dev):
            sending(k, off).wait_send()
        for off in range(1, n_groups):
            group_send(k, off).wait_send()


    tile = filt_ref.shape[2]
    n_tiles = rows // tile

    @pl.loop(0, n_tiles)
    def _(q):
        for e in range(model // LANES):
            part = u_ref[pl.ds(pl.multiple_of(q * tile, tile), tile), e * LANES : (e + 1) * LANES]
            filt_ref[e, q] = part.astype(F32)

    def returned(k):
        for off in range(1, n_dev):
            returning(k, off).wait()
        storing(k).wait()

    def pair_in(k, j):
        return (
            pltpu.make_async_copy(back_ref.at[k], block_ref.at[:, j], pair_sem.at[j, 0]),
            pltpu.make_async_copy(gate_ref.at[k], mixed_ref.at[:, j], pair_sem.at[j, 1]),
            pltpu.make_async_copy(w_out_ref.at[:, k], w_pair_ref.at[j], pair_sem.at[j, 2]),
        )

    n_pairs = n_chunks // 2 - 1

    def sum_out(q):
        return pltpu.make_async_copy(filt_ref.at[:, q], sum_ref.at[:, q], sum_sem.at[q])

    @pl.loop(0, n_pairs)
    def _(p):
        for j in range(2):
            returned(2 * p + j)
            for copy in pair_in(2 * p + j, j):
                copy.start()
        for j in range(2):
            for copy in pair_in(2 * p + j, j):
                copy.wait()

        @pl.loop(0, n_tiles)
        def _(q):
            for t in range(tile // LANES):
                for j in range(2):
                    at = pl.ds(pl.multiple_of((q * (tile // LANES) + t) * n_chan, n_chan), n_chan)
                    gated = block_ref[:, j, at, :] * mixed_ref[:, j, at, :].astype(F32)
                    gated_ref[t * LANES : (t + 1) * LANES, j * LANES : (j + 1) * LANES] = gated.reshape(LANES, LANES).T.astype(BF16)
            added = dot32(gated_ref[...], w_pair_ref[...].reshape(2 * LANES, model))
            for e in range(model // LANES):
                filt_ref[e, q] = filt_ref[e, q] + added[:, e * LANES : (e + 1) * LANES]

            @pl.when(p == n_pairs - 1)
            def _():
                sum_out(q).start()

    for k in range(n_chunks - 2, n_chunks):
        returned(k)

    @pl.loop(0, n_tiles)
    def _(q):
        if n_pairs == 0:
            sum_out(q).start()
        sum_out(q).wait()


def hyena(skip_one, skip_two, u, filt_one, filt_two, w_in, w_out, bias, taps, tables, n_dev, n_groups, units, group=4):
    rows, depth = u.shape
    model = w_in.shape[1] // 3
    width = 2 * LANES
    n_rows = rows // LANES
    n_chunks = n_dev
    n_high = n_dev * n_rows
    chunk_rows = LANES // n_chunks * n_rows
    hbm_spec = pl.BlockSpec(memory_space=pltpu.HBM)
    consts = (bias, taps, *tables)
    dma = pltpu.SemaphoreType.DMA
    return pl.pallas_call(
        functools.partial(hyena_body, n_dev, n_groups, units, group),
        in_specs=[hbm_spec] * (7 + len(consts)),
        out_specs=[hbm_spec] * 5,
        out_shape=[
            jax.ShapeDtypeStruct((n_chunks, n_dev, 2, chunk_rows, LANES), F32),
            jax.ShapeDtypeStruct((n_chunks, n_dev, chunk_rows, LANES), BF16),
            jax.ShapeDtypeStruct((n_chunks, n_dev, 2, chunk_rows, LANES), F32),
            jax.ShapeDtypeStruct((n_chunks, n_dev, chunk_rows, LANES), F32),
            jax.ShapeDtypeStruct((n_chunks, rows // (2 * chunk_rows), 2 * chunk_rows, LANES), F32),
        ],
        scratch_shapes=[
            pltpu.SMEM(skip_one.shape, F32),
            pltpu.SMEM(skip_two.shape, F32),
            *[pltpu.VMEM(c.shape, c.dtype) for c in consts],
            dma((2 + len(consts),)),
            pltpu.VMEM((rows, depth), BF16),
            pltpu.VMEM((2, depth, width), BF16),
            pltpu.VMEM((rows + 8, width), F32),
            pltpu.VMEM((2, rows, LANES), F32),
            pltpu.VMEM((2, n_chunks, width // LANES, chunk_rows, LANES), F32),
            pltpu.VMEM((n_chunks, width // LANES, chunk_rows, LANES), BF16),
            pltpu.VMEM((8, depth), F32),
            pltpu.VMEM((8, depth), F32),
            pltpu.VMEM((n_chunks, n_dev, 2 * chunk_rows, LANES), F32),
            pltpu.VMEM((n_dev, 2, chunk_rows, LANES), F32),
            pltpu.VMEM((n_chunks, n_dev, chunk_rows, LANES), F32),
            pltpu.VMEM((group * n_high, 6 * LANES), BF16),
            pltpu.VMEM((group * n_high, 2 * LANES), F32),
            pltpu.VMEM((group * n_high, 2 * LANES), F32),
            pltpu.VMEM((2 * chunk_rows, 2 * LANES), BF16),
            pltpu.VMEM((2, n_dev, LANES // n_chunks, model), BF16),
            dma((2,)),
            dma((2,)),
            dma((2,)),
            dma((3,)),
            dma((2,)),
            dma((n_dev,)),
            dma((n_dev,)),
            dma((n_chunks,)),
            dma((n_chunks,)),
            dma((n_chunks, n_dev)),
            dma((n_chunks, n_dev)),
            dma((n_dev,)),
            dma((n_chunks, n_dev)),
            dma((n_chunks, n_dev)),
            dma((2, 3)),
            dma((rows // (2 * chunk_rows),)),
        ],
        cost_estimate=pl.CostEstimate(flops=10**11, bytes_accessed=100 * 2**20, transcendentals=0),
        compiler_params=pltpu.CompilerParams(collective_id=0, has_side_effects=True, vmem_limit_bytes=54 * 2**20),
        name="hyena",
    )(u, filt_one, filt_two, w_in, w_out, skip_one, skip_two, *consts)


def finish_body(n_rows, sum_hbm_ref, gate_hbm_ref, back_hbm_ref, w_hbm_ref, out_hbm_ref, *refs):
    sum_ref, gate_ref, back_ref, w_ref, out_ref, gated_ref, in_sem, w_sem, out_sem = refs
    first = gate_hbm_ref.shape[0] - 2
    tile = n_rows * LANES
    n_tiles = out_ref.shape[0] // tile

    def rows_of(i):
        return pl.ds(pl.multiple_of(i * tile, tile), tile)

    def tile_in(i):
        narrow = pl.ds(i * n_rows, n_rows)
        return (
            pltpu.make_async_copy(sum_hbm_ref.at[:, rows_of(i)], sum_ref.at[:, rows_of(i)], in_sem.at[i, 0]),
            pltpu.make_async_copy(gate_hbm_ref.at[pl.ds(first, 2), :, narrow], gate_ref.at[:, :, narrow], in_sem.at[i, 1]),
            pltpu.make_async_copy(back_hbm_ref.at[pl.ds(first, 2), :, narrow], back_ref.at[:, :, narrow], in_sem.at[i, 2]),
        )

    def tile_out(i):
        return pltpu.make_async_copy(out_ref.at[rows_of(i)], out_hbm_ref.at[rows_of(i)], out_sem.at[i])

    w_in = pltpu.make_async_copy(w_hbm_ref.at[:, pl.ds(first, 2)], w_ref, w_sem)
    w_in.start()

    @pl.loop(0, n_tiles)
    def _(i):
        for copy in tile_in(i):
            copy.start()

    w_in.wait()

    @pl.loop(0, n_tiles)
    def _(i):
        for copy in tile_in(i):
            copy.wait()
        for r in range(n_rows):
            for j in range(2):
                gated = back_ref[j, :, i * n_rows + r] * gate_ref[j, :, i * n_rows + r].astype(F32)
                gated_ref[r * LANES : (r + 1) * LANES, j * LANES : (j + 1) * LANES] = gated.reshape(LANES, LANES).T.astype(BF16)
        w_pair = jnp.concatenate([w_ref[:, j].reshape(LANES, w_ref.shape[3]) for j in range(2)], axis=0)
        added = dot32(gated_ref[...], w_pair)
        for e in range(sum_ref.shape[0]):
            cols = slice(e * LANES, (e + 1) * LANES)
            out_ref[rows_of(i), cols] = (sum_ref[e, rows_of(i)] + added[:, cols]).astype(BF16)
        tile_out(i).start()

    @pl.loop(0, n_tiles)
    def _(i):
        tile_out(i).wait()


def finish(partial, gate, back, w_out, n_rows=2):
    _, n_src, all_rows, n_chan, _ = back.shape
    rows, model = all_rows * LANES, w_out.shape[3]
    n_tiles = all_rows // n_rows
    hbm_spec = pl.BlockSpec(memory_space=pltpu.HBM)
    return pl.pallas_call(
        functools.partial(finish_body, n_rows),
        in_specs=[hbm_spec] * 4,
        out_specs=hbm_spec,
        out_shape=jax.ShapeDtypeStruct((rows, model), BF16),
        scratch_shapes=[
            pltpu.VMEM(partial.shape, F32),
            pltpu.VMEM((2,) + gate.shape[1:], BF16),
            pltpu.VMEM((2,) + back.shape[1:], F32),
            pltpu.VMEM((n_src, 2, n_chan, model), BF16),
            pltpu.VMEM((rows, model), BF16),
            pltpu.VMEM((n_rows * LANES, 2 * LANES), BF16),
            pltpu.SemaphoreType.DMA((n_tiles, 3)),
            pltpu.SemaphoreType.DMA,
            pltpu.SemaphoreType.DMA((n_tiles,)),
        ],
        cost_estimate=pl.CostEstimate(flops=4 * rows * model * LANES, bytes_accessed=16 * 2**20, transcendentals=0),
        compiler_params=pltpu.CompilerParams(vmem_limit_bytes=56 * 2**20),
        name="finish",
    )(partial, gate, back, w_out)


def solution(mesh):
    n_dev, n_groups = mesh.shape["sp"], mesh.shape["dp"]
    n_chunks = n_dev
    n_chan = LANES // n_chunks
    if n_groups < 2 or (2 * n_chan) % n_groups:
        raise ValueError("uneven groups")
    units = 2 * n_chan // n_groups

    def local_step(u_in, w_in, b_in, conv_taps, w_out, skip_one, skip_two, filt_one, filt_two):
        u = u_in[0]
        rows = u.shape[0]
        tables = [jnp.asarray(t) for t in transform_tables(rows * n_dev)]
        w_blocks = w_out.reshape(n_dev, n_chunks, n_chan, w_out.shape[1])
        _, gate, _, back, partial = hyena(
            skip_one, skip_two, u, filt_one, filt_two, w_in, w_blocks, b_in[None], conv_taps, tables, n_dev, n_groups, units
        )
        by_row = (n_chunks, n_dev, rows // LANES, n_chan, LANES)
        return finish(partial.reshape(-1, rows, LANES), gate.reshape(by_row), back.reshape(by_row), w_blocks)[None]

    seq_spec = P("dp", "sp", None)
    filt_spec = P("sp", None)
    return jax.shard_map(
        local_step,
        mesh=mesh,
        in_specs=(seq_spec, P(), P(), P(), P(), P(), P(), filt_spec, filt_spec),
        out_specs=seq_spec,
        check_vma=False,
    )
```

```python
import functools
import math
import jax
import jax.numpy as jnp
import numpy as np
from jax import lax
from jax.experimental import pallas as pl
from jax.experimental.pallas import tpu as pltpu
from jax.sharding import PartitionSpec as P

LANES = 128
F32 = jnp.float32
BF16 = jnp.bfloat16


def split_table(table, n_parts=3):
    parts, rest = [], np.asarray(table, np.float64)
    for _ in range(n_parts):
        part = rest.astype(jnp.bfloat16)
        parts.append(part)
        rest = rest - part.astype(np.float64)
    return parts


def transform_tables(seq_len):
    n_high = seq_len // LANES
    quarter = np.arange(n_high)[:, None] + 0.25
    high = 2.0 * np.pi * quarter * np.arange(n_high)[None, :] / n_high
    twist = 2.0 * np.pi * quarter * np.arange(LANES)[None, :] / seq_len
    low = 2.0 * np.pi * np.outer(np.arange(LANES), np.arange(LANES)) / LANES
    first = np.concatenate([np.cos(high), -np.sin(high)], axis=0)
    last = np.concatenate([np.cos(high.T), -np.sin(high.T)], axis=1)
    er, ei = np.cos(low), -np.sin(low)
    fwd = np.block([[er, ei], [-ei, er]])
    inv = np.block([[er, -ei], [ei, er]])
    a, b, c = split_table(first)
    first_wide = np.concatenate([a, a, a, b, b, c], axis=1)
    first_thin = np.concatenate([a, b, c], axis=1)
    fwd_parts = np.concatenate(split_table(fwd), axis=0)
    inv_parts = np.concatenate(split_table(inv), axis=0)
    last_parts = np.concatenate(split_table(last), axis=0)
    twist_tab = np.stack([np.cos(twist), -np.sin(twist)]).astype(np.float32)
    return first_wide, first_thin, fwd_parts, inv_parts, last_parts, twist_tab


def split3(x):
    hi = x.astype(BF16)
    rest = x - hi.astype(F32)
    mid = rest.astype(BF16)
    low = (rest - mid.astype(F32)).astype(BF16)
    return hi, mid, low


def dot32(a, b):
    return jnp.dot(a, b, preferred_element_type=F32)


def turn_rows(block, into_ref, n_chunks, row, n_rows):
    turned = block.T
    n_chan = LANES // n_chunks
    for k in range(n_chunks):
        into_ref[k, pl.ds(row, n_chan, stride=n_rows), :] = turned[k * n_chan : (k + 1) * n_chan]


def far_first(n_dev):
    return sorted(range(1, n_dev), key=lambda off: -min(off, n_dev - off))


def spectrum_tools(group, n_high, tables, parts_ref):
    wide_ref, thin_ref, fwd_ref, inv_ref, last_ref, twist_ref = tables
    wide = 2 * LANES
    scale = 1.0 / (n_high * LANES)

    def complex_dot(tab_ref):
        return (
            dot32(parts_ref[:, 2 * wide :], tab_ref[:wide])
            + dot32(parts_ref[:, wide : 2 * wide], tab_ref[:wide])
            + dot32(parts_ref[:, :wide], tab_ref[wide : 2 * wide])
            + dot32(parts_ref[:, wide : 2 * wide], tab_ref[wide : 2 * wide])
            + dot32(parts_ref[:, :wide], tab_ref[2 * wide :])
            + dot32(parts_ref[:, :wide], tab_ref[:wide])
        )

    def store_parts(g, real, imag):
        for t, (re, im) in enumerate(zip(split3(real), split3(imag))):
            parts_ref[g * n_high : (g + 1) * n_high, 2 * t * LANES : (2 * t + 1) * LANES] = re
            parts_ref[g * n_high : (g + 1) * n_high, (2 * t + 1) * LANES : (2 * t + 2) * LANES] = im

    def spectrum(signals, exact):
        tr, ti = twist_ref[0], twist_ref[1]
        for g in range(0, group, 2):
            pair = jnp.concatenate([signals[g], signals[g + 1]], axis=1)
            if exact:
                short = pair.astype(BF16)
                coarse = dot32(thin_ref[...], jnp.concatenate([short, short, short], axis=0))
            else:
                hi, mid, low = split3(pair)
                coarse = dot32(wide_ref[...], jnp.concatenate([hi, mid, low, hi, mid, hi], axis=0))
            for j in range(2):
                re = coarse[:n_high, j * LANES : (j + 1) * LANES]
                im = coarse[n_high:, j * LANES : (j + 1) * LANES]
                store_parts(g + j, re * tr - im * ti, re * ti + im * tr)
        return complex_dot(fwd_ref)

    def signal(spec_a, spec_b):
        tr, ti = twist_ref[0], twist_ref[1]
        for g in range(group):
            rows = slice(g * n_high, (g + 1) * n_high)
            ar, ai = spec_a[rows, :LANES], spec_a[rows, LANES:]
            br, bi = spec_b[rows, :LANES], spec_b[rows, LANES:]
            store_parts(g, ar * br - ai * bi, ar * bi + ai * br)
        fine = complex_dot(inv_ref)
        results = []
        for g in range(0, group, 2):
            halves = []
            for j in range(2):
                rows = slice((g + j) * n_high, (g + j + 1) * n_high)
                re, im = fine[rows, :LANES] * scale, fine[rows, LANES:] * scale
                halves.append(jnp.concatenate([re * tr + im * ti, im * tr - re * ti], axis=0))
            hi, mid, low = split3(jnp.concatenate(halves, axis=1))
            d_hi = dot32(last_ref[...], hi)
            d_mid = dot32(last_ref[: 2 * n_high], mid)
            d_low = dot32(last_ref[:n_high], low)
            small = d_hi[2 * n_high :] + d_mid[n_high:] + d_low
            total = d_hi[:n_high] + ((d_hi[n_high : 2 * n_high] + d_mid[:n_high]) + small)
            results += [total[:, :LANES], total[:, LANES:]]
        return results

    return spectrum, signal


def hyena_body(n_dev, n_groups, units, group, u_hbm_ref, one_ref, two_ref, w_hbm_ref, w_out_ref, *refs):
    consts_in, refs = refs[:10], refs[10:]
    consts, const_sem, refs = refs[6:16], refs[16], refs[:6] + refs[17:]
    skip_one_ref, skip_two_ref, bias_ref, taps_ref, *tables = consts
    sent_ref, gate_ref, got_ref, back_ref, sum_ref, most_ref = refs[:6]
    u_ref, w_ref, p_ref, stage_ref, turned_ref, mixed_ref, halo_ref, tail_ref = refs[6:14]
    filt_ref, block_ref, done_ref, parts_ref, spec_one_ref, spec_two_ref, gated_ref, w_pair_ref = refs[14:22]
    (u_sem, w_sem, stage_sem, out_sem, halo_sem, hold_sem, share_sem, group_sem, filt_sem, sent_sem, got_sem, block_sem, done_sem, back_sem, pair_sem, sum_sem, most_sem, piece_sem, piece_got_sem) = refs[22:]
    me, my_group = lax.axis_index("sp"), lax.axis_index("dp")
    rows, depth = u_ref.shape
    n_rows = rows // LANES
    n_chunks = n_dev
    n_chan = LANES // n_chunks
    n_high = n_dev * n_rows
    model = w_hbm_ref.shape[1] // 3
    width = w_ref.shape[2]
    steps = model // width
    share_rows = units * n_rows
    first_unit = my_group * units
    which_mine = first_unit // n_chan
    mesh_id = pl.DeviceIdType.MESH

    def target(off):
        return lax.rem(me + off, n_dev)

    def own_rows(first):
        return pl.ds(pl.multiple_of(first * share_rows, share_rows), share_rows)


    def loading(item, off, which):
        cols = pl.ds(pl.multiple_of(target(off) * LANES, LANES), LANES)
        return pltpu.make_async_copy((one_ref, two_ref)[which].at[:, cols], stage_ref.at[item % 2], stage_sem.at[item % 2])

    def weights(which, step):
        cols = pl.ds(pl.multiple_of(which * model + step * width, width), width)
        slot = lax.rem(which + step, 2)
        return pltpu.make_async_copy(w_hbm_ref.at[:, cols], w_ref.at[slot], w_sem.at[slot])

    def u_part(start, size, idx):
        return pltpu.make_async_copy(u_hbm_ref.at[pl.ds(start, size), :], u_ref.at[pl.ds(start, size), :], u_sem.at[idx])

    def halo_send():
        return pltpu.make_async_remote_copy(tail_ref, halo_ref, halo_sem.at[0], halo_sem.at[1], device_id={"sp": target(1)}, device_id_type=mesh_id)

    def hold_of(dest):
        return done_ref.at[dest, :, pl.ds(0, share_rows), :]

    def share_send(off):
        dest = target(off)
        return pltpu.make_async_remote_copy(
            hold_of(dest), filt_ref.at[:, me, own_rows(my_group), :], hold_sem.at[off], share_sem.at[off], device_id={"sp": dest}, device_id_type=mesh_id
        )

    def group_send(k, off):
        mine = filt_ref.at[k, :, own_rows(my_group), :]
        return pltpu.make_async_remote_copy(
            mine, mine, group_sem.at[k], filt_sem.at[k], device_id={"dp": lax.rem(my_group + off, n_groups)}, device_id_type=mesh_id
        )

    def other_groups(k):
        same_size = filt_ref.at[k, :, pl.ds(0, (n_groups - 1) * share_rows), :]
        return pltpu.make_async_copy(same_size, same_size, filt_sem.at[k])

    def turned_out(slot, step):
        return pltpu.make_async_copy(turned_ref.at[slot], sent_ref.at[:, pl.ds(step * (width // LANES), width // LANES), slot], out_sem.at[slot])

    def mixed_out(step):
        return pltpu.make_async_copy(mixed_ref, gate_ref.at[:, pl.ds(step * (width // LANES), width // LANES)], out_sem.at[2])

    def sending(k, off):
        dest = target(off)
        return pltpu.make_async_remote_copy(
            sent_ref.at[k, dest], got_ref.at[k, me], sent_sem.at[k, off], got_sem.at[k, off], device_id={"sp": dest}, device_id_type=mesh_id
        )

    def block_in(k, off):
        src = lax.rem(me - off + n_dev, n_dev)
        from_ref = got_ref if off else sent_ref
        return pltpu.make_async_copy(from_ref.at[k, src], block_ref.at[src], block_sem.at[off])

    def returning(k, off):
        dest = target(off)
        return pltpu.make_async_remote_copy(
            done_ref.at[k, dest], back_ref.at[k, me], done_sem.at[k, off], back_sem.at[k, off], device_id={"sp": dest}, device_id_type=mesh_id
        )

    def storing(k):
        return pltpu.make_async_copy(done_ref.at[k, me], back_ref.at[k, me], done_sem.at[k, 0])

    last_pair = n_chunks - 2
    tile = filt_ref.shape[2]
    n_tiles = rows // tile
    piece = tile // LANES * n_chan

    def piece_of(q):
        return pl.ds(pl.multiple_of(q * piece, piece), piece)

    def returning_rows(q, off):
        dest = target(off)
        return pltpu.make_async_remote_copy(
            done_ref.at[pl.ds(last_pair, 2), dest, piece_of(q)],
            back_ref.at[pl.ds(last_pair, 2), me, piece_of(q)],
            piece_sem.at[q, off],
            piece_got_sem.at[q, off],
            device_id={"sp": dest},
            device_id_type=mesh_id,
        )

    def storing_rows(q):
        last = pl.ds(last_pair, 2)
        return pltpu.make_async_copy(done_ref.at[last, me, piece_of(q)], back_ref.at[last, me, piece_of(q)], piece_sem.at[q, 0])

    def constant(idx):
        return pltpu.make_async_copy(consts_in[idx], consts[idx], const_sem.at[idx])


    barrier = pltpu.get_barrier_semaphore()
    for off in range(1, n_dev):
        pl.semaphore_signal(barrier, inc=1, device_id={"sp": target(off)}, device_id_type=mesh_id)
    for off in range(1, n_groups):
        pl.semaphore_signal(barrier, inc=1, device_id={"dp": lax.rem(my_group + off, n_groups)}, device_id_type=mesh_id)

    order = far_first(n_dev) + [0]

    def load(item):
        for which in range(2):

            @pl.when(which_mine == which)
            def _():
                loading(item, order[item], which).start()

    load(0)
    u_part(rows - 16, 16, 1).start()
    for item, off in enumerate(order):
        if item + 1 < len(order):
            load(item + 1)
        if item == 0:
            u_part(0, rows - 16, 0).start()
            weights(0, 0).start()
            for idx in range(len(consts)):
                constant(idx).start()
        loading(item, off, 0).wait()
        if units < n_chan:
            into = turned_ref.at[0, :, 0]
        elif off:
            into = done_ref.at[target(off)]
        else:
            into = filt_ref.at[:, me, own_rows(my_group), :]
        together = math.gcd(n_rows, 4)

        @pl.loop(0, n_rows // together)
        def _(i):
            for j in range(together):
                r = i * together + j
                turn_rows(stage_ref[item % 2, pl.ds(pl.multiple_of(r * LANES, LANES), LANES), :], into, n_chunks, r, n_rows)

        if units < n_chan:
            start = pl.multiple_of(lax.rem(first_unit, n_chan) * n_rows, n_rows)
            share = turned_ref[0, :, 0, pl.ds(start, share_rows), :]
            if off:
                done_ref[target(off), :, pl.ds(0, share_rows), :] = share
            else:
                filt_ref[:, me, own_rows(my_group), :] = share
        if item == 0:
            u_part(rows - 16, 16, 1).wait()
            tail_ref[...] = u_ref[pl.ds(rows - 16, 16), :].astype(F32)[8:]
            pl.semaphore_wait(barrier, n_dev + n_groups - 2)
            halo_send().start()
        if off:
            share_send(off).start()


    for idx in range(len(consts)):
        constant(idx).wait()
    u_part(0, rows - 16, 0).wait()
    halo_send().wait()

    @pl.loop(0, steps)
    def _(step):
        for which in range(3):
            if which < 2:
                weights(which + 1, step).start()
            else:

                @pl.when(step + 1 < steps)
                def _():
                    weights(0, step + 1).start()

            weights(which, step).wait()
            w_now = w_ref.at[lax.rem(which + step, 2)]
            cols = pl.ds(pl.multiple_of(which * model + step * width, width), width)
            bias = bias_ref[:, cols]
            halo = (dot32(halo_ref[...].astype(BF16), w_now[...]) + bias).astype(BF16).astype(F32)
            p_ref[0:8, :] = jnp.where(me > 0, halo, 0.0)
            tile = 2 * LANES

            @pl.loop(0, rows // tile)
            def _(i):
                start = pl.multiple_of(i * tile, tile)
                proj = dot32(u_ref[pl.ds(start, tile), :], w_now[...]) + bias
                p_ref[pl.ds(start + 8, tile), :] = proj.astype(BF16).astype(F32)

            c0, c1, c2 = (taps_ref[t : t + 1, cols] for t in range(3))
            slot = 1 if which == 0 else 0

            @pl.when(step > 0)
            def _():
                if which == 1:
                    mixed_out(step - 1).wait()
                else:
                    turned_out(slot, step - 1).wait()

            @pl.loop(0, n_rows)
            def _(r):
                start = pl.multiple_of(r * LANES, LANES)
                window = p_ref[pl.ds(start, LANES + 8), :]
                mixed = c0 * window[8:] + c1 * window[7:-1] + c2 * window[6:-2]
                mixed = mixed.astype(BF16)
                for d in range(width // LANES):
                    block = mixed[:, d * LANES : (d + 1) * LANES].astype(F32)
                    if which != 1:
                        turn_rows(block, turned_ref.at[slot, :, d], n_chunks, r, n_rows)
                        continue
                    turned = block.T.astype(BF16)
                    for k in range(n_chunks):
                        at = pl.ds(pl.multiple_of(r * n_chan, n_chan), n_chan)
                        mixed_ref[k, d, at, :] = turned[k * n_chan : (k + 1) * n_chan]

            if which == 1:
                mixed_out(step).start()
            else:
                turned_out(slot, step).start()

    turned_out(0, steps - 1).wait()
    turned_out(1, steps - 1).wait()
    mixed_out(steps - 1).wait()

    @pl.loop(0, n_chunks)
    def _(k):
        for off in far_first(n_dev):
            sending(k, off).start()


    for off in range(1, n_dev):
        share_send(off).wait()

    @pl.loop(0, n_chunks)
    def _(k):
        for off in range(1, n_groups):
            group_send(k, off).start()


    spectrum, signal = spectrum_tools(group, n_high, tables, parts_ref)

    @pl.loop(0, n_chunks)
    def _(k):
        block_in(k, 0).start()
        for off in range(1, n_dev):
            sending(k, off).wait_recv()
            block_in(k, off).start()
        other_groups(k).wait()
        for off in range(n_dev):
            block_in(k, off).wait()

        @pl.loop(0, n_chan // group)
        def _(i):
            first = i * group

            def load_h(which, g):
                start = pl.multiple_of((which * n_chan + first + g) * n_rows, n_rows)
                return filt_ref[k, :, pl.ds(start, n_rows), :].reshape(n_high, LANES)

            def load_x(which, g):
                start = pl.multiple_of((first + g) * n_rows, n_rows)
                return block_ref[:, which, pl.ds(start, n_rows), :].reshape(n_high, LANES)

            chan = me * LANES + k * n_chan + first
            spec_one_ref[...] = spectrum([load_h(0, g) for g in range(group)], False)
            spec_two_ref[...] = spectrum([load_h(1, g) for g in range(group)], False)
            values = [load_x(0, g) for g in range(group)]
            conv = signal(spectrum(values, True), spec_one_ref)
            gated = [load_x(1, g) * (conv[g] + skip_one_ref[chan + g] * values[g]) for g in range(group)]
            conv = signal(spectrum(gated, False), spec_two_ref)
            for g in range(group):
                result = conv[g] + skip_two_ref[chan + g] * gated[g]
                done_ref[k, :, pl.ds(first + g, n_rows, stride=n_chan), :] = result.reshape(n_dev, n_rows, LANES)

        @pl.when(k < last_pair)
        def _():
            storing(k).start()
            for off in far_first(n_dev):
                returning(k, off).start()


    @pl.loop(0, n_tiles)
    def _(q):
        storing_rows(q).start()
        for off in far_first(n_dev):
            returning_rows(q, off).start()

    @pl.loop(0, n_chunks)
    def _(k):
        for off in range(1, n_dev):
            sending(k, off).wait_send()
        for off in range(1, n_groups):
            group_send(k, off).wait_send()


    @pl.loop(0, n_tiles)
    def _(q):
        for e in range(model // LANES):
            part = u_ref[pl.ds(pl.multiple_of(q * tile, tile), tile), e * LANES : (e + 1) * LANES]
            filt_ref[e, q] = part.astype(F32)

    def pair_in(k, j):
        return (
            pltpu.make_async_copy(back_ref.at[k], block_ref.at[:, j], pair_sem.at[j, 0]),
            pltpu.make_async_copy(gate_ref.at[k], mixed_ref.at[:, j], pair_sem.at[j, 1]),
            w_pair_in(k, j),
        )

    def w_pair_in(k, j):
        return pltpu.make_async_copy(w_out_ref.at[:, k], w_pair_ref.at[j], pair_sem.at[j, 2])

    def product(q):
        for t in range(tile // LANES):
            for j in range(2):
                at = pl.ds(pl.multiple_of((q * (tile // LANES) + t) * n_chan, n_chan), n_chan)
                gated = block_ref[:, j, at, :] * mixed_ref[:, j, at, :].astype(F32)
                gated_ref[t * LANES : (t + 1) * LANES, j * LANES : (j + 1) * LANES] = gated.reshape(LANES, LANES).T.astype(BF16)
        return dot32(gated_ref[...], w_pair_ref[...].reshape(2 * LANES, model))

    @pl.loop(0, n_chunks // 2 - 1)
    def _(p):
        for j in range(2):
            storing(2 * p + j).wait()
            for off in range(1, n_dev):
                returning(2 * p + j, off).wait()
            for copy in pair_in(2 * p + j, j):
                copy.start()
        for j in range(2):
            for copy in pair_in(2 * p + j, j):
                copy.wait()

        @pl.loop(0, n_tiles)
        def _(q):
            added = product(q)
            for e in range(model // LANES):
                filt_ref[e, q] = filt_ref[e, q] + added[:, e * LANES : (e + 1) * LANES]

    sum_out = pltpu.make_async_copy(filt_ref.at[:, n_tiles - 1], sum_ref, sum_sem)
    sum_out.start()

    def rows_of(q):
        return pl.ds(pl.multiple_of(q * tile, tile), tile)

    def most_out(q):
        return pltpu.make_async_copy(u_ref.at[rows_of(q)], most_ref.at[rows_of(q)], most_sem.at[q])

    def rows_in(q, j):
        k = last_pair + j
        return (
            pltpu.make_async_copy(back_ref.at[k, :, piece_of(q)], block_ref.at[:, j, piece_of(q)], pair_sem.at[j, 0]),
            pltpu.make_async_copy(gate_ref.at[k, :, piece_of(q)], mixed_ref.at[:, j, piece_of(q)], pair_sem.at[j, 1]),
        )

    if n_tiles > 1:
        for j in range(2):
            w_pair_in(last_pair + j, j).start()
        for j in range(2):
            w_pair_in(last_pair + j, j).wait()

    @pl.loop(0, n_tiles - 1)
    def _(q):
        storing_rows(q).wait()
        for off in range(1, n_dev):
            returning_rows(q, off).wait()
        for j in range(2):
            for copy in rows_in(q, j):
                copy.start()
        for j in range(2):
            for copy in rows_in(q, j):
                copy.wait()
        added = product(q)
        for e in range(model // LANES):
            cols = slice(e * LANES, (e + 1) * LANES)
            u_ref[rows_of(q), cols] = (filt_ref[e, q] + added[:, cols]).astype(BF16)
        most_out(q).start()

    storing_rows(n_tiles - 1).wait()
    for off in range(1, n_dev):
        returning_rows(n_tiles - 1, off).wait()
    sum_out.wait()

    @pl.loop(0, n_tiles - 1)
    def _(q):
        most_out(q).wait()


def hyena(skip_one, skip_two, u, filt_one, filt_two, w_in, w_out, bias, taps, tables, n_dev, n_groups, units, group=4):
    rows, depth = u.shape
    model = w_in.shape[1] // 3
    width = 2 * LANES
    n_rows = rows // LANES
    n_chunks = n_dev
    n_high = n_dev * n_rows
    chunk_rows = LANES // n_chunks * n_rows
    tile = 2 * chunk_rows
    hbm_spec = pl.BlockSpec(memory_space=pltpu.HBM)
    consts = (bias, taps, *tables)
    dma = pltpu.SemaphoreType.DMA
    return pl.pallas_call(
        functools.partial(hyena_body, n_dev, n_groups, units, group),
        in_specs=[hbm_spec] * (7 + len(consts)),
        out_specs=[hbm_spec] * 6,
        out_shape=[
            jax.ShapeDtypeStruct((n_chunks, n_dev, 2, chunk_rows, LANES), F32),
            jax.ShapeDtypeStruct((n_chunks, n_dev, chunk_rows, LANES), BF16),
            jax.ShapeDtypeStruct((n_chunks, n_dev, 2, chunk_rows, LANES), F32),
            jax.ShapeDtypeStruct((n_chunks, n_dev, chunk_rows, LANES), F32),
            jax.ShapeDtypeStruct((model // LANES, tile, LANES), F32),
            jax.ShapeDtypeStruct((rows, model), BF16),
        ],
        scratch_shapes=[
            pltpu.SMEM(skip_one.shape, F32),
            pltpu.SMEM(skip_two.shape, F32),
            *[pltpu.VMEM(c.shape, c.dtype) for c in consts],
            dma((2 + len(consts),)),
            pltpu.VMEM((rows, depth), BF16),
            pltpu.VMEM((2, depth, width), BF16),
            pltpu.VMEM((rows + 8, width), F32),
            pltpu.VMEM((2, rows, LANES), F32),
            pltpu.VMEM((2, n_chunks, width // LANES, chunk_rows, LANES), F32),
            pltpu.VMEM((n_chunks, width // LANES, chunk_rows, LANES), BF16),
            pltpu.VMEM((8, depth), F32),
            pltpu.VMEM((8, depth), F32),
            pltpu.VMEM((n_chunks, n_dev, 2 * chunk_rows, LANES), F32),
            pltpu.VMEM((n_dev, 2, chunk_rows, LANES), F32),
            pltpu.VMEM((n_chunks, n_dev, chunk_rows, LANES), F32),
            pltpu.VMEM((group * n_high, 6 * LANES), BF16),
            pltpu.VMEM((group * n_high, 2 * LANES), F32),
            pltpu.VMEM((group * n_high, 2 * LANES), F32),
            pltpu.VMEM((2 * chunk_rows, 2 * LANES), BF16),
            pltpu.VMEM((2, n_dev, LANES // n_chunks, model), BF16),
            dma((2,)),
            dma((2,)),
            dma((2,)),
            dma((3,)),
            dma((2,)),
            dma((n_dev,)),
            dma((n_dev,)),
            dma((n_chunks,)),
            dma((n_chunks,)),
            dma((n_chunks, n_dev)),
            dma((n_chunks, n_dev)),
            dma((n_dev,)),
            dma((n_chunks, n_dev)),
            dma((n_chunks, n_dev)),
            dma((2, 3)),
            dma,
            dma((rows // tile,)),
            dma((rows // tile, n_dev)),
            dma((rows // tile, n_dev)),
        ],
        cost_estimate=pl.CostEstimate(flops=10**11, bytes_accessed=100 * 2**20, transcendentals=0),
        compiler_params=pltpu.CompilerParams(collective_id=0, has_side_effects=True, vmem_limit_bytes=54 * 2**20),
        name="hyena",
    )(u, filt_one, filt_two, w_in, w_out, skip_one, skip_two, *consts)


def finish_body(n_rows, most_hbm_ref, sum_hbm_ref, gate_hbm_ref, back_hbm_ref, w_hbm_ref, out_hbm_ref, *refs):
    sum_ref, gate_ref, back_ref, w_ref, out_ref, gated_ref, in_sem, w_sem, most_sem, out_sem = refs
    first = gate_hbm_ref.shape[0] - 2
    rows = out_ref.shape[0]
    first_row = rows - sum_ref.shape[1]
    tile = n_rows * LANES
    n_tiles = sum_ref.shape[1] // tile
    n_most = first_row // sum_ref.shape[1]

    def tile_in(i):
        at = pl.ds(i * tile, tile)
        narrow, wide = pl.ds(i * n_rows, n_rows), pl.ds(first_row // LANES + i * n_rows, n_rows)
        return (
            pltpu.make_async_copy(sum_hbm_ref.at[:, at], sum_ref.at[:, at], in_sem.at[i, 0]),
            pltpu.make_async_copy(gate_hbm_ref.at[pl.ds(first, 2), :, wide], gate_ref.at[:, :, narrow], in_sem.at[i, 1]),
            pltpu.make_async_copy(back_hbm_ref.at[pl.ds(first, 2), :, wide], back_ref.at[:, :, narrow], in_sem.at[i, 2]),
        )

    def most(i, out):
        at = pl.ds(i * sum_ref.shape[1], sum_ref.shape[1])
        if out:
            return pltpu.make_async_copy(out_ref.at[at], out_hbm_ref.at[at], most_sem.at[i])
        return pltpu.make_async_copy(most_hbm_ref.at[at], out_ref.at[at], most_sem.at[i])

    def tile_out(i):
        at = pl.ds(first_row + i * tile, tile)
        return pltpu.make_async_copy(out_ref.at[at], out_hbm_ref.at[at], out_sem.at[i])

    w_in = pltpu.make_async_copy(w_hbm_ref.at[:, pl.ds(first, 2)], w_ref, w_sem)
    w_in.start()
    for i in range(n_tiles):
        for copy in tile_in(i):
            copy.start()
    for i in range(n_most):
        most(i, False).start()
    w_in.wait()
    w_pair = jnp.concatenate([w_ref[:, j].reshape(LANES, w_ref.shape[3]) for j in range(2)], axis=0)
    for i in range(n_tiles):
        for copy in tile_in(i):
            copy.wait()
        for r in range(n_rows):
            for j in range(2):
                gated = back_ref[j, :, i * n_rows + r] * gate_ref[j, :, i * n_rows + r].astype(F32)
                gated_ref[r * LANES : (r + 1) * LANES, j * LANES : (j + 1) * LANES] = gated.reshape(LANES, LANES).T.astype(BF16)
        added = dot32(gated_ref[...], w_pair)
        for e in range(sum_ref.shape[0]):
            cols = slice(e * LANES, (e + 1) * LANES)
            out_ref[first_row + i * tile : first_row + (i + 1) * tile, cols] = (sum_ref[e, i * tile : (i + 1) * tile] + added[:, cols]).astype(BF16)
        tile_out(i).start()
    for i in range(n_most):
        most(i, False).wait()
        most(i, True).start()
    for i in range(n_tiles):
        tile_out(i).wait()
    for i in range(n_most):
        most(i, True).wait()


def finish(most, partial, gate, back, w_out, n_rows=2):
    _, n_src, _, n_chan, _ = back.shape
    rows, model = most.shape
    last_rows = partial.shape[1]
    n_tiles = last_rows // (n_rows * LANES)
    hbm_spec = pl.BlockSpec(memory_space=pltpu.HBM)
    returned = (2, n_src, last_rows // LANES, n_chan, LANES)
    return pl.pallas_call(
        functools.partial(finish_body, n_rows),
        in_specs=[hbm_spec] * 5,
        out_specs=hbm_spec,
        out_shape=jax.ShapeDtypeStruct((rows, model), BF16),
        scratch_shapes=[
            pltpu.VMEM(partial.shape, F32),
            pltpu.VMEM(returned, BF16),
            pltpu.VMEM(returned, F32),
            pltpu.VMEM((n_src, 2, n_chan, model), BF16),
            pltpu.VMEM((rows, model), BF16),
            pltpu.VMEM((n_rows * LANES, 2 * LANES), BF16),
            pltpu.SemaphoreType.DMA((n_tiles, 3)),
            pltpu.SemaphoreType.DMA,
            pltpu.SemaphoreType.DMA((max(1, rows // last_rows - 1),)),
            pltpu.SemaphoreType.DMA((n_tiles,)),
        ],
        cost_estimate=pl.CostEstimate(flops=4 * last_rows * model * LANES, bytes_accessed=11 * 2**20, transcendentals=0),
        compiler_params=pltpu.CompilerParams(vmem_limit_bytes=56 * 2**20),
        name="finish",
    )(most, partial, gate, back, w_out)


def solution(mesh):
    n_dev, n_groups = mesh.shape["sp"], mesh.shape["dp"]
    n_chunks = n_dev
    n_chan = LANES // n_chunks
    if n_groups < 2 or (2 * n_chan) % n_groups:
        raise ValueError("uneven groups")
    units = 2 * n_chan // n_groups

    def local_step(u_in, w_in, b_in, conv_taps, w_out, skip_one, skip_two, filt_one, filt_two):
        u = u_in[0]
        rows = u.shape[0]
        tables = [jnp.asarray(t) for t in transform_tables(rows * n_dev)]
        w_blocks = w_out.reshape(n_dev, n_chunks, n_chan, w_out.shape[1])
        _, gate, _, back, partial, most = hyena(
            skip_one, skip_two, u, filt_one, filt_two, w_in, w_blocks, b_in[None], conv_taps, tables, n_dev, n_groups, units
        )
        by_row = (n_chunks, n_dev, rows // LANES, n_chan, LANES)
        return finish(most, partial, gate.reshape(by_row), back.reshape(by_row), w_blocks)[None]

    seq_spec = P("dp", "sp", None)
    filt_spec = P("sp", None)
    return jax.shard_map(
        local_step,
        mesh=mesh,
        in_specs=(seq_spec, P(), P(), P(), P(), P(), P(), filt_spec, filt_spec),
        out_specs=seq_spec,
        check_vma=False,
    )
```

```python
import functools
import math
import jax
import jax.numpy as jnp
import numpy as np
from jax import lax
from jax.experimental import pallas as pl
from jax.experimental.pallas import tpu as pltpu
from jax.sharding import PartitionSpec as P

LANES = 128
F32 = jnp.float32
BF16 = jnp.bfloat16


def split_table(table, n_parts=3):
    parts, rest = [], np.asarray(table, np.float64)
    for _ in range(n_parts):
        part = rest.astype(jnp.bfloat16)
        parts.append(part)
        rest = rest - part.astype(np.float64)
    return parts


def transform_tables(seq_len):
    n_high = seq_len // LANES
    quarter = np.arange(n_high)[:, None] + 0.25
    high = 2.0 * np.pi * quarter * np.arange(n_high)[None, :] / n_high
    twist = 2.0 * np.pi * quarter * np.arange(LANES)[None, :] / seq_len
    low = 2.0 * np.pi * np.outer(np.arange(LANES), np.arange(LANES)) / LANES
    first = np.concatenate([np.cos(high), -np.sin(high)], axis=0)
    last = np.concatenate([np.cos(high.T), -np.sin(high.T)], axis=1)
    er, ei = np.cos(low), -np.sin(low)
    fwd = np.block([[er, ei], [-ei, er]])
    inv = np.block([[er, -ei], [ei, er]])
    a, b, c = split_table(first)
    first_wide = np.concatenate([a, a, a, b, b, c], axis=1)
    first_thin = np.concatenate([a, b, c], axis=1)
    fwd_parts = np.concatenate(split_table(fwd), axis=0)
    inv_parts = np.concatenate(split_table(inv), axis=0)
    last_parts = np.concatenate(split_table(last), axis=0)
    twist_tab = np.stack([np.cos(twist), -np.sin(twist)]).astype(np.float32)
    return first_wide, first_thin, fwd_parts, inv_parts, last_parts, twist_tab


def split3(x):
    hi = x.astype(BF16)
    rest = x - hi.astype(F32)
    mid = rest.astype(BF16)
    low = (rest - mid.astype(F32)).astype(BF16)
    return hi, mid, low


def dot32(a, b):
    return jnp.dot(a, b, preferred_element_type=F32)


def turn_rows(block, into_ref, n_chunks, row, n_rows):
    turned = block.T
    n_chan = LANES // n_chunks
    for k in range(n_chunks):
        into_ref[k, pl.ds(row, n_chan, stride=n_rows), :] = turned[k * n_chan : (k + 1) * n_chan]


def far_first(n_dev):
    return sorted(range(1, n_dev), key=lambda off: -min(off, n_dev - off))


def send_spans(n_chunks):
    half = n_chunks // 2
    return [(k, 1) for k in range(half)] + [(k, 2) for k in range(half, n_chunks, 2)] if half % 2 == 0 else [(k, 1) for k in range(n_chunks)]


def row_spans(n_tiles):
    return [(0, n_tiles - 2), (n_tiles - 2, 1), (n_tiles - 1, 1)] if n_tiles > 2 else [(q, 1) for q in range(n_tiles)]


def spectrum_tools(group, n_high, tables, parts_ref):
    wide_ref, thin_ref, fwd_ref, inv_ref, last_ref, twist_ref = tables
    wide = 2 * LANES
    scale = 1.0 / (n_high * LANES)

    def complex_dot(tab_ref):
        return (
            dot32(parts_ref[:, 2 * wide :], tab_ref[:wide])
            + dot32(parts_ref[:, wide : 2 * wide], tab_ref[:wide])
            + dot32(parts_ref[:, :wide], tab_ref[wide : 2 * wide])
            + dot32(parts_ref[:, wide : 2 * wide], tab_ref[wide : 2 * wide])
            + dot32(parts_ref[:, :wide], tab_ref[2 * wide :])
            + dot32(parts_ref[:, :wide], tab_ref[:wide])
        )

    def store_parts(g, real, imag):
        for t, (re, im) in enumerate(zip(split3(real), split3(imag))):
            parts_ref[g * n_high : (g + 1) * n_high, 2 * t * LANES : (2 * t + 1) * LANES] = re
            parts_ref[g * n_high : (g + 1) * n_high, (2 * t + 1) * LANES : (2 * t + 2) * LANES] = im

    def spectrum(signals, exact):
        tr, ti = twist_ref[0], twist_ref[1]
        for g in range(0, group, 2):
            pair = jnp.concatenate([signals[g], signals[g + 1]], axis=1)
            if exact:
                short = pair.astype(BF16)
                coarse = dot32(thin_ref[...], jnp.concatenate([short, short, short], axis=0))
            else:
                hi, mid, low = split3(pair)
                coarse = dot32(wide_ref[...], jnp.concatenate([hi, mid, low, hi, mid, hi], axis=0))
            for j in range(2):
                re = coarse[:n_high, j * LANES : (j + 1) * LANES]
                im = coarse[n_high:, j * LANES : (j + 1) * LANES]
                store_parts(g + j, re * tr - im * ti, re * ti + im * tr)
        return complex_dot(fwd_ref)

    def signal(spec_a, spec_b):
        tr, ti = twist_ref[0], twist_ref[1]
        for g in range(group):
            rows = slice(g * n_high, (g + 1) * n_high)
            ar, ai = spec_a[rows, :LANES], spec_a[rows, LANES:]
            br, bi = spec_b[rows, :LANES], spec_b[rows, LANES:]
            store_parts(g, ar * br - ai * bi, ar * bi + ai * br)
        fine = complex_dot(inv_ref)
        results = []
        for g in range(0, group, 2):
            halves = []
            for j in range(2):
                rows = slice((g + j) * n_high, (g + j + 1) * n_high)
                re, im = fine[rows, :LANES] * scale, fine[rows, LANES:] * scale
                halves.append(jnp.concatenate([re * tr + im * ti, im * tr - re * ti], axis=0))
            hi, mid, low = split3(jnp.concatenate(halves, axis=1))
            d_hi = dot32(last_ref[...], hi)
            d_mid = dot32(last_ref[: 2 * n_high], mid)
            d_low = dot32(last_ref[:n_high], low)
            small = d_hi[2 * n_high :] + d_mid[n_high:] + d_low
            total = d_hi[:n_high] + ((d_hi[n_high : 2 * n_high] + d_mid[:n_high]) + small)
            results += [total[:, :LANES], total[:, LANES:]]
        return results

    return spectrum, signal


def hyena_body(n_dev, n_groups, units, group, u_hbm_ref, one_ref, two_ref, w_hbm_ref, w_out_ref, *refs):
    consts_in, refs = refs[:10], refs[10:]
    consts, const_sem, refs = refs[6:16], refs[16], refs[:6] + refs[17:]
    skip_one_ref, skip_two_ref, bias_ref, taps_ref, *tables = consts
    sent_ref, gate_ref, got_ref, back_ref, sum_ref, most_ref = refs[:6]
    u_ref, w_ref, p_ref, stage_ref, turned_ref, mixed_ref, halo_ref, tail_ref = refs[6:14]
    filt_ref, block_ref, done_ref, parts_ref, spec_one_ref, spec_two_ref, gated_ref, w_pair_ref = refs[14:22]
    (u_sem, w_sem, stage_sem, out_sem, halo_sem, hold_sem, share_sem, group_sem, filt_sem, sent_sem, got_sem, block_sem, done_sem, back_sem, pair_sem, sum_sem, most_sem, piece_sem, piece_got_sem) = refs[22:]
    me, my_group = lax.axis_index("sp"), lax.axis_index("dp")
    rows, depth = u_ref.shape
    n_rows = rows // LANES
    n_chunks = n_dev
    n_chan = LANES // n_chunks
    n_high = n_dev * n_rows
    model = w_hbm_ref.shape[1] // 3
    width = w_ref.shape[2]
    steps = model // width
    share_rows = units * n_rows
    first_unit = my_group * units
    which_mine = first_unit // n_chan
    mesh_id = pl.DeviceIdType.MESH

    def target(off):
        return lax.rem(me + off, n_dev)

    def own_rows(first):
        return pl.ds(pl.multiple_of(first * share_rows, share_rows), share_rows)


    def loading(item, off, which):
        cols = pl.ds(pl.multiple_of(target(off) * LANES, LANES), LANES)
        return pltpu.make_async_copy((one_ref, two_ref)[which].at[:, cols], stage_ref.at[item % 2], stage_sem.at[item % 2])

    def weights(which, step):
        cols = pl.ds(pl.multiple_of(which * model + step * width, width), width)
        slot = lax.rem(which + step, 2)
        return pltpu.make_async_copy(w_hbm_ref.at[:, cols], w_ref.at[slot], w_sem.at[slot])

    def u_part(start, size, idx):
        return pltpu.make_async_copy(u_hbm_ref.at[pl.ds(start, size), :], u_ref.at[pl.ds(start, size), :], u_sem.at[idx])

    def halo_send():
        return pltpu.make_async_remote_copy(tail_ref, halo_ref, halo_sem.at[0], halo_sem.at[1], device_id={"sp": target(1)}, device_id_type=mesh_id)

    def hold_of(dest):
        return done_ref.at[dest, :, pl.ds(0, share_rows), :]

    def share_send(off):
        dest = target(off)
        return pltpu.make_async_remote_copy(
            hold_of(dest), filt_ref.at[:, me, own_rows(my_group), :], hold_sem.at[off], share_sem.at[off], device_id={"sp": dest}, device_id_type=mesh_id
        )

    def group_send(k, off):
        mine = filt_ref.at[k, :, own_rows(my_group), :]
        return pltpu.make_async_remote_copy(
            mine, mine, group_sem.at[k], filt_sem.at[k], device_id={"dp": lax.rem(my_group + off, n_groups)}, device_id_type=mesh_id
        )

    def other_groups(k):
        same_size = filt_ref.at[k, :, pl.ds(0, (n_groups - 1) * share_rows), :]
        return pltpu.make_async_copy(same_size, same_size, filt_sem.at[k])

    def turned_out(slot, step):
        return pltpu.make_async_copy(turned_ref.at[slot], sent_ref.at[:, pl.ds(step * (width // LANES), width // LANES), slot], out_sem.at[slot])

    def mixed_out(step):
        return pltpu.make_async_copy(mixed_ref, gate_ref.at[:, pl.ds(step * (width // LANES), width // LANES)], out_sem.at[2])

    def sending(k, off, span):
        dest, chunks = target(off), pl.ds(k, span)
        return pltpu.make_async_remote_copy(
            sent_ref.at[chunks, dest], got_ref.at[chunks, me], sent_sem.at[k, off], got_sem.at[k, off], device_id={"sp": dest}, device_id_type=mesh_id
        )

    def block_in(k, off):
        src = lax.rem(me - off + n_dev, n_dev)
        from_ref = got_ref if off else sent_ref
        return pltpu.make_async_copy(from_ref.at[k, src], block_ref.at[src], block_sem.at[off])

    def returning(k, off):
        dest = target(off)
        return pltpu.make_async_remote_copy(
            done_ref.at[pl.ds(k, 2), dest],
            back_ref.at[pl.ds(k, 2), me],
            done_sem.at[k, off],
            back_sem.at[k, off],
            device_id={"sp": dest},
            device_id_type=mesh_id,
        )

    def storing(k):
        return pltpu.make_async_copy(done_ref.at[pl.ds(k, 2), me], back_ref.at[pl.ds(k, 2), me], done_sem.at[k, 0])

    last_pair = n_chunks - 2
    tile = filt_ref.shape[2]
    n_tiles = rows // tile
    piece = tile // LANES * n_chan

    def piece_of(part):
        return pl.ds(part[0] * piece, part[1] * piece)

    def returning_rows(part, off):
        dest = target(off)
        return pltpu.make_async_remote_copy(
            done_ref.at[pl.ds(last_pair, 2), dest, piece_of(part)],
            back_ref.at[pl.ds(last_pair, 2), me, piece_of(part)],
            piece_sem.at[part[0], off],
            piece_got_sem.at[part[0], off],
            device_id={"sp": dest},
            device_id_type=mesh_id,
        )

    def storing_rows(part):
        last = pl.ds(last_pair, 2)
        return pltpu.make_async_copy(done_ref.at[last, me, piece_of(part)], back_ref.at[last, me, piece_of(part)], piece_sem.at[part[0], 0])

    def constant(idx):
        return pltpu.make_async_copy(consts_in[idx], consts[idx], const_sem.at[idx])


    barrier = pltpu.get_barrier_semaphore()
    for off in range(1, n_dev):
        pl.semaphore_signal(barrier, inc=1, device_id={"sp": target(off)}, device_id_type=mesh_id)
    for off in range(1, n_groups):
        pl.semaphore_signal(barrier, inc=1, device_id={"dp": lax.rem(my_group + off, n_groups)}, device_id_type=mesh_id)

    order = far_first(n_dev) + [0]

    def load(item):
        for which in range(2):

            @pl.when(which_mine == which)
            def _():
                loading(item, order[item], which).start()

    load(0)
    u_part(rows - 16, 16, 1).start()
    for item, off in enumerate(order):
        if item + 1 < len(order):
            load(item + 1)
        if item == 0:
            u_part(0, rows - 16, 0).start()
            weights(0, 0).start()
            for idx in range(len(consts)):
                constant(idx).start()
        loading(item, off, 0).wait()
        if units < n_chan:
            into = turned_ref.at[0, :, 0]
        elif off:
            into = done_ref.at[target(off)]
        else:
            into = filt_ref.at[:, me, own_rows(my_group), :]
        together = math.gcd(n_rows, 4)

        @pl.loop(0, n_rows // together)
        def _(i):
            for j in range(together):
                r = i * together + j
                turn_rows(stage_ref[item % 2, pl.ds(pl.multiple_of(r * LANES, LANES), LANES), :], into, n_chunks, r, n_rows)

        if units < n_chan:
            start = pl.multiple_of(lax.rem(first_unit, n_chan) * n_rows, n_rows)
            share = turned_ref[0, :, 0, pl.ds(start, share_rows), :]
            if off:
                done_ref[target(off), :, pl.ds(0, share_rows), :] = share
            else:
                filt_ref[:, me, own_rows(my_group), :] = share
        if item == 0:
            u_part(rows - 16, 16, 1).wait()
            tail_ref[...] = u_ref[pl.ds(rows - 16, 16), :].astype(F32)[8:]
            pl.semaphore_wait(barrier, n_dev + n_groups - 2)
            halo_send().start()
        if off:
            share_send(off).start()


    for idx in range(len(consts)):
        constant(idx).wait()
    u_part(0, rows - 16, 0).wait()
    halo_send().wait()

    @pl.loop(0, steps)
    def _(step):
        for which in range(3):
            if which < 2:
                weights(which + 1, step).start()
            else:

                @pl.when(step + 1 < steps)
                def _():
                    weights(0, step + 1).start()

            weights(which, step).wait()
            w_now = w_ref.at[lax.rem(which + step, 2)]
            cols = pl.ds(pl.multiple_of(which * model + step * width, width), width)
            bias = bias_ref[:, cols]
            halo = (dot32(halo_ref[...].astype(BF16), w_now[...]) + bias).astype(BF16).astype(F32)
            p_ref[0:8, :] = jnp.where(me > 0, halo, 0.0)
            tile = 2 * LANES

            @pl.loop(0, rows // tile)
            def _(i):
                start = pl.multiple_of(i * tile, tile)
                proj = dot32(u_ref[pl.ds(start, tile), :], w_now[...]) + bias
                p_ref[pl.ds(start + 8, tile), :] = proj.astype(BF16).astype(F32)

            c0, c1, c2 = (taps_ref[t : t + 1, cols] for t in range(3))
            slot = 1 if which == 0 else 0

            @pl.when(step > 0)
            def _():
                if which == 1:
                    mixed_out(step - 1).wait()
                else:
                    turned_out(slot, step - 1).wait()

            @pl.loop(0, n_rows)
            def _(r):
                start = pl.multiple_of(r * LANES, LANES)
                window = p_ref[pl.ds(start, LANES + 8), :]
                mixed = c0 * window[8:] + c1 * window[7:-1] + c2 * window[6:-2]
                mixed = mixed.astype(BF16)
                for d in range(width // LANES):
                    block = mixed[:, d * LANES : (d + 1) * LANES].astype(F32)
                    if which != 1:
                        turn_rows(block, turned_ref.at[slot, :, d], n_chunks, r, n_rows)
                        continue
                    turned = block.T.astype(BF16)
                    for k in range(n_chunks):
                        at = pl.ds(pl.multiple_of(r * n_chan, n_chan), n_chan)
                        mixed_ref[k, d, at, :] = turned[k * n_chan : (k + 1) * n_chan]

            if which == 1:
                mixed_out(step).start()
            else:
                turned_out(slot, step).start()

    turned_out(0, steps - 1).wait()
    turned_out(1, steps - 1).wait()
    mixed_out(steps - 1).wait()

    spans = send_spans(n_chunks)
    for k, span in spans:
        for off in far_first(n_dev):
            sending(k, off, span).start()


    for off in range(1, n_dev):
        share_send(off).wait()

    @pl.loop(0, n_chunks)
    def _(k):
        for off in range(1, n_groups):
            group_send(k, off).start()


    spectrum, signal = spectrum_tools(group, n_high, tables, parts_ref)

    @pl.loop(0, n_chunks)
    def _(k):
        block_in(k, 0).start()
        for span in (1, 2):
            firsts = [first for first, size in spans if size == span]
            if firsts:
                begins = jnp.logical_and(k >= firsts[0], k <= firsts[-1])
                if span == 2:
                    begins = jnp.logical_and(begins, lax.rem(k - firsts[0], 2) == 0)

                @pl.when(begins)
                def _():
                    for off in range(1, n_dev):
                        sending(k, off, span).wait_recv()

        for off in range(1, n_dev):
            block_in(k, off).start()
        other_groups(k).wait()
        for off in range(n_dev):
            block_in(k, off).wait()

        @pl.loop(0, n_chan // group)
        def _(i):
            first = i * group

            def load_h(which, g):
                start = pl.multiple_of((which * n_chan + first + g) * n_rows, n_rows)
                return filt_ref[k, :, pl.ds(start, n_rows), :].reshape(n_high, LANES)

            def load_x(which, g):
                start = pl.multiple_of((first + g) * n_rows, n_rows)
                return block_ref[:, which, pl.ds(start, n_rows), :].reshape(n_high, LANES)

            chan = me * LANES + k * n_chan + first
            spec_one_ref[...] = spectrum([load_h(0, g) for g in range(group)], False)
            spec_two_ref[...] = spectrum([load_h(1, g) for g in range(group)], False)
            values = [load_x(0, g) for g in range(group)]
            conv = signal(spectrum(values, True), spec_one_ref)
            gated = [load_x(1, g) * (conv[g] + skip_one_ref[chan + g] * values[g]) for g in range(group)]
            conv = signal(spectrum(gated, False), spec_two_ref)
            for g in range(group):
                result = conv[g] + skip_two_ref[chan + g] * gated[g]
                done_ref[k, :, pl.ds(first + g, n_rows, stride=n_chan), :] = result.reshape(n_dev, n_rows, LANES)

        @pl.when(jnp.logical_and(k < last_pair, lax.rem(k, 2) == 1))
        def _():
            storing(k - 1).start()
            for off in far_first(n_dev):
                returning(k - 1, off).start()


    parts = row_spans(n_tiles)
    for part in parts:
        storing_rows(part).start()
        for off in far_first(n_dev):
            returning_rows(part, off).start()

    for k, span in spans:
        for off in range(1, n_dev):
            sending(k, off, span).wait_send()

    @pl.loop(0, n_chunks)
    def _(k):
        for off in range(1, n_groups):
            group_send(k, off).wait_send()


    @pl.loop(0, n_tiles)
    def _(q):
        for e in range(model // LANES):
            part = u_ref[pl.ds(pl.multiple_of(q * tile, tile), tile), e * LANES : (e + 1) * LANES]
            filt_ref[e, q] = part.astype(F32)

    def pair_in(k, j):
        return (
            pltpu.make_async_copy(back_ref.at[k], block_ref.at[:, j], pair_sem.at[j, 0]),
            pltpu.make_async_copy(gate_ref.at[k], mixed_ref.at[:, j], pair_sem.at[j, 1]),
            w_pair_in(k, j),
        )

    def w_pair_in(k, j):
        return pltpu.make_async_copy(w_out_ref.at[:, k], w_pair_ref.at[j], pair_sem.at[j, 2])

    def product(q):
        for t in range(tile // LANES):
            for j in range(2):
                at = pl.ds(pl.multiple_of((q * (tile // LANES) + t) * n_chan, n_chan), n_chan)
                gated = block_ref[:, j, at, :] * mixed_ref[:, j, at, :].astype(F32)
                gated_ref[t * LANES : (t + 1) * LANES, j * LANES : (j + 1) * LANES] = gated.reshape(LANES, LANES).T.astype(BF16)
        return dot32(gated_ref[...], w_pair_ref[...].reshape(2 * LANES, model))

    @pl.loop(0, n_chunks // 2 - 1)
    def _(p):
        storing(2 * p).wait()
        for off in range(1, n_dev):
            returning(2 * p, off).wait()
        for j in range(2):
            for copy in pair_in(2 * p + j, j):
                copy.start()
        for j in range(2):
            for copy in pair_in(2 * p + j, j):
                copy.wait()

        @pl.loop(0, n_tiles)
        def _(q):
            added = product(q)
            for e in range(model // LANES):
                filt_ref[e, q] = filt_ref[e, q] + added[:, e * LANES : (e + 1) * LANES]

    sum_out = pltpu.make_async_copy(filt_ref.at[:, n_tiles - 1], sum_ref, sum_sem)
    sum_out.start()

    def rows_of(q):
        return pl.ds(pl.multiple_of(q * tile, tile), tile)

    def most_out(q):
        return pltpu.make_async_copy(u_ref.at[rows_of(q)], most_ref.at[rows_of(q)], most_sem.at[q])

    def rows_in(part, j):
        k, at = last_pair + j, piece_of(part)
        return (
            pltpu.make_async_copy(back_ref.at[k, :, at], block_ref.at[:, j, at], pair_sem.at[j, 0]),
            pltpu.make_async_copy(gate_ref.at[k, :, at], mixed_ref.at[:, j, at], pair_sem.at[j, 1]),
        )

    if n_tiles > 1:
        for j in range(2):
            w_pair_in(last_pair + j, j).start()
        for j in range(2):
            w_pair_in(last_pair + j, j).wait()

    for part in parts[:-1]:
        storing_rows(part).wait()
        for off in range(1, n_dev):
            returning_rows(part, off).wait()
        for j in range(2):
            for copy in rows_in(part, j):
                copy.start()
        for j in range(2):
            for copy in rows_in(part, j):
                copy.wait()

        @pl.loop(part[0], part[0] + part[1])
        def _(q):
            added = product(q)
            for e in range(model // LANES):
                cols = slice(e * LANES, (e + 1) * LANES)
                u_ref[rows_of(q), cols] = (filt_ref[e, q] + added[:, cols]).astype(BF16)
            most_out(q).start()

    storing_rows(parts[-1]).wait()
    for off in range(1, n_dev):
        returning_rows(parts[-1], off).wait()
    sum_out.wait()

    @pl.loop(0, n_tiles - 1)
    def _(q):
        most_out(q).wait()


def hyena(skip_one, skip_two, u, filt_one, filt_two, w_in, w_out, bias, taps, tables, n_dev, n_groups, units, group=4):
    rows, depth = u.shape
    model = w_in.shape[1] // 3
    width = 2 * LANES
    n_rows = rows // LANES
    n_chunks = n_dev
    n_high = n_dev * n_rows
    chunk_rows = LANES // n_chunks * n_rows
    tile = 2 * chunk_rows
    hbm_spec = pl.BlockSpec(memory_space=pltpu.HBM)
    consts = (bias, taps, *tables)
    dma = pltpu.SemaphoreType.DMA
    return pl.pallas_call(
        functools.partial(hyena_body, n_dev, n_groups, units, group),
        in_specs=[hbm_spec] * (7 + len(consts)),
        out_specs=[hbm_spec] * 6,
        out_shape=[
            jax.ShapeDtypeStruct((n_chunks, n_dev, 2, chunk_rows, LANES), F32),
            jax.ShapeDtypeStruct((n_chunks, n_dev, chunk_rows, LANES), BF16),
            jax.ShapeDtypeStruct((n_chunks, n_dev, 2, chunk_rows, LANES), F32),
            jax.ShapeDtypeStruct((n_chunks, n_dev, chunk_rows, LANES), F32),
            jax.ShapeDtypeStruct((model // LANES, tile, LANES), F32),
            jax.ShapeDtypeStruct((rows, model), BF16),
        ],
        scratch_shapes=[
            pltpu.SMEM(skip_one.shape, F32),
            pltpu.SMEM(skip_two.shape, F32),
            *[pltpu.VMEM(c.shape, c.dtype) for c in consts],
            dma((2 + len(consts),)),
            pltpu.VMEM((rows, depth), BF16),
            pltpu.VMEM((2, depth, width), BF16),
            pltpu.VMEM((rows + 8, width), F32),
            pltpu.VMEM((2, rows, LANES), F32),
            pltpu.VMEM((2, n_chunks, width // LANES, chunk_rows, LANES), F32),
            pltpu.VMEM((n_chunks, width // LANES, chunk_rows, LANES), BF16),
            pltpu.VMEM((8, depth), F32),
            pltpu.VMEM((8, depth), F32),
            pltpu.VMEM((n_chunks, n_dev, 2 * chunk_rows, LANES), F32),
            pltpu.VMEM((n_dev, 2, chunk_rows, LANES), F32),
            pltpu.VMEM((n_chunks, n_dev, chunk_rows, LANES), F32),
            pltpu.VMEM((group * n_high, 6 * LANES), BF16),
            pltpu.VMEM((group * n_high, 2 * LANES), F32),
            pltpu.VMEM((group * n_high, 2 * LANES), F32),
            pltpu.VMEM((2 * chunk_rows, 2 * LANES), BF16),
            pltpu.VMEM((2, n_dev, LANES // n_chunks, model), BF16),
            dma((2,)),
            dma((2,)),
            dma((2,)),
            dma((3,)),
            dma((2,)),
            dma((n_dev,)),
            dma((n_dev,)),
            dma((n_chunks,)),
            dma((n_chunks,)),
            dma((n_chunks, n_dev)),
            dma((n_chunks, n_dev)),
            dma((n_dev,)),
            dma((n_chunks, n_dev)),
            dma((n_chunks, n_dev)),
            dma((2, 3)),
            dma,
            dma((rows // tile,)),
            dma((rows // tile, n_dev)),
            dma((rows // tile, n_dev)),
        ],
        cost_estimate=pl.CostEstimate(flops=10**11, bytes_accessed=100 * 2**20, transcendentals=0),
        compiler_params=pltpu.CompilerParams(collective_id=0, has_side_effects=True, vmem_limit_bytes=54 * 2**20),
        name="hyena",
    )(u, filt_one, filt_two, w_in, w_out, skip_one, skip_two, *consts)


def finish_body(n_rows, most_hbm_ref, sum_hbm_ref, gate_hbm_ref, back_hbm_ref, w_hbm_ref, out_hbm_ref, *refs):
    sum_ref, gate_ref, back_ref, w_ref, out_ref, gated_ref, in_sem, w_sem, most_sem, out_sem = refs
    first = gate_hbm_ref.shape[0] - 2
    rows = out_ref.shape[0]
    first_row = rows - sum_ref.shape[1]
    tile = n_rows * LANES
    n_tiles = sum_ref.shape[1] // tile
    n_most = first_row // sum_ref.shape[1]

    def tile_in(i):
        at = pl.ds(i * tile, tile)
        narrow, wide = pl.ds(i * n_rows, n_rows), pl.ds(first_row // LANES + i * n_rows, n_rows)
        return (
            pltpu.make_async_copy(sum_hbm_ref.at[:, at], sum_ref.at[:, at], in_sem.at[i, 0]),
            pltpu.make_async_copy(gate_hbm_ref.at[pl.ds(first, 2), :, wide], gate_ref.at[:, :, narrow], in_sem.at[i, 1]),
            pltpu.make_async_copy(back_hbm_ref.at[pl.ds(first, 2), :, wide], back_ref.at[:, :, narrow], in_sem.at[i, 2]),
        )

    def most(i, out):
        at = pl.ds(i * sum_ref.shape[1], sum_ref.shape[1])
        if out:
            return pltpu.make_async_copy(out_ref.at[at], out_hbm_ref.at[at], most_sem.at[i])
        return pltpu.make_async_copy(most_hbm_ref.at[at], out_ref.at[at], most_sem.at[i])

    def tile_out(i):
        at = pl.ds(first_row + i * tile, tile)
        return pltpu.make_async_copy(out_ref.at[at], out_hbm_ref.at[at], out_sem.at[i])

    w_in = pltpu.make_async_copy(w_hbm_ref.at[:, pl.ds(first, 2)], w_ref, w_sem)
    w_in.start()
    for i in range(n_tiles):
        for copy in tile_in(i):
            copy.start()
    for i in range(n_most):
        most(i, False).start()
    w_in.wait()
    w_pair = jnp.concatenate([w_ref[:, j].reshape(LANES, w_ref.shape[3]) for j in range(2)], axis=0)
    for i in range(n_tiles):
        for copy in tile_in(i):
            copy.wait()
        for r in range(n_rows):
            for j in range(2):
                gated = back_ref[j, :, i * n_rows + r] * gate_ref[j, :, i * n_rows + r].astype(F32)
                gated_ref[r * LANES : (r + 1) * LANES, j * LANES : (j + 1) * LANES] = gated.reshape(LANES, LANES).T.astype(BF16)
        added = dot32(gated_ref[...], w_pair)
        for e in range(sum_ref.shape[0]):
            cols = slice(e * LANES, (e + 1) * LANES)
            out_ref[first_row + i * tile : first_row + (i + 1) * tile, cols] = (sum_ref[e, i * tile : (i + 1) * tile] + added[:, cols]).astype(BF16)
        tile_out(i).start()
    for i in range(n_most):
        most(i, False).wait()
        most(i, True).start()
    for i in range(n_tiles):
        tile_out(i).wait()
    for i in range(n_most):
        most(i, True).wait()


def finish(most, partial, gate, back, w_out, n_rows=2):
    _, n_src, _, n_chan, _ = back.shape
    rows, model = most.shape
    last_rows = partial.shape[1]
    n_tiles = last_rows // (n_rows * LANES)
    hbm_spec = pl.BlockSpec(memory_space=pltpu.HBM)
    returned = (2, n_src, last_rows // LANES, n_chan, LANES)
    return pl.pallas_call(
        functools.partial(finish_body, n_rows),
        in_specs=[hbm_spec] * 5,
        out_specs=hbm_spec,
        out_shape=jax.ShapeDtypeStruct((rows, model), BF16),
        scratch_shapes=[
            pltpu.VMEM(partial.shape, F32),
            pltpu.VMEM(returned, BF16),
            pltpu.VMEM(returned, F32),
            pltpu.VMEM((n_src, 2, n_chan, model), BF16),
            pltpu.VMEM((rows, model), BF16),
            pltpu.VMEM((n_rows * LANES, 2 * LANES), BF16),
            pltpu.SemaphoreType.DMA((n_tiles, 3)),
            pltpu.SemaphoreType.DMA,
            pltpu.SemaphoreType.DMA((max(1, rows // last_rows - 1),)),
            pltpu.SemaphoreType.DMA((n_tiles,)),
        ],
        cost_estimate=pl.CostEstimate(flops=4 * last_rows * model * LANES, bytes_accessed=11 * 2**20, transcendentals=0),
        compiler_params=pltpu.CompilerParams(vmem_limit_bytes=56 * 2**20),
        name="finish",
    )(most, partial, gate, back, w_out)


def solution(mesh):
    n_dev, n_groups = mesh.shape["sp"], mesh.shape["dp"]
    n_chunks = n_dev
    n_chan = LANES // n_chunks
    if n_groups < 2 or (2 * n_chan) % n_groups:
        raise ValueError("uneven groups")
    units = 2 * n_chan // n_groups

    def local_step(u_in, w_in, b_in, conv_taps, w_out, skip_one, skip_two, filt_one, filt_two):
        u = u_in[0]
        rows = u.shape[0]
        tables = [jnp.asarray(t) for t in transform_tables(rows * n_dev)]
        w_blocks = w_out.reshape(n_dev, n_chunks, n_chan, w_out.shape[1])
        _, gate, _, back, partial, most = hyena(
            skip_one, skip_two, u, filt_one, filt_two, w_in, w_blocks, b_in[None], conv_taps, tables, n_dev, n_groups, units
        )
        by_row = (n_chunks, n_dev, rows // LANES, n_chan, LANES)
        return finish(most, partial, gate.reshape(by_row), back.reshape(by_row), w_blocks)[None]

    seq_spec = P("dp", "sp", None)
    filt_spec = P("sp", None)
    return jax.shard_map(
        local_step,
        mesh=mesh,
        in_specs=(seq_spec, P(), P(), P(), P(), P(), P(), filt_spec, filt_spec),
        out_specs=seq_spec,
        check_vma=False,
    )
```

```python
import functools
import math
import jax
import jax.numpy as jnp
import numpy as np
from jax import lax
from jax.experimental import pallas as pl
from jax.experimental.pallas import tpu as pltpu
from jax.sharding import PartitionSpec as P

LANES = 128
F32 = jnp.float32
BF16 = jnp.bfloat16


def split_table(table, n_parts=3):
    parts, rest = [], np.asarray(table, np.float64)
    for _ in range(n_parts):
        part = rest.astype(jnp.bfloat16)
        parts.append(part)
        rest = rest - part.astype(np.float64)
    return parts


def transform_tables(seq_len):
    n_high = seq_len // LANES
    quarter = np.arange(n_high)[:, None] + 0.25
    high = 2.0 * np.pi * quarter * np.arange(n_high)[None, :] / n_high
    twist = 2.0 * np.pi * quarter * np.arange(LANES)[None, :] / seq_len
    low = 2.0 * np.pi * np.outer(np.arange(LANES), np.arange(LANES)) / LANES
    first = np.concatenate([np.cos(high), -np.sin(high)], axis=0)
    last = np.concatenate([np.cos(high.T), -np.sin(high.T)], axis=1)
    er, ei = np.cos(low), -np.sin(low)
    fwd = np.block([[er, ei], [-ei, er]])
    inv = np.block([[er, -ei], [ei, er]])
    a, b, c = split_table(first)
    first_wide = np.concatenate([a, a, a, b, b, c], axis=1)
    first_thin = np.concatenate([a, b, c], axis=1)
    fwd_parts = np.concatenate(split_table(fwd), axis=0)
    inv_parts = np.concatenate(split_table(inv), axis=0)
    last_parts = np.concatenate(split_table(last), axis=0)
    twist_tab = np.stack([np.cos(twist), -np.sin(twist)]).astype(np.float32)
    return first_wide, first_thin, fwd_parts, inv_parts, last_parts, twist_tab


def split3(x):
    hi = x.astype(BF16)
    rest = x - hi.astype(F32)
    mid = rest.astype(BF16)
    low = (rest - mid.astype(F32)).astype(BF16)
    return hi, mid, low


def dot32(a, b):
    return jnp.dot(a, b, preferred_element_type=F32)


def turn_rows(block, into_ref, n_chunks, row, n_rows):
    turned = block.T
    n_chan = LANES // n_chunks
    for k in range(n_chunks):
        into_ref[k, pl.ds(row, n_chan, stride=n_rows), :] = turned[k * n_chan : (k + 1) * n_chan]


def far_first(n_dev):
    return sorted(range(1, n_dev), key=lambda off: -min(off, n_dev - off))


def send_spans(n_chunks):
    return [(k, 1) for k in range(n_chunks - 2)] + [(n_chunks - 2, 2)]


def row_spans(n_tiles):
    return [(0, n_tiles - 2), (n_tiles - 2, 1), (n_tiles - 1, 1)] if n_tiles > 2 else [(q, 1) for q in range(n_tiles)]


def spectrum_tools(group, n_high, tables, parts_ref):
    wide_ref, thin_ref, fwd_ref, inv_ref, last_ref, twist_ref = tables
    wide = 2 * LANES
    scale = 1.0 / (n_high * LANES)

    def complex_dot(tab_ref):
        return (
            dot32(parts_ref[:, 2 * wide :], tab_ref[:wide])
            + dot32(parts_ref[:, wide : 2 * wide], tab_ref[:wide])
            + dot32(parts_ref[:, :wide], tab_ref[wide : 2 * wide])
            + dot32(parts_ref[:, wide : 2 * wide], tab_ref[wide : 2 * wide])
            + dot32(parts_ref[:, :wide], tab_ref[2 * wide :])
            + dot32(parts_ref[:, :wide], tab_ref[:wide])
        )

    def store_parts(g, real, imag):
        for t, (re, im) in enumerate(zip(split3(real), split3(imag))):
            parts_ref[g * n_high : (g + 1) * n_high, 2 * t * LANES : (2 * t + 1) * LANES] = re
            parts_ref[g * n_high : (g + 1) * n_high, (2 * t + 1) * LANES : (2 * t + 2) * LANES] = im

    def spectrum(signals, exact):
        tr, ti = twist_ref[0], twist_ref[1]
        for g in range(0, group, 2):
            pair = jnp.concatenate([signals[g], signals[g + 1]], axis=1)
            if exact:
                short = pair.astype(BF16)
                coarse = dot32(thin_ref[...], jnp.concatenate([short, short, short], axis=0))
            else:
                hi, mid, low = split3(pair)
                coarse = dot32(wide_ref[...], jnp.concatenate([hi, mid, low, hi, mid, hi], axis=0))
            for j in range(2):
                re = coarse[:n_high, j * LANES : (j + 1) * LANES]
                im = coarse[n_high:, j * LANES : (j + 1) * LANES]
                store_parts(g + j, re * tr - im * ti, re * ti + im * tr)
        return complex_dot(fwd_ref)

    def signal(spec_a, spec_b):
        tr, ti = twist_ref[0], twist_ref[1]
        for g in range(group):
            rows = slice(g * n_high, (g + 1) * n_high)
            ar, ai = spec_a[rows, :LANES], spec_a[rows, LANES:]
            br, bi = spec_b[rows, :LANES], spec_b[rows, LANES:]
            store_parts(g, ar * br - ai * bi, ar * bi + ai * br)
        fine = complex_dot(inv_ref)
        results = []
        for g in range(0, group, 2):
            halves = []
            for j in range(2):
                rows = slice((g + j) * n_high, (g + j + 1) * n_high)
                re, im = fine[rows, :LANES] * scale, fine[rows, LANES:] * scale
                halves.append(jnp.concatenate([re * tr + im * ti, im * tr - re * ti], axis=0))
            hi, mid, low = split3(jnp.concatenate(halves, axis=1))
            d_hi = dot32(last_ref[...], hi)
            d_mid = dot32(last_ref[: 2 * n_high], mid)
            d_low = dot32(last_ref[:n_high], low)
            small = d_hi[2 * n_high :] + d_mid[n_high:] + d_low
            total = d_hi[:n_high] + ((d_hi[n_high : 2 * n_high] + d_mid[:n_high]) + small)
            results += [total[:, :LANES], total[:, LANES:]]
        return results

    return spectrum, signal


def hyena_body(n_dev, n_groups, units, group, u_hbm_ref, one_ref, two_ref, w_hbm_ref, w_out_ref, *refs):
    consts_in, refs = refs[:10], refs[10:]
    consts, const_sem, refs = refs[6:16], refs[16], refs[:6] + refs[17:]
    skip_one_ref, skip_two_ref, bias_ref, taps_ref, *tables = consts
    sent_ref, gate_ref, got_ref, back_ref, sum_ref, most_ref = refs[:6]
    u_ref, w_ref, p_ref, stage_ref, turned_ref, mixed_ref, halo_ref, tail_ref = refs[6:14]
    filt_ref, block_ref, done_ref, parts_ref, spec_one_ref, spec_two_ref, gated_ref, w_pair_ref = refs[14:22]
    (u_sem, w_sem, stage_sem, out_sem, halo_sem, hold_sem, share_sem, group_sem, filt_sem, sent_sem, got_sem, block_sem, done_sem, back_sem, pair_sem, sum_sem, most_sem, piece_sem, piece_got_sem) = refs[22:]
    me, my_group = lax.axis_index("sp"), lax.axis_index("dp")
    rows, depth = u_ref.shape
    n_rows = rows // LANES
    n_chunks = n_dev
    n_chan = LANES // n_chunks
    n_high = n_dev * n_rows
    model = w_hbm_ref.shape[1] // 3
    width = w_ref.shape[2]
    steps = model // width
    share_rows = units * n_rows
    first_unit = my_group * units
    which_mine = first_unit // n_chan
    mesh_id = pl.DeviceIdType.MESH

    def target(off):
        return lax.rem(me + off, n_dev)

    def own_rows(first):
        return pl.ds(pl.multiple_of(first * share_rows, share_rows), share_rows)


    def loading(item, off, which):
        cols = pl.ds(pl.multiple_of(target(off) * LANES, LANES), LANES)
        return pltpu.make_async_copy((one_ref, two_ref)[which].at[:, cols], stage_ref.at[item % 2], stage_sem.at[item % 2])

    def weights(which, step):
        cols = pl.ds(pl.multiple_of(which * model + step * width, width), width)
        slot = lax.rem(which + step, 2)
        return pltpu.make_async_copy(w_hbm_ref.at[:, cols], w_ref.at[slot], w_sem.at[slot])

    def u_part(start, size, idx):
        return pltpu.make_async_copy(u_hbm_ref.at[pl.ds(start, size), :], u_ref.at[pl.ds(start, size), :], u_sem.at[idx])

    def halo_send():
        return pltpu.make_async_remote_copy(tail_ref, halo_ref, halo_sem.at[0], halo_sem.at[1], device_id={"sp": target(1)}, device_id_type=mesh_id)

    def hold_of(dest):
        return done_ref.at[dest, :, pl.ds(0, share_rows), :]

    def share_send(off):
        dest = target(off)
        return pltpu.make_async_remote_copy(
            hold_of(dest), filt_ref.at[:, me, own_rows(my_group), :], hold_sem.at[off], share_sem.at[off], device_id={"sp": dest}, device_id_type=mesh_id
        )

    def group_send(k, off):
        mine = filt_ref.at[k, :, own_rows(my_group), :]
        return pltpu.make_async_remote_copy(
            mine, mine, group_sem.at[k], filt_sem.at[k], device_id={"dp": lax.rem(my_group + off, n_groups)}, device_id_type=mesh_id
        )

    def other_groups(k):
        same_size = filt_ref.at[k, :, pl.ds(0, (n_groups - 1) * share_rows), :]
        return pltpu.make_async_copy(same_size, same_size, filt_sem.at[k])

    def turned_out(slot, step):
        return pltpu.make_async_copy(turned_ref.at[slot], sent_ref.at[:, pl.ds(step * (width // LANES), width // LANES), slot], out_sem.at[slot])

    def mixed_out(step):
        return pltpu.make_async_copy(mixed_ref, gate_ref.at[:, pl.ds(step * (width // LANES), width // LANES)], out_sem.at[2])

    def sending(k, off, span):
        dest, chunks = target(off), pl.ds(k, span)
        return pltpu.make_async_remote_copy(
            sent_ref.at[chunks, dest], got_ref.at[chunks, me], sent_sem.at[k, off], got_sem.at[k, off], device_id={"sp": dest}, device_id_type=mesh_id
        )

    def block_in(k, off):
        src = lax.rem(me - off + n_dev, n_dev)
        from_ref, slot = (got_ref if off else sent_ref), lax.rem(k, 2)
        return pltpu.make_async_copy(from_ref.at[k, src], block_ref.at[slot, src], block_sem.at[slot, off])

    def returning(k, off):
        dest = target(off)
        return pltpu.make_async_remote_copy(
            done_ref.at[pl.ds(k, 2), dest],
            back_ref.at[pl.ds(k, 2), me],
            done_sem.at[k, off],
            back_sem.at[k, off],
            device_id={"sp": dest},
            device_id_type=mesh_id,
        )

    def storing(k):
        return pltpu.make_async_copy(done_ref.at[pl.ds(k, 2), me], back_ref.at[pl.ds(k, 2), me], done_sem.at[k, 0])

    last_pair = n_chunks - 2
    tile = filt_ref.shape[2]
    n_tiles = rows // tile
    piece = tile // LANES * n_chan

    def piece_of(part):
        return pl.ds(part[0] * piece, part[1] * piece)

    def returning_rows(part, off):
        dest = target(off)
        return pltpu.make_async_remote_copy(
            done_ref.at[pl.ds(last_pair, 2), dest, piece_of(part)],
            back_ref.at[pl.ds(last_pair, 2), me, piece_of(part)],
            piece_sem.at[part[0], off],
            piece_got_sem.at[part[0], off],
            device_id={"sp": dest},
            device_id_type=mesh_id,
        )

    def storing_rows(part):
        last = pl.ds(last_pair, 2)
        return pltpu.make_async_copy(done_ref.at[last, me, piece_of(part)], back_ref.at[last, me, piece_of(part)], piece_sem.at[part[0], 0])

    def constant(idx):
        return pltpu.make_async_copy(consts_in[idx], consts[idx], const_sem.at[idx])


    barrier = pltpu.get_barrier_semaphore()
    for off in range(1, n_dev):
        pl.semaphore_signal(barrier, inc=1, device_id={"sp": target(off)}, device_id_type=mesh_id)
    for off in range(1, n_groups):
        pl.semaphore_signal(barrier, inc=1, device_id={"dp": lax.rem(my_group + off, n_groups)}, device_id_type=mesh_id)

    order = far_first(n_dev) + [0]

    def load(item):
        for which in range(2):

            @pl.when(which_mine == which)
            def _():
                loading(item, order[item], which).start()

    load(0)
    u_part(rows - 16, 16, 1).start()
    for item, off in enumerate(order):
        if item + 1 < len(order):
            load(item + 1)
        if item == 0:
            u_part(0, rows - 16, 0).start()
            weights(0, 0).start()
            for idx in range(len(consts)):
                constant(idx).start()
        loading(item, off, 0).wait()
        if units < n_chan:
            into = turned_ref.at[0, :, 0]
        elif off:
            into = done_ref.at[target(off)]
        else:
            into = filt_ref.at[:, me, own_rows(my_group), :]
        together = math.gcd(n_rows, 4)

        @pl.loop(0, n_rows // together)
        def _(i):
            for j in range(together):
                r = i * together + j
                turn_rows(stage_ref[item % 2, pl.ds(pl.multiple_of(r * LANES, LANES), LANES), :], into, n_chunks, r, n_rows)

        if units < n_chan:
            start = pl.multiple_of(lax.rem(first_unit, n_chan) * n_rows, n_rows)
            share = turned_ref[0, :, 0, pl.ds(start, share_rows), :]
            if off:
                done_ref[target(off), :, pl.ds(0, share_rows), :] = share
            else:
                filt_ref[:, me, own_rows(my_group), :] = share
        if item == 0:
            u_part(rows - 16, 16, 1).wait()
            tail_ref[...] = u_ref[pl.ds(rows - 16, 16), :].astype(F32)[8:]
            pl.semaphore_wait(barrier, n_dev + n_groups - 2)
            halo_send().start()
        if off:
            share_send(off).start()


    for idx in range(len(consts)):
        constant(idx).wait()
    u_part(0, rows - 16, 0).wait()
    halo_send().wait()

    @pl.loop(0, steps)
    def _(step):
        for which in range(3):
            if which < 2:
                weights(which + 1, step).start()
            else:

                @pl.when(step + 1 < steps)
                def _():
                    weights(0, step + 1).start()

            weights(which, step).wait()
            w_now = w_ref.at[lax.rem(which + step, 2)]
            cols = pl.ds(pl.multiple_of(which * model + step * width, width), width)
            bias = bias_ref[:, cols]
            halo = (dot32(halo_ref[...].astype(BF16), w_now[...]) + bias).astype(BF16).astype(F32)
            p_ref[0:8, :] = jnp.where(me > 0, halo, 0.0)
            tile = 2 * LANES

            @pl.loop(0, rows // tile)
            def _(i):
                start = pl.multiple_of(i * tile, tile)
                proj = dot32(u_ref[pl.ds(start, tile), :], w_now[...]) + bias
                p_ref[pl.ds(start + 8, tile), :] = proj.astype(BF16).astype(F32)

            c0, c1, c2 = (taps_ref[t : t + 1, cols] for t in range(3))
            slot = 1 if which == 0 else 0

            @pl.when(step > 0)
            def _():
                if which == 1:
                    mixed_out(step - 1).wait()
                else:
                    turned_out(slot, step - 1).wait()

            @pl.loop(0, n_rows)
            def _(r):
                start = pl.multiple_of(r * LANES, LANES)
                window = p_ref[pl.ds(start, LANES + 8), :]
                mixed = c0 * window[8:] + c1 * window[7:-1] + c2 * window[6:-2]
                mixed = mixed.astype(BF16)
                for d in range(width // LANES):
                    block = mixed[:, d * LANES : (d + 1) * LANES].astype(F32)
                    if which != 1:
                        turn_rows(block, turned_ref.at[slot, :, d], n_chunks, r, n_rows)
                        continue
                    turned = block.T.astype(BF16)
                    for k in range(n_chunks):
                        at = pl.ds(pl.multiple_of(r * n_chan, n_chan), n_chan)
                        mixed_ref[k, d, at, :] = turned[k * n_chan : (k + 1) * n_chan]

            if which == 1:
                mixed_out(step).start()
            else:
                turned_out(slot, step).start()

    turned_out(0, steps - 1).wait()
    turned_out(1, steps - 1).wait()
    mixed_out(steps - 1).wait()

    spans = send_spans(n_chunks)
    for k, span in spans:
        for off in far_first(n_dev):
            sending(k, off, span).start()


    for off in range(1, n_dev):
        share_send(off).wait()

    @pl.loop(0, n_chunks)
    def _(k):
        for off in range(1, n_groups):
            group_send(k, off).start()


    spectrum, signal = spectrum_tools(group, n_high, tables, parts_ref)

    def fetch(k):
        block_in(k, 0).start()
        for first, span in spans:

            @pl.when(k == first)
            def _():
                for off in range(1, n_dev):
                    sending(first, off, span).wait_recv()

        for off in range(1, n_dev):
            block_in(k, off).start()

    fetch(jnp.int32(0))

    @pl.loop(0, n_chunks)
    def _(k):
        slot = lax.rem(k, 2)
        other_groups(k).wait()
        for off in range(n_dev):
            block_in(k, off).wait()

        @pl.loop(0, n_chan // group)
        def _(i):
            first = i * group

            @pl.when(jnp.logical_and(i == n_chan // group - 1, k + 1 < n_chunks))
            def _():
                fetch(k + 1)

            def load_h(which, g):
                start = pl.multiple_of((which * n_chan + first + g) * n_rows, n_rows)
                return filt_ref[k, :, pl.ds(start, n_rows), :].reshape(n_high, LANES)

            def load_x(which, g):
                start = pl.multiple_of((first + g) * n_rows, n_rows)
                return block_ref[slot, :, which, pl.ds(start, n_rows), :].reshape(n_high, LANES)

            chan = me * LANES + k * n_chan + first
            spec_one_ref[...] = spectrum([load_h(0, g) for g in range(group)], False)
            spec_two_ref[...] = spectrum([load_h(1, g) for g in range(group)], False)
            values = [load_x(0, g) for g in range(group)]
            conv = signal(spectrum(values, True), spec_one_ref)
            gated = [load_x(1, g) * (conv[g] + skip_one_ref[chan + g] * values[g]) for g in range(group)]
            conv = signal(spectrum(gated, False), spec_two_ref)
            for g in range(group):
                result = conv[g] + skip_two_ref[chan + g] * gated[g]
                done_ref[k, :, pl.ds(first + g, n_rows, stride=n_chan), :] = result.reshape(n_dev, n_rows, LANES)

        @pl.when(jnp.logical_and(k < last_pair, lax.rem(k, 2) == 1))
        def _():
            storing(k - 1).start()
            for off in far_first(n_dev):
                returning(k - 1, off).start()


    parts = row_spans(n_tiles)
    for part in parts:
        storing_rows(part).start()
        for off in far_first(n_dev):
            returning_rows(part, off).start()

    for k, span in spans:
        for off in range(1, n_dev):
            sending(k, off, span).wait_send()

    @pl.loop(0, n_chunks)
    def _(k):
        for off in range(1, n_groups):
            group_send(k, off).wait_send()


    @pl.loop(0, n_tiles)
    def _(q):
        for e in range(model // LANES):
            part = u_ref[pl.ds(pl.multiple_of(q * tile, tile), tile), e * LANES : (e + 1) * LANES]
            filt_ref[e, q] = part.astype(F32)

    def pair_in(k, j):
        return (
            pltpu.make_async_copy(back_ref.at[k], block_ref.at[0, :, j], pair_sem.at[j, 0]),
            pltpu.make_async_copy(gate_ref.at[k], mixed_ref.at[:, j], pair_sem.at[j, 1]),
            w_pair_in(k, j),
        )

    def w_pair_in(k, j):
        return pltpu.make_async_copy(w_out_ref.at[:, k], w_pair_ref.at[j], pair_sem.at[j, 2])

    def product(q):
        for t in range(tile // LANES):
            for j in range(2):
                at = pl.ds(pl.multiple_of((q * (tile // LANES) + t) * n_chan, n_chan), n_chan)
                gated = block_ref[0, :, j, at, :] * mixed_ref[:, j, at, :].astype(F32)
                gated_ref[t * LANES : (t + 1) * LANES, j * LANES : (j + 1) * LANES] = gated.reshape(LANES, LANES).T.astype(BF16)
        return dot32(gated_ref[...], w_pair_ref[...].reshape(2 * LANES, model))

    @pl.loop(0, n_chunks // 2 - 1)
    def _(p):
        storing(2 * p).wait()
        for off in range(1, n_dev):
            returning(2 * p, off).wait()
        for j in range(2):
            for copy in pair_in(2 * p + j, j):
                copy.start()
        for j in range(2):
            for copy in pair_in(2 * p + j, j):
                copy.wait()

        @pl.loop(0, n_tiles)
        def _(q):
            added = product(q)
            for e in range(model // LANES):
                filt_ref[e, q] = filt_ref[e, q] + added[:, e * LANES : (e + 1) * LANES]

    sum_out = pltpu.make_async_copy(filt_ref.at[:, n_tiles - 1], sum_ref, sum_sem)
    sum_out.start()

    def rows_of(q):
        return pl.ds(pl.multiple_of(q * tile, tile), tile)

    def most_out(q):
        return pltpu.make_async_copy(u_ref.at[rows_of(q)], most_ref.at[rows_of(q)], most_sem.at[q])

    def rows_in(part, j):
        k, at = last_pair + j, piece_of(part)
        return (
            pltpu.make_async_copy(back_ref.at[k, :, at], block_ref.at[0, :, j, at], pair_sem.at[j, 0]),
            pltpu.make_async_copy(gate_ref.at[k, :, at], mixed_ref.at[:, j, at], pair_sem.at[j, 1]),
        )

    if n_tiles > 1:
        for j in range(2):
            w_pair_in(last_pair + j, j).start()
        for j in range(2):
            w_pair_in(last_pair + j, j).wait()

    for part in parts[:-1]:
        storing_rows(part).wait()
        for off in range(1, n_dev):
            returning_rows(part, off).wait()
        for j in range(2):
            for copy in rows_in(part, j):
                copy.start()
        for j in range(2):
            for copy in rows_in(part, j):
                copy.wait()

        @pl.loop(part[0], part[0] + part[1])
        def _(q):
            added = product(q)
            for e in range(model // LANES):
                cols = slice(e * LANES, (e + 1) * LANES)
                u_ref[rows_of(q), cols] = (filt_ref[e, q] + added[:, cols]).astype(BF16)
            most_out(q).start()

    storing_rows(parts[-1]).wait()
    for off in range(1, n_dev):
        returning_rows(parts[-1], off).wait()
    sum_out.wait()

    @pl.loop(0, n_tiles - 1)
    def _(q):
        most_out(q).wait()


def hyena(skip_one, skip_two, u, filt_one, filt_two, w_in, w_out, bias, taps, tables, n_dev, n_groups, units, group=4):
    rows, depth = u.shape
    model = w_in.shape[1] // 3
    width = 2 * LANES
    n_rows = rows // LANES
    n_chunks = n_dev
    n_high = n_dev * n_rows
    chunk_rows = LANES // n_chunks * n_rows
    tile = 2 * chunk_rows
    hbm_spec = pl.BlockSpec(memory_space=pltpu.HBM)
    consts = (bias, taps, *tables)
    dma = pltpu.SemaphoreType.DMA
    return pl.pallas_call(
        functools.partial(hyena_body, n_dev, n_groups, units, group),
        in_specs=[hbm_spec] * (7 + len(consts)),
        out_specs=[hbm_spec] * 6,
        out_shape=[
            jax.ShapeDtypeStruct((n_chunks, n_dev, 2, chunk_rows, LANES), F32),
            jax.ShapeDtypeStruct((n_chunks, n_dev, chunk_rows, LANES), BF16),
            jax.ShapeDtypeStruct((n_chunks, n_dev, 2, chunk_rows, LANES), F32),
            jax.ShapeDtypeStruct((n_chunks, n_dev, chunk_rows, LANES), F32),
            jax.ShapeDtypeStruct((model // LANES, tile, LANES), F32),
            jax.ShapeDtypeStruct((rows, model), BF16),
        ],
        scratch_shapes=[
            pltpu.SMEM(skip_one.shape, F32),
            pltpu.SMEM(skip_two.shape, F32),
            *[pltpu.VMEM(c.shape, c.dtype) for c in consts],
            dma((2 + len(consts),)),
            pltpu.VMEM((rows, depth), BF16),
            pltpu.VMEM((2, depth, width), BF16),
            pltpu.VMEM((rows + 8, width), F32),
            pltpu.VMEM((2, rows, LANES), F32),
            pltpu.VMEM((2, n_chunks, width // LANES, chunk_rows, LANES), F32),
            pltpu.VMEM((n_chunks, width // LANES, chunk_rows, LANES), BF16),
            pltpu.VMEM((8, depth), F32),
            pltpu.VMEM((8, depth), F32),
            pltpu.VMEM((n_chunks, n_dev, 2 * chunk_rows, LANES), F32),
            pltpu.VMEM((2, n_dev, 2, chunk_rows, LANES), F32),
            pltpu.VMEM((n_chunks, n_dev, chunk_rows, LANES), F32),
            pltpu.VMEM((group * n_high, 6 * LANES), BF16),
            pltpu.VMEM((group * n_high, 2 * LANES), F32),
            pltpu.VMEM((group * n_high, 2 * LANES), F32),
            pltpu.VMEM((2 * chunk_rows, 2 * LANES), BF16),
            pltpu.VMEM((2, n_dev, LANES // n_chunks, model), BF16),
            dma((2,)),
            dma((2,)),
            dma((2,)),
            dma((3,)),
            dma((2,)),
            dma((n_dev,)),
            dma((n_dev,)),
            dma((n_chunks,)),
            dma((n_chunks,)),
            dma((n_chunks, n_dev)),
            dma((n_chunks, n_dev)),
            dma((2, n_dev)),
            dma((n_chunks, n_dev)),
            dma((n_chunks, n_dev)),
            dma((2, 3)),
            dma,
            dma((rows // tile,)),
            dma((rows // tile, n_dev)),
            dma((rows // tile, n_dev)),
        ],
        cost_estimate=pl.CostEstimate(flops=10**11, bytes_accessed=100 * 2**20, transcendentals=0),
        compiler_params=pltpu.CompilerParams(collective_id=0, has_side_effects=True, vmem_limit_bytes=54 * 2**20),
        name="hyena",
    )(u, filt_one, filt_two, w_in, w_out, skip_one, skip_two, *consts)


def finish_body(n_rows, most_hbm_ref, sum_hbm_ref, gate_hbm_ref, back_hbm_ref, w_hbm_ref, out_hbm_ref, *refs):
    sum_ref, gate_ref, back_ref, w_ref, out_ref, gated_ref, in_sem, w_sem, most_sem, out_sem = refs
    first = gate_hbm_ref.shape[0] - 2
    rows = out_ref.shape[0]
    first_row = rows - sum_ref.shape[1]
    tile = n_rows * LANES
    n_tiles = sum_ref.shape[1] // tile
    n_most = first_row // sum_ref.shape[1]

    def tile_in(i):
        at = pl.ds(i * tile, tile)
        narrow, wide = pl.ds(i * n_rows, n_rows), pl.ds(first_row // LANES + i * n_rows, n_rows)
        return (
            pltpu.make_async_copy(sum_hbm_ref.at[:, at], sum_ref.at[:, at], in_sem.at[i, 0]),
            pltpu.make_async_copy(gate_hbm_ref.at[pl.ds(first, 2), :, wide], gate_ref.at[:, :, narrow], in_sem.at[i, 1]),
            pltpu.make_async_copy(back_hbm_ref.at[pl.ds(first, 2), :, wide], back_ref.at[:, :, narrow], in_sem.at[i, 2]),
        )

    def most(i, out):
        at = pl.ds(i * sum_ref.shape[1], sum_ref.shape[1])
        if out:
            return pltpu.make_async_copy(out_ref.at[at], out_hbm_ref.at[at], most_sem.at[i])
        return pltpu.make_async_copy(most_hbm_ref.at[at], out_ref.at[at], most_sem.at[i])

    def tile_out(i):
        at = pl.ds(first_row + i * tile, tile)
        return pltpu.make_async_copy(out_ref.at[at], out_hbm_ref.at[at], out_sem.at[i])

    w_in = pltpu.make_async_copy(w_hbm_ref.at[:, pl.ds(first, 2)], w_ref, w_sem)
    w_in.start()
    for i in range(n_tiles):
        for copy in tile_in(i):
            copy.start()
    for i in range(n_most):
        most(i, False).start()
    w_in.wait()
    w_pair = jnp.concatenate([w_ref[:, j].reshape(LANES, w_ref.shape[3]) for j in range(2)], axis=0)
    for i in range(n_tiles):
        for copy in tile_in(i):
            copy.wait()
        for r in range(n_rows):
            for j in range(2):
                gated = back_ref[j, :, i * n_rows + r] * gate_ref[j, :, i * n_rows + r].astype(F32)
                gated_ref[r * LANES : (r + 1) * LANES, j * LANES : (j + 1) * LANES] = gated.reshape(LANES, LANES).T.astype(BF16)
        added = dot32(gated_ref[...], w_pair)
        for e in range(sum_ref.shape[0]):
            cols = slice(e * LANES, (e + 1) * LANES)
            out_ref[first_row + i * tile : first_row + (i + 1) * tile, cols] = (sum_ref[e, i * tile : (i + 1) * tile] + added[:, cols]).astype(BF16)
        tile_out(i).start()
    for i in range(n_most):
        most(i, False).wait()
        most(i, True).start()
    for i in range(n_tiles):
        tile_out(i).wait()
    for i in range(n_most):
        most(i, True).wait()


def finish(most, partial, gate, back, w_out, n_rows=2):
    _, n_src, _, n_chan, _ = back.shape
    rows, model = most.shape
    last_rows = partial.shape[1]
    n_tiles = last_rows // (n_rows * LANES)
    hbm_spec = pl.BlockSpec(memory_space=pltpu.HBM)
    returned = (2, n_src, last_rows // LANES, n_chan, LANES)
    return pl.pallas_call(
        functools.partial(finish_body, n_rows),
        in_specs=[hbm_spec] * 5,
        out_specs=hbm_spec,
        out_shape=jax.ShapeDtypeStruct((rows, model), BF16),
        scratch_shapes=[
            pltpu.VMEM(partial.shape, F32),
            pltpu.VMEM(returned, BF16),
            pltpu.VMEM(returned, F32),
            pltpu.VMEM((n_src, 2, n_chan, model), BF16),
            pltpu.VMEM((rows, model), BF16),
            pltpu.VMEM((n_rows * LANES, 2 * LANES), BF16),
            pltpu.SemaphoreType.DMA((n_tiles, 3)),
            pltpu.SemaphoreType.DMA,
            pltpu.SemaphoreType.DMA((max(1, rows // last_rows - 1),)),
            pltpu.SemaphoreType.DMA((n_tiles,)),
        ],
        cost_estimate=pl.CostEstimate(flops=4 * last_rows * model * LANES, bytes_accessed=11 * 2**20, transcendentals=0),
        compiler_params=pltpu.CompilerParams(vmem_limit_bytes=56 * 2**20),
        name="finish",
    )(most, partial, gate, back, w_out)


def solution(mesh):
    n_dev, n_groups = mesh.shape["sp"], mesh.shape["dp"]
    n_chunks = n_dev
    n_chan = LANES // n_chunks
    if n_groups < 2 or (2 * n_chan) % n_groups:
        raise ValueError("uneven groups")
    units = 2 * n_chan // n_groups

    def local_step(u_in, w_in, b_in, conv_taps, w_out, skip_one, skip_two, filt_one, filt_two):
        u = u_in[0]
        rows = u.shape[0]
        tables = [jnp.asarray(t) for t in transform_tables(rows * n_dev)]
        w_blocks = w_out.reshape(n_dev, n_chunks, n_chan, w_out.shape[1])
        _, gate, _, back, partial, most = hyena(
            skip_one, skip_two, u, filt_one, filt_two, w_in, w_blocks, b_in[None], conv_taps, tables, n_dev, n_groups, units
        )
        by_row = (n_chunks, n_dev, rows // LANES, n_chan, LANES)
        return finish(most, partial, gate.reshape(by_row), back.reshape(by_row), w_blocks)[None]

    seq_spec = P("dp", "sp", None)
    filt_spec = P("sp", None)
    return jax.shard_map(
        local_step,
        mesh=mesh,
        in_specs=(seq_spec, P(), P(), P(), P(), P(), P(), filt_spec, filt_spec),
        out_specs=seq_spec,
        check_vma=False,
    )
```

```python
import functools
import math
import jax
import jax.numpy as jnp
import numpy as np
from jax import lax
from jax.experimental import pallas as pl
from jax.experimental.pallas import tpu as pltpu
from jax.sharding import PartitionSpec as P

LANES = 128
F32 = jnp.float32
BF16 = jnp.bfloat16


def split_table(table, n_parts=3):
    parts, rest = [], np.asarray(table, np.float64)
    for _ in range(n_parts):
        part = rest.astype(jnp.bfloat16)
        parts.append(part)
        rest = rest - part.astype(np.float64)
    return parts


def transform_tables(seq_len):
    n_high = seq_len // LANES
    quarter = np.arange(n_high)[:, None] + 0.25
    high = 2.0 * np.pi * quarter * np.arange(n_high)[None, :] / n_high
    twist = 2.0 * np.pi * quarter * np.arange(LANES)[None, :] / seq_len
    low = 2.0 * np.pi * np.outer(np.arange(LANES), np.arange(LANES)) / LANES
    first = np.concatenate([np.cos(high), -np.sin(high)], axis=0)
    last = np.concatenate([np.cos(high.T), -np.sin(high.T)], axis=1)
    er, ei = np.cos(low), -np.sin(low)
    fwd = np.block([[er, ei], [-ei, er]])
    inv = np.block([[er, -ei], [ei, er]])
    a, b, c = split_table(first)
    first_wide = np.concatenate([a, a, a, b, b, c], axis=1)
    first_thin = np.concatenate([a, b, c], axis=1)
    fwd_parts = np.concatenate(split_table(fwd), axis=0)
    inv_parts = np.concatenate(split_table(inv), axis=0)
    last_parts = np.concatenate(split_table(last), axis=0)
    twist_tab = np.stack([np.cos(twist), -np.sin(twist)]).astype(np.float32)
    return first_wide, first_thin, fwd_parts, inv_parts, last_parts, twist_tab


def split3(x):
    hi = x.astype(BF16)
    rest = x - hi.astype(F32)
    mid = rest.astype(BF16)
    low = (rest - mid.astype(F32)).astype(BF16)
    return hi, mid, low


def dot32(a, b):
    return jnp.dot(a, b, preferred_element_type=F32)


def turn_rows(block, into_ref, n_chunks, row, n_rows):
    turned = block.T
    n_chan = LANES // n_chunks
    for k in range(n_chunks):
        into_ref[k, pl.ds(row, n_chan, stride=n_rows), :] = turned[k * n_chan : (k + 1) * n_chan]


def far_first(n_dev):
    return sorted(range(1, n_dev), key=lambda off: -min(off, n_dev - off))


def send_spans(n_chunks):
    return [(k, 1) for k in range(n_chunks - 2)] + [(n_chunks - 2, 2)]


def row_spans(n_tiles):
    return [(0, n_tiles - 2), (n_tiles - 2, 1), (n_tiles - 1, 1)] if n_tiles > 2 else [(q, 1) for q in range(n_tiles)]


def spectrum_tools(group, n_high, tables, parts_ref):
    wide_ref, thin_ref, fwd_ref, inv_ref, last_ref, twist_ref = tables
    wide = 2 * LANES
    scale = 1.0 / (n_high * LANES)

    def complex_dot(tab_ref):
        return (
            dot32(parts_ref[:, 2 * wide :], tab_ref[:wide])
            + dot32(parts_ref[:, wide : 2 * wide], tab_ref[:wide])
            + dot32(parts_ref[:, :wide], tab_ref[wide : 2 * wide])
            + dot32(parts_ref[:, wide : 2 * wide], tab_ref[wide : 2 * wide])
            + dot32(parts_ref[:, :wide], tab_ref[2 * wide :])
            + dot32(parts_ref[:, :wide], tab_ref[:wide])
        )

    def store_parts(g, real, imag):
        for t, (re, im) in enumerate(zip(split3(real), split3(imag))):
            parts_ref[g * n_high : (g + 1) * n_high, 2 * t * LANES : (2 * t + 1) * LANES] = re
            parts_ref[g * n_high : (g + 1) * n_high, (2 * t + 1) * LANES : (2 * t + 2) * LANES] = im

    def spectrum(signals, exact):
        tr, ti = twist_ref[0], twist_ref[1]
        for g in range(0, group, 2):
            pair = jnp.concatenate([signals[g], signals[g + 1]], axis=1)
            if exact:
                short = pair.astype(BF16)
                coarse = dot32(thin_ref[...], jnp.concatenate([short, short, short], axis=0))
            else:
                hi, mid, low = split3(pair)
                coarse = dot32(wide_ref[...], jnp.concatenate([hi, mid, low, hi, mid, hi], axis=0))
            for j in range(2):
                re = coarse[:n_high, j * LANES : (j + 1) * LANES]
                im = coarse[n_high:, j * LANES : (j + 1) * LANES]
                store_parts(g + j, re * tr - im * ti, re * ti + im * tr)
        return complex_dot(fwd_ref)

    def signal(spec_a, spec_b):
        tr, ti = twist_ref[0], twist_ref[1]
        for g in range(group):
            rows = slice(g * n_high, (g + 1) * n_high)
            ar, ai = spec_a[rows, :LANES], spec_a[rows, LANES:]
            br, bi = spec_b[rows, :LANES], spec_b[rows, LANES:]
            store_parts(g, ar * br - ai * bi, ar * bi + ai * br)
        fine = complex_dot(inv_ref)
        results = []
        for g in range(0, group, 2):
            halves = []
            for j in range(2):
                rows = slice((g + j) * n_high, (g + j + 1) * n_high)
                re, im = fine[rows, :LANES] * scale, fine[rows, LANES:] * scale
                halves.append(jnp.concatenate([re * tr + im * ti, im * tr - re * ti], axis=0))
            hi, mid, low = split3(jnp.concatenate(halves, axis=1))
            d_hi = dot32(last_ref[...], hi)
            d_mid = dot32(last_ref[: 2 * n_high], mid)
            d_low = dot32(last_ref[:n_high], low)
            small = d_hi[2 * n_high :] + d_mid[n_high:] + d_low
            total = d_hi[:n_high] + ((d_hi[n_high : 2 * n_high] + d_mid[:n_high]) + small)
            results += [total[:, :LANES], total[:, LANES:]]
        return results

    return spectrum, signal


def hyena_body(n_dev, n_groups, units, group, u_hbm_ref, one_ref, two_ref, w_hbm_ref, w_out_ref, *refs):
    consts_in, refs = refs[:10], refs[10:]
    consts, const_sem, refs = refs[6:16], refs[16], refs[:6] + refs[17:]
    skip_one_ref, skip_two_ref, bias_ref, taps_ref, *tables = consts
    sent_ref, gate_ref, got_ref, back_ref, sum_ref, most_ref = refs[:6]
    u_ref, w_ref, p_ref, stage_ref, turned_ref, mixed_ref, halo_ref, tail_ref = refs[6:14]
    filt_ref, block_ref, done_ref, parts_ref, spec_one_ref, spec_two_ref, gated_ref, w_pair_ref = refs[14:22]
    (u_sem, w_sem, stage_sem, out_sem, halo_sem, hold_sem, share_sem, group_sem, filt_sem, sent_sem, got_sem, block_sem, done_sem, back_sem, pair_sem, sum_sem, most_sem, piece_sem, piece_got_sem) = refs[22:]
    me, my_group = lax.axis_index("sp"), lax.axis_index("dp")
    rows, depth = u_ref.shape
    n_rows = rows // LANES
    n_chunks = n_dev
    n_chan = LANES // n_chunks
    n_high = n_dev * n_rows
    model = w_hbm_ref.shape[1] // 3
    width = w_ref.shape[2]
    steps = model // width
    share_rows = units * n_rows
    first_unit = my_group * units
    which_mine = first_unit // n_chan
    mesh_id = pl.DeviceIdType.MESH

    def target(off):
        return lax.rem(me + off, n_dev)

    def own_rows(first):
        return pl.ds(pl.multiple_of(first * share_rows, share_rows), share_rows)


    def loading(item, off, which):
        cols = pl.ds(pl.multiple_of(target(off) * LANES, LANES), LANES)
        return pltpu.make_async_copy((one_ref, two_ref)[which].at[:, cols], stage_ref.at[item % 2], stage_sem.at[item % 2])

    def weights(which, step):
        cols = pl.ds(pl.multiple_of(which * model + step * width, width), width)
        slot = lax.rem(which + step, 2)
        return pltpu.make_async_copy(w_hbm_ref.at[:, cols], w_ref.at[slot], w_sem.at[slot])

    def u_part(start, size, idx):
        return pltpu.make_async_copy(u_hbm_ref.at[pl.ds(start, size), :], u_ref.at[pl.ds(start, size), :], u_sem.at[idx])

    def halo_send():
        return pltpu.make_async_remote_copy(tail_ref, halo_ref, halo_sem.at[0], halo_sem.at[1], device_id={"sp": target(1)}, device_id_type=mesh_id)

    def hold_of(dest):
        return done_ref.at[dest, :, pl.ds(0, share_rows), :]

    def share_send(off):
        dest = target(off)
        return pltpu.make_async_remote_copy(
            hold_of(dest), filt_ref.at[:, me, own_rows(my_group), :], hold_sem.at[off], share_sem.at[off], device_id={"sp": dest}, device_id_type=mesh_id
        )

    def group_send(k, off):
        mine = filt_ref.at[k, :, own_rows(my_group), :]
        return pltpu.make_async_remote_copy(
            mine, mine, group_sem.at[k], filt_sem.at[k], device_id={"dp": lax.rem(my_group + off, n_groups)}, device_id_type=mesh_id
        )

    def other_groups(k):
        same_size = filt_ref.at[k, :, pl.ds(0, (n_groups - 1) * share_rows), :]
        return pltpu.make_async_copy(same_size, same_size, filt_sem.at[k])

    def turned_out(slot, step):
        return pltpu.make_async_copy(turned_ref.at[slot], sent_ref.at[:, pl.ds(step * (width // LANES), width // LANES), slot], out_sem.at[slot])

    def mixed_out(step):
        return pltpu.make_async_copy(mixed_ref, gate_ref.at[:, pl.ds(step * (width // LANES), width // LANES)], out_sem.at[2])

    def sending(k, off, span):
        dest, chunks = target(off), pl.ds(k, span)
        return pltpu.make_async_remote_copy(
            sent_ref.at[chunks, dest], got_ref.at[chunks, me], sent_sem.at[k, off], got_sem.at[k, off], device_id={"sp": dest}, device_id_type=mesh_id
        )

    def block_in(k, off):
        src = lax.rem(me - off + n_dev, n_dev)
        from_ref, slot = (got_ref if off else sent_ref), lax.rem(k, 2)
        return pltpu.make_async_copy(from_ref.at[k, src], block_ref.at[slot, src], block_sem.at[slot, off])

    def returning(k, off):
        dest = target(off)
        return pltpu.make_async_remote_copy(
            done_ref.at[pl.ds(k, 2), dest],
            back_ref.at[pl.ds(k, 2), me],
            done_sem.at[k, off],
            back_sem.at[k, off],
            device_id={"sp": dest},
            device_id_type=mesh_id,
        )

    def storing(k):
        return pltpu.make_async_copy(done_ref.at[pl.ds(k, 2), me], back_ref.at[pl.ds(k, 2), me], done_sem.at[k, 0])

    last_pair = n_chunks - 2
    tile = filt_ref.shape[2]
    n_tiles = rows // tile
    piece = tile // LANES * n_chan

    def piece_of(part):
        return pl.ds(part[0] * piece, part[1] * piece)

    def returning_rows(part, off):
        dest = target(off)
        return pltpu.make_async_remote_copy(
            done_ref.at[pl.ds(last_pair, 2), dest, piece_of(part)],
            back_ref.at[pl.ds(last_pair, 2), me, piece_of(part)],
            piece_sem.at[part[0], off],
            piece_got_sem.at[part[0], off],
            device_id={"sp": dest},
            device_id_type=mesh_id,
        )

    def storing_rows(part):
        last = pl.ds(last_pair, 2)
        return pltpu.make_async_copy(done_ref.at[last, me, piece_of(part)], back_ref.at[last, me, piece_of(part)], piece_sem.at[part[0], 0])

    def constant(idx):
        return pltpu.make_async_copy(consts_in[idx], consts[idx], const_sem.at[idx])


    barrier = pltpu.get_barrier_semaphore()
    for off in range(1, n_dev):
        pl.semaphore_signal(barrier, inc=1, device_id={"sp": target(off)}, device_id_type=mesh_id)
    for off in range(1, n_groups):
        pl.semaphore_signal(barrier, inc=1, device_id={"dp": lax.rem(my_group + off, n_groups)}, device_id_type=mesh_id)

    order = far_first(n_dev) + [0]

    def load(item):
        for which in range(2):

            @pl.when(which_mine == which)
            def _():
                loading(item, order[item], which).start()

    load(0)
    u_part(rows - 16, 16, 1).start()
    for item, off in enumerate(order):
        if item + 1 < len(order):
            load(item + 1)
        if item == 0:
            u_part(0, rows - 16, 0).start()
            weights(0, 0).start()
            for idx in range(len(consts)):
                constant(idx).start()
        loading(item, off, 0).wait()
        if units < n_chan:
            into = turned_ref.at[0, :, 0]
        elif off:
            into = done_ref.at[target(off)]
        else:
            into = filt_ref.at[:, me, own_rows(my_group), :]
        together = math.gcd(n_rows, 4)

        @pl.loop(0, n_rows // together)
        def _(i):
            for j in range(together):
                r = i * together + j
                turn_rows(stage_ref[item % 2, pl.ds(pl.multiple_of(r * LANES, LANES), LANES), :], into, n_chunks, r, n_rows)

        if units < n_chan:
            start = pl.multiple_of(lax.rem(first_unit, n_chan) * n_rows, n_rows)
            share = turned_ref[0, :, 0, pl.ds(start, share_rows), :]
            if off:
                done_ref[target(off), :, pl.ds(0, share_rows), :] = share
            else:
                filt_ref[:, me, own_rows(my_group), :] = share
        if item == 0:
            u_part(rows - 16, 16, 1).wait()
            tail_ref[...] = u_ref[pl.ds(rows - 16, 16), :].astype(F32)[8:]
            pl.semaphore_wait(barrier, n_dev + n_groups - 2)
            halo_send().start()
        if off:
            share_send(off).start()


    for idx in range(len(consts)):
        constant(idx).wait()
    u_part(0, rows - 16, 0).wait()
    halo_send().wait()

    @pl.loop(0, steps)
    def _(step):
        for which in range(3):
            if which < 2:
                weights(which + 1, step).start()
            else:

                @pl.when(step + 1 < steps)
                def _():
                    weights(0, step + 1).start()

            weights(which, step).wait()
            w_now = w_ref.at[lax.rem(which + step, 2)]
            cols = pl.ds(pl.multiple_of(which * model + step * width, width), width)
            bias = bias_ref[:, cols]
            halo = (dot32(halo_ref[...].astype(BF16), w_now[...]) + bias).astype(BF16).astype(F32)
            p_ref[0:8, :] = jnp.where(me > 0, halo, 0.0)
            tile = 2 * LANES

            @pl.loop(0, rows // tile)
            def _(i):
                start = pl.multiple_of(i * tile, tile)
                proj = dot32(u_ref[pl.ds(start, tile), :], w_now[...]) + bias
                p_ref[pl.ds(start + 8, tile), :] = proj.astype(BF16).astype(F32)

            c0, c1, c2 = (taps_ref[t : t + 1, cols] for t in range(3))
            slot = 1 if which == 0 else 0

            @pl.when(step > 0)
            def _():
                if which == 1:
                    mixed_out(step - 1).wait()
                else:
                    turned_out(slot, step - 1).wait()

            @pl.loop(0, n_rows)
            def _(r):
                start = pl.multiple_of(r * LANES, LANES)
                window = p_ref[pl.ds(start, LANES + 8), :]
                mixed = c0 * window[8:] + c1 * window[7:-1] + c2 * window[6:-2]
                mixed = mixed.astype(BF16)
                for d in range(width // LANES):
                    block = mixed[:, d * LANES : (d + 1) * LANES].astype(F32)
                    if which != 1:
                        turn_rows(block, turned_ref.at[slot, :, d], n_chunks, r, n_rows)
                        continue
                    turned = block.T.astype(BF16)
                    for k in range(n_chunks):
                        at = pl.ds(pl.multiple_of(r * n_chan, n_chan), n_chan)
                        mixed_ref[k, d, at, :] = turned[k * n_chan : (k + 1) * n_chan]

            if which == 1:
                mixed_out(step).start()
            else:
                turned_out(slot, step).start()

    turned_out(0, steps - 1).wait()
    turned_out(1, steps - 1).wait()
    mixed_out(steps - 1).wait()

    spans = send_spans(n_chunks)
    for k, span in spans:
        for off in far_first(n_dev):
            sending(k, off, span).start()


    for off in range(1, n_dev):
        share_send(off).wait()

    @pl.loop(0, n_chunks)
    def _(k):
        for off in range(1, n_groups):
            group_send(k, off).start()


    spectrum, signal = spectrum_tools(group, n_high, tables, parts_ref)

    def fetch(k):
        block_in(k, 0).start()
        for first, span in spans:

            @pl.when(k == first)
            def _():
                for off in range(1, n_dev):
                    sending(first, off, span).wait_recv()

        for off in range(1, n_dev):
            block_in(k, off).start()

    fetch(jnp.int32(0))

    @pl.loop(0, n_chunks)
    def _(k):
        slot = lax.rem(k, 2)
        other_groups(k).wait()
        for off in range(n_dev):
            block_in(k, off).wait()

        @pl.loop(0, n_chan // group)
        def _(i):
            first = i * group

            @pl.when(jnp.logical_and(i == n_chan // group - 1, k + 1 < n_chunks))
            def _():
                fetch(k + 1)

            def load_h(which, g):
                start = pl.multiple_of((which * n_chan + first + g) * n_rows, n_rows)
                return filt_ref[k, :, pl.ds(start, n_rows), :].reshape(n_high, LANES)

            def load_x(which, g):
                start = pl.multiple_of((first + g) * n_rows, n_rows)
                return block_ref[slot, :, which, pl.ds(start, n_rows), :].reshape(n_high, LANES)

            chan = me * LANES + k * n_chan + first
            spec_one_ref[...] = spectrum([load_h(0, g) for g in range(group)], False)
            spec_two_ref[...] = spectrum([load_h(1, g) for g in range(group)], False)
            values = [load_x(0, g) for g in range(group)]
            conv = signal(spectrum(values, True), spec_one_ref)
            gated = [load_x(1, g) * (conv[g] + skip_one_ref[chan + g] * values[g]) for g in range(group)]
            conv = signal(spectrum(gated, False), spec_two_ref)
            for g in range(group):
                result = conv[g] + skip_two_ref[chan + g] * gated[g]
                done_ref[k, :, pl.ds(first + g, n_rows, stride=n_chan), :] = result.reshape(n_dev, n_rows, LANES)

        @pl.when(jnp.logical_and(k < last_pair, lax.rem(k, 2) == 1))
        def _():
            storing(k - 1).start()
            for off in far_first(n_dev):
                returning(k - 1, off).start()


    parts = row_spans(n_tiles)
    for part in parts:
        storing_rows(part).start()
        for off in far_first(n_dev):
            returning_rows(part, off).start()

    for k, span in spans:
        for off in range(1, n_dev):
            sending(k, off, span).wait_send()

    @pl.loop(0, n_chunks)
    def _(k):
        for off in range(1, n_groups):
            group_send(k, off).wait_send()


    @pl.loop(0, n_tiles)
    def _(q):
        for e in range(model // LANES):
            part = u_ref[pl.ds(pl.multiple_of(q * tile, tile), tile), e * LANES : (e + 1) * LANES]
            filt_ref[e, q] = part.astype(F32)

    def pair_in(k, j):
        return (
            pltpu.make_async_copy(back_ref.at[k], block_ref.at[0, :, j], pair_sem.at[j, 0]),
            pltpu.make_async_copy(gate_ref.at[k], mixed_ref.at[:, j], pair_sem.at[j, 1]),
            w_pair_in(k, j),
        )

    def w_pair_in(k, j):
        return pltpu.make_async_copy(w_out_ref.at[:, k], w_pair_ref.at[j], pair_sem.at[j, 2])

    def product(q):
        for t in range(tile // LANES):
            for j in range(2):
                at = pl.ds(pl.multiple_of((q * (tile // LANES) + t) * n_chan, n_chan), n_chan)
                gated = block_ref[0, :, j, at, :] * mixed_ref[:, j, at, :].astype(F32)
                gated_ref[t * LANES : (t + 1) * LANES, j * LANES : (j + 1) * LANES] = gated.reshape(LANES, LANES).T.astype(BF16)
        return dot32(gated_ref[...], w_pair_ref[...].reshape(2 * LANES, model))

    @pl.loop(0, n_chunks // 2 - 1)
    def _(p):
        storing(2 * p).wait()
        for off in range(1, n_dev):
            returning(2 * p, off).wait()
        for j in range(2):
            for copy in pair_in(2 * p + j, j):
                copy.start()
        for j in range(2):
            for copy in pair_in(2 * p + j, j):
                copy.wait()

        @pl.loop(0, n_tiles)
        def _(q):
            added = product(q)
            for e in range(model // LANES):
                filt_ref[e, q] = filt_ref[e, q] + added[:, e * LANES : (e + 1) * LANES]

    sum_out = pltpu.make_async_copy(filt_ref.at[:, n_tiles - 1], sum_ref, sum_sem)
    sum_out.start()

    def rows_of(q):
        return pl.ds(pl.multiple_of(q * tile, tile), tile)

    def most_out(q):
        return pltpu.make_async_copy(u_ref.at[rows_of(q)], most_ref.at[rows_of(q)], most_sem.at[q])

    def rows_in(part, j):
        k, at = last_pair + j, piece_of(part)
        return (
            pltpu.make_async_copy(back_ref.at[k, :, at], block_ref.at[0, :, j, at], pair_sem.at[j, 0]),
            pltpu.make_async_copy(gate_ref.at[k, :, at], mixed_ref.at[:, j, at], pair_sem.at[j, 1]),
        )

    if n_tiles > 1:
        for j in range(2):
            w_pair_in(last_pair + j, j).start()
        for j in range(2):
            w_pair_in(last_pair + j, j).wait()

    for part in parts[:-1]:
        storing_rows(part).wait()
        for off in range(1, n_dev):
            returning_rows(part, off).wait()
        for j in range(2):
            for copy in rows_in(part, j):
                copy.start()
        for j in range(2):
            for copy in rows_in(part, j):
                copy.wait()

        @pl.loop(part[0], part[0] + part[1])
        def _(q):
            added = product(q)
            for e in range(model // LANES):
                cols = slice(e * LANES, (e + 1) * LANES)
                u_ref[rows_of(q), cols] = (filt_ref[e, q] + added[:, cols]).astype(BF16)
            most_out(q).start()

    storing_rows(parts[-1]).wait()
    for off in range(1, n_dev):
        returning_rows(parts[-1], off).wait()
    sum_out.wait()

    @pl.loop(0, n_tiles - 1)
    def _(q):
        most_out(q).wait()


def hyena(skip_one, skip_two, u, filt_one, filt_two, w_in, w_out, bias, taps, tables, n_dev, n_groups, units, group=4):
    rows, depth = u.shape
    model = w_in.shape[1] // 3
    width = 2 * LANES
    n_rows = rows // LANES
    n_chunks = n_dev
    n_high = n_dev * n_rows
    chunk_rows = LANES // n_chunks * n_rows
    tile = 2 * chunk_rows
    hbm_spec = pl.BlockSpec(memory_space=pltpu.HBM)
    consts = (bias, taps, *tables)
    dma = pltpu.SemaphoreType.DMA
    return pl.pallas_call(
        functools.partial(hyena_body, n_dev, n_groups, units, group),
        in_specs=[hbm_spec] * (7 + len(consts)),
        out_specs=[hbm_spec] * 6,
        out_shape=[
            jax.ShapeDtypeStruct((n_chunks, n_dev, 2, chunk_rows, LANES), F32),
            jax.ShapeDtypeStruct((n_chunks, n_dev, chunk_rows, LANES), BF16),
            jax.ShapeDtypeStruct((n_chunks, n_dev, 2, chunk_rows, LANES), F32),
            jax.ShapeDtypeStruct((n_chunks, n_dev, chunk_rows, LANES), F32),
            jax.ShapeDtypeStruct((model // LANES, tile, LANES), F32),
            jax.ShapeDtypeStruct((rows, model), BF16),
        ],
        scratch_shapes=[
            pltpu.SMEM(skip_one.shape, F32),
            pltpu.SMEM(skip_two.shape, F32),
            *[pltpu.VMEM(c.shape, c.dtype) for c in consts],
            dma((2 + len(consts),)),
            pltpu.VMEM((rows, depth), BF16),
            pltpu.VMEM((2, depth, width), BF16),
            pltpu.VMEM((rows + 8, width), F32),
            pltpu.VMEM((2, rows, LANES), F32),
            pltpu.VMEM((2, n_chunks, width // LANES, chunk_rows, LANES), F32),
            pltpu.VMEM((n_chunks, width // LANES, chunk_rows, LANES), BF16),
            pltpu.VMEM((8, depth), F32),
            pltpu.VMEM((8, depth), F32),
            pltpu.VMEM((n_chunks, n_dev, 2 * chunk_rows, LANES), F32),
            pltpu.VMEM((2, n_dev, 2, chunk_rows, LANES), F32),
            pltpu.VMEM((n_chunks, n_dev, chunk_rows, LANES), F32),
            pltpu.VMEM((group * n_high, 6 * LANES), BF16),
            pltpu.VMEM((group * n_high, 2 * LANES), F32),
            pltpu.VMEM((group * n_high, 2 * LANES), F32),
            pltpu.VMEM((2 * chunk_rows, 2 * LANES), BF16),
            pltpu.VMEM((2, n_dev, LANES // n_chunks, model), BF16),
            dma((2,)),
            dma((2,)),
            dma((2,)),
            dma((3,)),
            dma((2,)),
            dma((n_dev,)),
            dma((n_dev,)),
            dma((n_chunks,)),
            dma((n_chunks,)),
            dma((n_chunks, n_dev)),
            dma((n_chunks, n_dev)),
            dma((2, n_dev)),
            dma((n_chunks, n_dev)),
            dma((n_chunks, n_dev)),
            dma((2, 3)),
            dma,
            dma((rows // tile,)),
            dma((rows // tile, n_dev)),
            dma((rows // tile, n_dev)),
        ],
        cost_estimate=pl.CostEstimate(flops=10**11, bytes_accessed=100 * 2**20, transcendentals=0),
        compiler_params=pltpu.CompilerParams(collective_id=0, has_side_effects=True, vmem_limit_bytes=54 * 2**20),
        name="hyena",
    )(u, filt_one, filt_two, w_in, w_out, skip_one, skip_two, *consts)


def finish_body(n_rows, most_hbm_ref, sum_hbm_ref, gate_hbm_ref, back_hbm_ref, w_hbm_ref, out_hbm_ref, *refs):
    sum_ref, gate_ref, back_ref, w_ref, out_ref, gated_ref, in_sem, w_sem, most_sem, out_sem = refs
    first = gate_hbm_ref.shape[0] - 2
    rows = out_ref.shape[0]
    first_row = rows - sum_ref.shape[1]
    tile = n_rows * LANES
    n_tiles = sum_ref.shape[1] // tile
    n_most = first_row // sum_ref.shape[1]

    def tile_in(i):
        at = pl.ds(i * tile, tile)
        narrow, wide = pl.ds(i * n_rows, n_rows), pl.ds(first_row // LANES + i * n_rows, n_rows)
        return (
            pltpu.make_async_copy(sum_hbm_ref.at[:, at], sum_ref.at[:, at], in_sem.at[i, 0]),
            pltpu.make_async_copy(gate_hbm_ref.at[pl.ds(first, 2), :, wide], gate_ref.at[:, :, narrow], in_sem.at[i, 1]),
            pltpu.make_async_copy(back_hbm_ref.at[pl.ds(first, 2), :, wide], back_ref.at[:, :, narrow], in_sem.at[i, 2]),
        )

    def most(i, out):
        at = pl.ds(i * sum_ref.shape[1], sum_ref.shape[1])
        if out:
            return pltpu.make_async_copy(out_ref.at[at], out_hbm_ref.at[at], most_sem.at[i])
        return pltpu.make_async_copy(most_hbm_ref.at[at], out_ref.at[at], most_sem.at[i])

    def tile_out(i):
        at = pl.ds(first_row + i * tile, tile)
        return pltpu.make_async_copy(out_ref.at[at], out_hbm_ref.at[at], out_sem.at[i])

    w_in = pltpu.make_async_copy(w_hbm_ref.at[:, pl.ds(first, 2)], w_ref, w_sem)
    w_in.start()
    for i in range(n_tiles):
        if i == n_tiles - 1:
            for m in range(n_most):
                most(m, False).start()
        for copy in tile_in(i):
            copy.start()
    w_in.wait()
    w_pair = jnp.concatenate([w_ref[:, j].reshape(LANES, w_ref.shape[3]) for j in range(2)], axis=0)
    for i in range(n_tiles):
        if i == n_tiles - 1:
            for m in range(n_most):
                most(m, False).wait()
                most(m, True).start()
        for copy in tile_in(i):
            copy.wait()
        for r in range(n_rows):
            for j in range(2):
                gated = back_ref[j, :, i * n_rows + r] * gate_ref[j, :, i * n_rows + r].astype(F32)
                gated_ref[r * LANES : (r + 1) * LANES, j * LANES : (j + 1) * LANES] = gated.reshape(LANES, LANES).T.astype(BF16)
        added = dot32(gated_ref[...], w_pair)
        for e in range(sum_ref.shape[0]):
            cols = slice(e * LANES, (e + 1) * LANES)
            out_ref[first_row + i * tile : first_row + (i + 1) * tile, cols] = (sum_ref[e, i * tile : (i + 1) * tile] + added[:, cols]).astype(BF16)
        tile_out(i).start()
    for i in range(n_tiles):
        tile_out(i).wait()
    for i in range(n_most):
        most(i, True).wait()


def finish(most, partial, gate, back, w_out, n_rows=2):
    _, n_src, _, n_chan, _ = back.shape
    rows, model = most.shape
    last_rows = partial.shape[1]
    n_tiles = last_rows // (n_rows * LANES)
    hbm_spec = pl.BlockSpec(memory_space=pltpu.HBM)
    returned = (2, n_src, last_rows // LANES, n_chan, LANES)
    return pl.pallas_call(
        functools.partial(finish_body, n_rows),
        in_specs=[hbm_spec] * 5,
        out_specs=hbm_spec,
        out_shape=jax.ShapeDtypeStruct((rows, model), BF16),
        scratch_shapes=[
            pltpu.VMEM(partial.shape, F32),
            pltpu.VMEM(returned, BF16),
            pltpu.VMEM(returned, F32),
            pltpu.VMEM((n_src, 2, n_chan, model), BF16),
            pltpu.VMEM((rows, model), BF16),
            pltpu.VMEM((n_rows * LANES, 2 * LANES), BF16),
            pltpu.SemaphoreType.DMA((n_tiles, 3)),
            pltpu.SemaphoreType.DMA,
            pltpu.SemaphoreType.DMA((max(1, rows // last_rows - 1),)),
            pltpu.SemaphoreType.DMA((n_tiles,)),
        ],
        cost_estimate=pl.CostEstimate(flops=4 * last_rows * model * LANES, bytes_accessed=11 * 2**20, transcendentals=0),
        compiler_params=pltpu.CompilerParams(vmem_limit_bytes=56 * 2**20),
        name="finish",
    )(most, partial, gate, back, w_out)


def solution(mesh):
    n_dev, n_groups = mesh.shape["sp"], mesh.shape["dp"]
    n_chunks = n_dev
    n_chan = LANES // n_chunks
    if n_groups < 2 or (2 * n_chan) % n_groups:
        raise ValueError("uneven groups")
    units = 2 * n_chan // n_groups

    def local_step(u_in, w_in, b_in, conv_taps, w_out, skip_one, skip_two, filt_one, filt_two):
        u = u_in[0]
        rows = u.shape[0]
        tables = [jnp.asarray(t) for t in transform_tables(rows * n_dev)]
        w_blocks = w_out.reshape(n_dev, n_chunks, n_chan, w_out.shape[1])
        _, gate, _, back, partial, most = hyena(
            skip_one, skip_two, u, filt_one, filt_two, w_in, w_blocks, b_in[None], conv_taps, tables, n_dev, n_groups, units
        )
        by_row = (n_chunks, n_dev, rows // LANES, n_chan, LANES)
        return finish(most, partial, gate.reshape(by_row), back.reshape(by_row), w_blocks)[None]

    seq_spec = P("dp", "sp", None)
    filt_spec = P("sp", None)
    return jax.shard_map(
        local_step,
        mesh=mesh,
        in_specs=(seq_spec, P(), P(), P(), P(), P(), P(), filt_spec, filt_spec),
        out_specs=seq_spec,
        check_vma=False,
    )
```
